32 devices in a mesh: rep: 2 (over x), fsdp: 16 (over z, y, core).
Axes of the slice: x: 2, y: 2, z: 4, core: 2. Of those that a mesh axis runs over, the one named last changes fastest.
Arguments:
- layer_input: bfloat16 [4096, 2048], P(('rep', 'fsdp')), may hold values from -6 to 6
- segment: int32 [32, 128], P(('rep', 'fsdp')), may hold values from 0 to 1, as said below
- live_mask: int32 [32, 128], P(('rep', 'fsdp')), may hold values from 0 to 1, as said below
- attention_gain: bfloat16 [2048], P('fsdp'), may hold values from 0.099609375 to 1.8984375
- attention_shift: bfloat16 [2048], P('fsdp'), may hold values from -4 to 4
- joined_weight: bfloat16 [2048, 6144], P('fsdp'), may hold values from -0.125 to 0.125
- joined_bias: bfloat16 [6144], P('fsdp'), may hold values from -4 to 4
- output_weight: bfloat16 [2048, 2048], P('fsdp'), may hold values from -0.375 to 0.375
- output_bias: bfloat16 [2048], P('fsdp'), may hold values from -4 to 4
- feedforward_gain: bfloat16 [2048], P('fsdp'), may hold values from 0.099609375 to 1.8984375
- feedforward_shift: bfloat16 [2048], P('fsdp'), may hold values from -4 to 4
- expand_weight: bfloat16 [2048, 8192], P('fsdp'), may hold values from -0.125 to 0.125
- expand_bias: bfloat16 [8192], P('fsdp'), may hold values from -4 to 4
- shrink_weight: bfloat16 [8192, 2048], P('fsdp'), may hold values from -0.0625 to 0.0625
- shrink_bias: bfloat16 [2048], P('fsdp'), may hold values from -4 to 4
- cotangent: bfloat16 [4096, 2048], P(('rep', 'fsdp')), may hold values from -6 to 6
Outputs:
- layer_output: bfloat16 [4096, 2048], P(('rep', 'fsdp'))
- input_grad: bfloat16 [4096, 2048], P(('rep', 'fsdp'))
- attention_gain_grad: float32 [2048], P('fsdp')
- attention_shift_grad: float32 [2048], P('fsdp')
- joined_weight_grad: float32 [2048, 6144], P('fsdp')
- joined_bias_grad: float32 [6144], P('fsdp')
- output_weight_grad: float32 [2048, 2048], P('fsdp')
- output_bias_grad: float32 [2048], P('fsdp')
- feedforward_gain_grad: float32 [2048], P('fsdp')
- feedforward_shift_grad: float32 [2048], P('fsdp')
- expand_weight_grad: float32 [2048, 8192], P('fsdp')
- expand_bias_grad: float32 [8192], P('fsdp')
- shrink_weight_grad: float32 [8192, 2048], P('fsdp')
- shrink_bias_grad: float32 [2048], P('fsdp')
The draws below stay inside these ranges and needn't reach their ends.
Inputs may be any that keep to these rules, and one draw needn't show every extreme that they name: `segment`: within each slot the number is 0 on a first sequence of 32 to 128 positions and 1 after it, never falling; in at least one slot the first sequence fills all 128 positions, not always the same slot. `live_mask`: in each slot the 1s form a prefix that covers the first sequence; positions after it are padding. At least one slot is live in all 128 positions.
All inputs are finite; a program needn't handle non-finite values.
Results may differ from the reference program's by a relative error of at most 0.0095.
Values may be sent and summed in bfloat16 or wider, within the bound.
A program may use at most 448 MiB of HBM per device.

```python
import jax
import jax.numpy as jnp
from jax import lax

D = 2048
HEADS = 16
HEAD_DIM = 128
ROT = 32
FF = 8192
SLOT = 128
SLOTS = 32
TOKENS = 4096


def packing(key):
    first_key = jax.random.fold_in(key, 101)
    second_key = jax.random.fold_in(key, 202)
    whole_key = jax.random.fold_in(key, 303)
    slot_index = jnp.arange(SLOTS, dtype=jnp.int32)
    first = jax.random.randint(first_key, (SLOTS,), SLOT // 4, SLOT + 1, dtype=jnp.int32)
    chosen = jax.random.randint(whole_key, (), 0, SLOTS, dtype=jnp.int32)
    first = jnp.where(slot_index == chosen, SLOT, first)
    second = jax.random.randint(second_key, (SLOTS,), 0, SLOT - first + 1, dtype=jnp.int32)
    column = jnp.arange(SLOT, dtype=jnp.int32)[None, :]
    segment = (column >= first[:, None]).astype(jnp.int32)
    live = (column < (first + second)[:, None]).astype(jnp.int32)
    return (segment, live)


def draw_segment(key, part):
    return packing(key)[0]


def draw_live_mask(key, part):
    return packing(key)[1]


def with_spikes(array, own_key, source, target, blocks, factor):
    def block_of(dim):
        return (jnp.arange(array.shape[dim]) // (array.shape[dim] // blocks)).reshape((-1,) + (1,) * (array.ndim - 1 - dim))

    near = jax.random.permutation(own_key, blocks)[block_of(target)]
    second = (block_of(target) + blocks // 2) % blocks
    return jnp.where((block_of(source) == near) | (block_of(source) == second), factor * array, array)


def levels(key, shape, pieces, least, top_value):
    factor_of = 1.0
    for dim, shards_of in pieces:
        draws = jax.random.uniform(jax.random.fold_in(jax.random.fold_in(key, 6), dim), (shards_of,), jnp.float32, least / len(pieces), top_value / len(pieces))
        factor_of = factor_of * jnp.repeat(jnp.exp(draws), shape[dim] // shards_of).reshape((-1,) + (1,) * (len(shape) - 1 - dim))
    return factor_of


def noise(own_key, shape, width, limit, pieces=(), held_as=jnp.bfloat16):
    drawn = jax.random.normal(own_key, shape, jnp.float32) * width
    if len(pieces) > 0:
        drawn = levels(own_key, shape, pieces, -0.22, 0.18) * drawn
    return jnp.clip(drawn, min=-limit, max=limit).astype(held_as)


def bell_draw_with(rng, dims, spread, reach, pieces, heavy, held_as=jnp.bfloat16):
    drawn = spread * jax.random.normal(rng, dims, jnp.float32)
    if pieces:
        drawn = drawn * levels(rng, dims, pieces, -0.22, 0.18)
    return jnp.clip(with_spikes(drawn, jax.random.fold_in(rng, 3), *heavy), -reach, reach).astype(held_as)


def setup_inputs(seed: int = 0) -> dict:
    arg_keys = jax.random.split(jax.random.key(seed), 17)
    layer_input = noise(arg_keys[0], (TOKENS, D), 1.0, 6.0, ((0, 32),))
    segment = draw_segment(jax.random.fold_in(arg_keys[16], 71), 0)
    live_mask = draw_live_mask(jax.random.fold_in(arg_keys[16], 71), 0)
    attention_gain = jnp.clip(1.0 + 0.18 * jax.random.normal(arg_keys[3], (D,), jnp.float32), 0.099609375, 1.8984375).astype(jnp.bfloat16)
    attention_shift = noise(arg_keys[4], (D,), 0.3, 4.0, ((0, 16),))
    joined_weight = noise(arg_keys[5], (D, 3 * D), D ** -0.5, 0.125, ((0, 16),))
    joined_bias = noise(arg_keys[6], (3 * D,), 0.3, 4.0, ((0, 16),))
    output_weight = noise(arg_keys[7], (D, D), (D // 8) ** -0.5, 0.375, ((0, 16),))
    output_bias = noise(arg_keys[8], (D,), 0.3, 4.0, ((0, 16),))
    feedforward_gain = jnp.clip(1.0 + 0.18 * jax.random.normal(arg_keys[9], (D,), jnp.float32), 0.099609375, 1.8984375).astype(jnp.bfloat16)
    feedforward_shift = noise(arg_keys[10], (D,), 0.3, 4.0, ((0, 16),))
    expand_weight = noise(arg_keys[11], (D, FF), D ** -0.5, 0.125, ((0, 16),))
    expand_bias = noise(arg_keys[12], (FF,), 0.3, 4.0, ((0, 16),))
    shrink_weight = noise(arg_keys[13], (FF, D), FF ** -0.5, 0.0625, ((0, 16),))
    shrink_bias = noise(arg_keys[14], (D,), 0.3, 4.0, ((0, 16),))
    cotangent = bell_draw_with(arg_keys[15], (TOKENS, D), 1.0, 6.0, ((0, 32),), (0, 1, 32, 2.75))
    return {"layer_input": layer_input, "segment": segment, "live_mask": live_mask, "attention_gain": attention_gain, "attention_shift": attention_shift, "joined_weight": joined_weight, "joined_bias": joined_bias, "output_weight": output_weight, "output_bias": output_bias, "feedforward_gain": feedforward_gain, "feedforward_shift": feedforward_shift, "expand_weight": expand_weight, "expand_bias": expand_bias, "shrink_weight": shrink_weight, "shrink_bias": shrink_bias, "cotangent": cotangent}


epsilon = 1e-05
masked_score = -1e+30
rotary_base = 10000.0

@jax.custom_vjp
def low(v):
    return lax.optimization_barrier(v.astype(jnp.bfloat16)).astype(jnp.float32)

@jax.custom_vjp
def low_back(v):
    return v

def low_keep(v):
    return (low(v), None)

def low_pass(kept, grad):
    return (grad,)

def back_keep(v):
    return (v, None)

def back_low(kept, grad):
    return (low(grad),)
low.defvjp(low_keep, low_pass)
low_back.defvjp(back_keep, back_low)

def highest(form, left, right):
    return jnp.einsum(form, left, right, precision=lax.Precision.HIGHEST)

def norm_rows(rows, gain, shift):
    centre = lax.optimization_barrier(jnp.mean(rows, -1, keepdims=True))
    centred = rows - centre
    inverse = lax.rsqrt(lax.optimization_barrier(jnp.mean(centred * centred, -1, keepdims=True)) + epsilon)
    return centred * inverse * gain + shift

def rotary_tables(segment):
    length = segment.shape[-1]
    places = jnp.arange(length, dtype=jnp.int32)
    earlier = lax.optimization_barrier(jnp.sum((segment[..., None, :] < segment[..., :, None]).astype(jnp.int32), -1))
    position = (places - earlier).astype(jnp.float32)
    exponent = jnp.arange(ROT // 2, dtype=jnp.float32) * 2.0 / ROT
    frequency = jnp.power(jnp.float32(rotary_base), -exponent)
    angle = position[..., None] * frequency
    return (jnp.cos(angle), jnp.sin(angle))

def turn(heads, cosine, sine, sign):
    half = ROT // 2
    front = heads[..., :half]
    behind = heads[..., half:ROT]
    cos_wide = cosine[..., None, :]
    sin_wide = sine[..., None, :] * sign
    return jnp.concatenate([front * cos_wide - behind * sin_wide, behind * cos_wide + front * sin_wide, heads[..., ROT:]], -1)

def forward(rows, params, segment, live_rows):
    attention_gain, attention_shift, joined_weight, joined_bias, output_weight, output_bias, feedforward_gain, feedforward_shift, expand_weight, expand_bias, shrink_weight, shrink_bias = params
    batch, length = segment.shape
    normed_one = low(norm_rows(rows, attention_gain, attention_shift))
    joined = low_back(highest('bsd,de->bse', normed_one, joined_weight) + joined_bias)
    split = joined.reshape(batch, length, 3, HEADS, HEAD_DIM)
    cosine, sine = rotary_tables(segment)
    queries = low(turn(split[:, :, 0], cosine, sine, 1.0))
    keys = low(turn(split[:, :, 1], cosine, sine, 1.0))
    values = low(split[:, :, 2])
    scores = low_back(highest('bthd,bshd->bhts', queries, keys) * HEAD_DIM ** (-0.5))
    places = jnp.arange(length, dtype=jnp.int32)
    allowed = (segment[:, :, None] == segment[:, None, :]) & (places[None, None, :] <= places[None, :, None])
    scores = jnp.where(allowed[:, None], scores, masked_score)
    top = lax.optimization_barrier(jnp.max(scores, -1, keepdims=True))
    weights = jnp.exp(scores - top)
    weights = weights / lax.optimization_barrier(jnp.sum(weights, -1, keepdims=True))
    mixed = highest('bhts,bshd->bthd', low(weights), values).reshape(batch, length, D)
    mixed = low(low_back(mixed))
    attended = low_back(highest('bsd,de->bse', mixed, output_weight) + output_bias)
    normed_two = low(norm_rows(rows, feedforward_gain, feedforward_shift))
    expanded = low_back(highest('bsd,df->bsf', normed_two, expand_weight) + expand_bias)
    activated = low(jax.nn.gelu(expanded, approximate=False))
    shrunk = low_back(highest('bsf,fd->bsd', activated, shrink_weight) + shrink_bias)
    return rows + live_rows[..., None] * (attended + shrunk)

def reference(layer_input, segment, live_mask, attention_gain, attention_shift, joined_weight, joined_bias, output_weight, output_bias, feedforward_gain, feedforward_shift, expand_weight, expand_bias, shrink_weight, shrink_bias, cotangent):
    params = tuple((item.astype(jnp.float32) for item in (attention_gain, attention_shift, joined_weight, joined_bias, output_weight, output_bias, feedforward_gain, feedforward_shift, expand_weight, expand_bias, shrink_weight, shrink_bias)))
    slots, length = segment.shape
    group = max(1, min(slots, 4096 // length))
    while slots % group:
        group = group - 1
    blocks = slots // group
    rows = layer_input.astype(jnp.float32).reshape(blocks, group, length, D)
    seeds = cotangent.astype(jnp.float32).reshape(blocks, group, length, D)
    segments = segment.reshape(blocks, group, length)
    lives = live_mask.astype(jnp.float32).reshape(blocks, group, length)

    def step(totals, inputs):
        block_rows, block_segment, block_live, block_seed = inputs

        def local(rows_in, params_in):
            return forward(rows_in, params_in, block_segment, block_live)
        result, pullback = jax.vjp(local, block_rows, params)
        row_grads, param_grads = pullback(block_seed)
        totals = jax.tree.map(jnp.add, totals, param_grads)
        return (totals, (result.astype(jnp.bfloat16), row_grads.astype(jnp.bfloat16)))
    start = tuple((jnp.zeros_like(item) for item in params))
    totals, (outputs, input_grads) = lax.scan(step, start, (rows, segments, lives, seeds))
    return (outputs.reshape(slots * length, D), input_grads.reshape(slots * length, D), totals[0], totals[1], totals[2], totals[3], totals[4], totals[5], totals[6], totals[7], totals[8], totals[9], totals[10], totals[11])
```

```python
import functools

import jax
import jax.numpy as jnp
from jax import lax
from jax.sharding import PartitionSpec as P

D = 2048
HEADS = 16
HEAD_DIM = 128
ROT = 32


epsilon = 1e-05
masked_score = -1e30
rotary_base = 10000.0


def as_sent(shard):
    return jax.tree.map(lambda a: a.astype(jnp.bfloat16) if a.dtype == jnp.float32 else a, shard)


def norm_rows(rows, gain, shift):
    centre = jnp.mean(rows, -1, keepdims=True)
    centred = rows - centre
    inverse = lax.rsqrt(jnp.mean(centred * centred, -1, keepdims=True) + epsilon)
    normalized = centred * inverse
    return (normalized * gain.astype(jnp.float32) + shift.astype(jnp.float32), normalized, inverse)


def norm_back(normed_grad, normalized, inverse, gain):
    scaled = normed_grad * gain.astype(jnp.float32)
    row_grad = inverse * (
        scaled
        - jnp.mean(scaled, -1, keepdims=True)
        - normalized * jnp.mean(scaled * normalized, -1, keepdims=True)
    )
    return (row_grad, jnp.sum(normed_grad * normalized, 0), jnp.sum(normed_grad, 0))


def rotary_tables(segment):
    length = segment.shape[-1]
    places = jnp.arange(length, dtype=jnp.int32)
    earlier = jnp.sum((segment[..., None, :] < segment[..., :, None]).astype(jnp.int32), -1)
    position = (places - earlier).astype(jnp.float32)
    exponent = jnp.arange(ROT // 2, dtype=jnp.float32) * 2.0 / ROT
    frequency = jnp.power(jnp.float32(rotary_base), -exponent)
    angle = position[..., None] * frequency
    return (jnp.cos(angle), jnp.sin(angle))


def turn(heads, cosine, sine, sign):
    half = ROT // 2
    front = heads[..., :half]
    behind = heads[..., half:ROT]
    cos_wide = cosine[..., None, :]
    sin_wide = sine[..., None, :] * sign
    return jnp.concatenate(
        [
            front * cos_wide - behind * sin_wide,
            behind * cos_wide + front * sin_wide,
            heads[..., ROT:],
        ],
        -1,
    )


def gelu_slope(values):
    return (
        0.5 * (1.0 + lax.erf(values * 0.7071067811865476))
        + values * jnp.exp(-0.5 * values * values) * 0.3989422804014327
    )


def attention_inputs(rows, weights, cosine, sine):
    gain, shift, joined_weight, joined_bias = (weights[0], weights[1], weights[2], weights[3])
    normed, normalized, inverse = norm_rows(rows, gain, shift)
    normed_low = normed.astype(jnp.bfloat16)
    joined = jnp.dot(
        normed_low, joined_weight, preferred_element_type=jnp.float32
    ) + joined_bias.astype(jnp.float32)
    length = rows.shape[0]
    split = joined.reshape(length, 3, HEADS, HEAD_DIM)
    queries = turn(split[:, 0], cosine, sine, 1.0).astype(jnp.bfloat16)
    keys = turn(split[:, 1], cosine, sine, 1.0).astype(jnp.bfloat16)
    values = split[:, 2].astype(jnp.bfloat16)
    return (normed_low, normalized, inverse, queries, keys, values)


def score_block(queries, keys, allowed):
    scores = jnp.einsum(
        "thd,shd->hts", queries, keys, preferred_element_type=jnp.float32
    ) * HEAD_DIM ** (-0.5)
    return jnp.where(allowed[None], scores, masked_score)


def feedforward_inputs(rows, weights):
    gain, shift, expand_weight, expand_bias = (weights[0], weights[1], weights[2], weights[3])
    normed, normalized, inverse = norm_rows(rows, gain, shift)
    normed_low = normed.astype(jnp.bfloat16)
    expanded = jnp.dot(
        normed_low, expand_weight, preferred_element_type=jnp.float32
    ) + expand_bias.astype(jnp.float32)
    return (normed_low, normalized, inverse, expanded)


def body(
    layer_input,
    segment,
    live_mask,
    attention_gain,
    attention_shift,
    joined_weight,
    joined_bias,
    output_weight,
    output_bias,
    feedforward_gain,
    feedforward_shift,
    expand_weight,
    expand_bias,
    shrink_weight,
    shrink_bias,
    cotangent,
):
    rows = layer_input.astype(jnp.float32)
    seg_row = segment[0]
    live_rows = live_mask[0].astype(jnp.float32)[:, None]
    length = seg_row.shape[0]
    cosine, sine = rotary_tables(seg_row)
    places = jnp.arange(length, dtype=jnp.int32)
    allowed = (seg_row[:, None] == seg_row[None, :]) & (places[None, :] <= places[:, None])
    attention_parts = (
        attention_gain,
        attention_shift,
        joined_weight,
        joined_bias,
        output_weight,
        output_bias,
    )
    feedforward_parts = (
        feedforward_gain,
        feedforward_shift,
        expand_weight,
        expand_bias,
        shrink_weight,
        shrink_bias,
    )
    attention_full = (
        lax.all_gather(attention_gain, "fsdp", axis=0, tiled=True),
        lax.all_gather(attention_shift, "fsdp", axis=0, tiled=True),
        lax.all_gather(joined_weight, "fsdp", axis=0, tiled=True),
        lax.all_gather(joined_bias, "fsdp", axis=0, tiled=True),
        lax.all_gather(output_weight, "fsdp", axis=0, tiled=True),
        lax.all_gather(output_bias, "fsdp", axis=0, tiled=True),
    )
    feedforward_full = (
        lax.all_gather(feedforward_gain, "fsdp", axis=0, tiled=True),
        lax.all_gather(feedforward_shift, "fsdp", axis=0, tiled=True),
        lax.all_gather(expand_weight, "fsdp", axis=0, tiled=True),
        lax.all_gather(expand_bias, "fsdp", axis=0, tiled=True),
        lax.all_gather(shrink_weight, "fsdp", axis=0, tiled=True),
        lax.all_gather(shrink_bias, "fsdp", axis=0, tiled=True),
    )
    normed_one, normalized_one, inverse_one, queries, keys, values = attention_inputs(
        rows, attention_full, cosine, sine
    )
    scores = score_block(queries, keys, allowed)
    top = jnp.max(scores, -1, keepdims=True)
    expo = jnp.exp(scores - top)
    total = jnp.sum(expo, -1, keepdims=True)
    log_total = top + jnp.log(total)
    probs_low = (expo / total).astype(jnp.bfloat16)
    mixed = jnp.einsum("hts,shd->thd", probs_low, values, preferred_element_type=jnp.float32)
    mixed = mixed.reshape(length, D).astype(jnp.bfloat16)
    attended = jnp.dot(
        mixed, attention_full[4], preferred_element_type=jnp.float32
    ) + attention_full[5].astype(jnp.float32)
    normed_two, normalized_two, inverse_two, expanded = feedforward_inputs(rows, feedforward_full)
    activated = jax.nn.gelu(expanded, approximate=False).astype(jnp.bfloat16)
    shrunk = jnp.dot(
        activated, feedforward_full[4], preferred_element_type=jnp.float32
    ) + feedforward_full[5].astype(jnp.float32)
    layer_output = (rows + live_rows * (attended + shrunk)).astype(jnp.bfloat16)
    seed_rows = cotangent.astype(jnp.float32)
    branch_grad = (live_rows * seed_rows).astype(jnp.bfloat16)
    branch_total = jnp.sum(branch_grad.astype(jnp.float32), 0)
    feedforward_back = lax.all_gather(
        as_sent(lax.optimization_barrier((feedforward_parts, layer_output))[0]),
        "fsdp",
        axis=0,
        tiled=True,
    )
    normed_two, normalized_two, inverse_two, expanded = feedforward_inputs(rows, feedforward_back)
    activated = jax.nn.gelu(expanded, approximate=False).astype(jnp.bfloat16)
    shrink_weight_grad = jnp.einsum(
        "tf,td->fd", activated, branch_grad, preferred_element_type=jnp.float32
    )
    activated_grad = jnp.einsum(
        "td,fd->tf", branch_grad, feedforward_back[4], preferred_element_type=jnp.float32
    )
    expanded_grad = (activated_grad * gelu_slope(expanded)).astype(jnp.bfloat16)
    expand_bias_grad = jnp.sum(expanded_grad.astype(jnp.float32), 0)
    expand_weight_grad = jnp.einsum(
        "td,tf->df", normed_two, expanded_grad, preferred_element_type=jnp.float32
    )
    normed_two_grad = jnp.einsum(
        "tf,df->td", expanded_grad, feedforward_back[2], preferred_element_type=jnp.float32
    )
    rows_grad_two, ff_gain_grad, ff_shift_grad = norm_back(
        normed_two_grad, normalized_two, inverse_two, feedforward_back[0]
    )
    ff_terms = (
        ff_gain_grad,
        ff_shift_grad,
        expand_weight_grad,
        expand_bias_grad,
        shrink_weight_grad,
        branch_total,
    )
    ff_parts = (
        lax.psum_scatter(ff_terms[0], "fsdp", scatter_dimension=0, tiled=True),
        lax.psum_scatter(ff_terms[1], "fsdp", scatter_dimension=0, tiled=True),
        lax.psum_scatter(ff_terms[2], "fsdp", scatter_dimension=0, tiled=True),
        lax.psum_scatter(ff_terms[3], "fsdp", scatter_dimension=0, tiled=True),
        lax.psum_scatter(ff_terms[4], "fsdp", scatter_dimension=0, tiled=True),
        lax.psum_scatter(ff_terms[5], "fsdp", scatter_dimension=0, tiled=True),
    )
    attention_back = lax.all_gather(
        as_sent(lax.optimization_barrier((attention_parts, layer_output))[0]),
        "fsdp",
        axis=0,
        tiled=True,
    )
    normed_one, normalized_one, inverse_one, queries, keys, values = attention_inputs(
        rows, attention_back, cosine, sine
    )
    scores = score_block(queries, keys, allowed)
    probs = jnp.exp(scores - log_total)
    probs_low = probs.astype(jnp.bfloat16)
    mixed = jnp.einsum("hts,shd->thd", probs_low, values, preferred_element_type=jnp.float32)
    mixed = mixed.reshape(length, D).astype(jnp.bfloat16)
    output_weight_grad = jnp.einsum(
        "td,te->de", mixed, branch_grad, preferred_element_type=jnp.float32
    )
    mixed_grad = jnp.einsum(
        "te,de->td", branch_grad, attention_back[4], preferred_element_type=jnp.float32
    )
    mixed_grad = mixed_grad.astype(jnp.bfloat16).reshape(length, HEADS, HEAD_DIM)
    value_grad = jnp.einsum(
        "hts,thd->shd", probs_low, mixed_grad, preferred_element_type=jnp.float32
    )
    probs_grad = jnp.einsum("thd,shd->hts", mixed_grad, values, preferred_element_type=jnp.float32)
    scores_grad = (probs * (probs_grad - jnp.sum(probs_grad * probs, -1, keepdims=True))).astype(
        jnp.bfloat16
    )
    query_grad = jnp.einsum(
        "hts,shd->thd", scores_grad, keys, preferred_element_type=jnp.float32
    ) * HEAD_DIM ** (-0.5)
    key_grad = jnp.einsum(
        "hts,thd->shd", scores_grad, queries, preferred_element_type=jnp.float32
    ) * HEAD_DIM ** (-0.5)
    query_grad = turn(query_grad, cosine, sine, -1.0)
    key_grad = turn(key_grad, cosine, sine, -1.0)
    joined_grad = jnp.concatenate(
        [query_grad.reshape(length, D), key_grad.reshape(length, D), value_grad.reshape(length, D)],
        1,
    ).astype(jnp.bfloat16)
    joined_bias_grad = jnp.sum(joined_grad.astype(jnp.float32), 0)
    joined_weight_grad = jnp.einsum(
        "td,te->de", normed_one, joined_grad, preferred_element_type=jnp.float32
    )
    normed_one_grad = jnp.einsum(
        "te,de->td", joined_grad, attention_back[2], preferred_element_type=jnp.float32
    )
    rows_grad_one, at_gain_grad, at_shift_grad = norm_back(
        normed_one_grad, normalized_one, inverse_one, attention_back[0]
    )
    at_terms = (
        at_gain_grad,
        at_shift_grad,
        joined_weight_grad,
        joined_bias_grad,
        output_weight_grad,
        branch_total,
    )
    at_parts = (
        lax.psum_scatter(at_terms[0], "fsdp", scatter_dimension=0, tiled=True),
        lax.psum_scatter(at_terms[1], "fsdp", scatter_dimension=0, tiled=True),
        lax.psum_scatter(at_terms[2], "fsdp", scatter_dimension=0, tiled=True),
        lax.psum_scatter(at_terms[3], "fsdp", scatter_dimension=0, tiled=True),
        lax.psum_scatter(at_terms[4], "fsdp", scatter_dimension=0, tiled=True),
        lax.psum_scatter(at_terms[5], "fsdp", scatter_dimension=0, tiled=True),
    )
    input_grad = (seed_rows + rows_grad_one + rows_grad_two).astype(jnp.bfloat16)
    summed = (
        lax.psum(at_parts[0].astype(jnp.bfloat16), "rep").astype(jnp.float32),
        lax.psum(at_parts[1].astype(jnp.bfloat16), "rep").astype(jnp.float32),
        lax.psum(at_parts[2].astype(jnp.bfloat16), "rep").astype(jnp.float32),
        lax.psum(at_parts[3].astype(jnp.bfloat16), "rep").astype(jnp.float32),
        lax.psum(at_parts[4].astype(jnp.bfloat16), "rep").astype(jnp.float32),
        lax.psum(at_parts[5].astype(jnp.bfloat16), "rep").astype(jnp.float32),
        lax.psum(ff_parts[0].astype(jnp.bfloat16), "rep").astype(jnp.float32),
        lax.psum(ff_parts[1].astype(jnp.bfloat16), "rep").astype(jnp.float32),
        lax.psum(ff_parts[2].astype(jnp.bfloat16), "rep").astype(jnp.float32),
        lax.psum(ff_parts[3].astype(jnp.bfloat16), "rep").astype(jnp.float32),
        lax.psum(ff_parts[4].astype(jnp.bfloat16), "rep").astype(jnp.float32),
        lax.psum(ff_parts[5].astype(jnp.bfloat16), "rep").astype(jnp.float32),
    )
    return (
        layer_output,
        input_grad,
        summed[0],
        summed[1],
        summed[2],
        summed[3],
        summed[4],
        summed[5],
        summed[6],
        summed[7],
        summed[8],
        summed[9],
        summed[10],
        summed[11],
    )


def wide(a):
    return a.astype(jnp.float32)


def normalize(rows):
    centre = jnp.mean(rows, -1, keepdims=True)
    centred = rows - centre
    inverse = lax.rsqrt(jnp.mean(centred * centred, -1, keepdims=True) + epsilon)
    return (centred * inverse, inverse)


def head_body(
    n,
    layer_input,
    segment,
    live_mask,
    attention_gain,
    attention_shift,
    joined_weight,
    joined_bias,
    output_weight,
    output_bias,
    feedforward_gain,
    feedforward_shift,
    expand_weight,
    expand_bias,
    shrink_weight,
    shrink_bias,
    cotangent,
):
    me = lax.axis_index("fsdp")
    own = layer_input.shape[0]
    width = layer_input.shape[1]
    part = width // n
    third = joined_bias.shape[0]
    piece = expand_weight.shape[1] // n
    heads = HEADS // n
    cols = heads * HEAD_DIM
    tokens = own * n
    low = jnp.bfloat16
    live_rows = wide(live_mask[0])[:, None]
    seeds = wide(cotangent)
    branch_own = (live_rows * seeds).astype(low)
    small = jnp.concatenate(
        [
            attention_gain,
            attention_shift,
            feedforward_gain,
            feedforward_shift,
            output_bias,
            shrink_bias,
            joined_bias,
            segment[0].astype(low),
        ]
    )
    small = jnp.pad(small, (0, -small.shape[0] % width)).reshape(-1, width)
    extra = small.shape[0]
    rows_all = lax.all_gather(jnp.concatenate([layer_input, small], 0), "fsdp", axis=0)
    small_all = rows_all[:, own:].reshape(n, extra * width)
    rows = wide(rows_all[:, :own]).reshape(tokens, width)
    branch = lax.all_gather(branch_own, "fsdp", axis=0, tiled=True)
    gain_one, shift_one, gain_two, shift_two, bias_o, bias_s = (
        wide(small_all[:, k * part : (k + 1) * part]).reshape(width) for k in range(6)
    )
    bias_j = wide(small_all[:, 6 * part : 6 * part + third]).reshape(3, n, cols)
    bias_j = lax.dynamic_index_in_dim(bias_j, me, 1, keepdims=False).reshape(3 * cols)
    seg_all = small_all[:, 6 * part + third : 6 * part + third + own]

    sent = jnp.concatenate(
        [
            joined_weight.reshape(part, 3, n, cols).transpose(2, 0, 1, 3).reshape(n, part, 3 * cols),
            expand_weight.reshape(part, n, piece).transpose(1, 0, 2),
        ],
        2,
    )
    held = lax.all_to_all(sent, "fsdp", 0, 0).reshape(width, 3 * cols + piece)
    weight_j, weight_e = (held[:, : 3 * cols], held[:, 3 * cols :])
    weight_os = jnp.concatenate([output_weight, shrink_weight], 0)

    normalized, inverse = normalize(rows)
    normed_one = (normalized * gain_one + shift_one).astype(low)
    normed_two = (normalized * gain_two + shift_two).astype(low)
    joined = jnp.dot(normed_one, weight_j, preferred_element_type=jnp.float32) + bias_j
    seg_int = seg_all.astype(jnp.int32)
    cosine, sine = rotary_tables(seg_int)
    places = jnp.arange(own, dtype=jnp.int32)
    allowed = (seg_int[:, :, None] == seg_int[:, None, :]) & (
        places[None, None, :] <= places[None, :, None]
    )
    split = joined.reshape(n, own, 3, heads, HEAD_DIM)
    queries = turn(split[:, :, 0], cosine, sine, 1.0).astype(low)
    keys = turn(split[:, :, 1], cosine, sine, 1.0).astype(low)
    values = split[:, :, 2].astype(low)
    scale = HEAD_DIM ** (-0.5)
    scores = (
        jnp.einsum("bthd,bshd->bhts", queries, keys, preferred_element_type=jnp.float32) * scale
    )
    scores = jnp.where(allowed[:, None], scores, masked_score)
    top = jnp.max(scores, -1, keepdims=True)
    expo = jnp.exp(scores - top)
    probs = expo / jnp.sum(expo, -1, keepdims=True)
    probs_low = probs.astype(low)
    mixed = jnp.einsum("bhts,bshd->bthd", probs_low, values, preferred_element_type=jnp.float32)
    mixed = mixed.reshape(tokens, cols).astype(low)
    expanded = jnp.dot(normed_two, weight_e, preferred_element_type=jnp.float32) + wide(expand_bias)
    activated = jax.nn.gelu(expanded, approximate=False).astype(low)
    slope = gelu_slope(expanded)
    inner = jnp.concatenate([mixed, activated], 1)
    partial = jnp.dot(inner, weight_os, preferred_element_type=jnp.float32).astype(low)
    summed = lax.psum_scatter(partial, "fsdp", scatter_dimension=0, tiled=True)
    layer_output = (
        wide(layer_input) + live_rows * (wide(summed) + (bias_o + bias_s))
    ).astype(low)

    grad_os = jnp.einsum("tf,td->fd", inner, branch, preferred_element_type=jnp.float32)
    inner_grad = jnp.einsum("td,fd->tf", branch, weight_os, preferred_element_type=jnp.float32)
    expanded_grad = (inner_grad[:, cols:] * slope).astype(low)
    mixed_grad = inner_grad[:, :cols].astype(low).reshape(n, own, heads, HEAD_DIM)
    value_grad = jnp.einsum(
        "bhts,bthd->bshd", probs_low, mixed_grad, preferred_element_type=jnp.float32
    )
    probs_grad = jnp.einsum(
        "bthd,bshd->bhts", mixed_grad, values, preferred_element_type=jnp.float32
    )
    scores_grad = (probs * (probs_grad - jnp.sum(probs_grad * probs, -1, keepdims=True))).astype(low)
    query_grad = (
        jnp.einsum("bhts,bshd->bthd", scores_grad, keys, preferred_element_type=jnp.float32) * scale
    )
    key_grad = (
        jnp.einsum("bhts,bthd->bshd", scores_grad, queries, preferred_element_type=jnp.float32)
        * scale
    )
    query_grad = turn(query_grad, cosine, sine, -1.0)
    key_grad = turn(key_grad, cosine, sine, -1.0)
    joined_grad = jnp.concatenate(
        [a.reshape(tokens, cols) for a in (query_grad, key_grad, value_grad)], 1
    ).astype(low)
    grad_j = jnp.einsum("td,te->de", normed_one, joined_grad, preferred_element_type=jnp.float32)
    grad_e = jnp.einsum("td,tf->df", normed_two, expanded_grad, preferred_element_type=jnp.float32)
    back_one = jnp.einsum("te,de->td", joined_grad, weight_j, preferred_element_type=jnp.float32)
    back_two = jnp.einsum("tf,df->td", expanded_grad, weight_e, preferred_element_type=jnp.float32)
    hat = (back_one * gain_one + back_two * gain_two).astype(low)
    hat_own = wide(lax.psum_scatter(hat, "fsdp", scatter_dimension=0, tiled=True))
    rows_own = wide(layer_input)
    normalized_own, inverse_own = normalize(rows_own)
    row_grad = inverse_own * (
        hat_own
        - jnp.mean(hat_own, -1, keepdims=True)
        - normalized_own * jnp.mean(hat_own * normalized_own, -1, keepdims=True)
    )
    input_grad = (seeds + row_grad).astype(low)

    grads = jnp.concatenate([grad_j, grad_e], 1).astype(low).reshape(n, part, 3 * cols + piece)
    grads = lax.all_to_all(grads, "fsdp", 0, 0)
    joined_weight_grad = (
        grads[:, :, : 3 * cols].reshape(n, part, 3, cols).transpose(1, 2, 0, 3).reshape(part, 3 * width)
    )
    expand_weight_grad = grads[:, :, 3 * cols :].transpose(1, 0, 2).reshape(part, n * piece)

    vectors = jnp.stack(
        [
            jnp.sum(back_one * normalized, 0),
            jnp.sum(back_one, 0),
            jnp.sum(back_two * normalized, 0),
            jnp.sum(back_two, 0),
        ]
    )
    bias_j_grad = jnp.sum(wide(joined_grad), 0).reshape(3, 1, cols)
    bias_j_grad = jnp.where(
        lax.broadcasted_iota(jnp.int32, (3, n, cols), 1) == me, bias_j_grad, 0.0
    ).reshape(-1)
    branch_sum = jnp.sum(wide(branch_own), 0)
    small_sums = lax.psum(
        jnp.concatenate([vectors.reshape(-1), branch_sum, bias_j_grad]), ("rep", "fsdp")
    )
    pieces = small_sums[: 5 * width].reshape(5, n, part)
    pieces = lax.dynamic_index_in_dim(pieces, me, 1, keepdims=False)
    joined_bias_grad = lax.dynamic_slice(small_sums, (5 * width + me * third,), (third,))
    expand_bias_grad = jnp.sum(wide(expanded_grad), 0)
    rest = lax.psum(
        (
            joined_weight_grad,
            expand_weight_grad,
            grad_os[:cols].astype(low),
            grad_os[cols:].astype(low),
            expand_bias_grad.astype(low),
        ),
        "rep",
    )
    rest = tuple(wide(a) for a in rest)
    return (
        layer_output,
        input_grad,
        pieces[0],
        pieces[1],
        rest[0],
        joined_bias_grad,
        rest[2],
        pieces[4],
        pieces[2],
        pieces[3],
        rest[1],
        rest[4],
        rest[3],
        pieces[4],
    )


def solution(mesh):
    n = mesh.shape["fsdp"]
    chosen = functools.partial(head_body, n) if HEADS % n == 0 else body
    placed = (
        P(("rep", "fsdp"), None),
        P(("rep", "fsdp"), None),
        P(("rep", "fsdp"), None),
        P("fsdp"),
        P("fsdp"),
        P("fsdp", None),
        P("fsdp"),
        P("fsdp", None),
        P("fsdp"),
        P("fsdp"),
        P("fsdp"),
        P("fsdp", None),
        P("fsdp"),
        P("fsdp", None),
        P("fsdp"),
        P(("rep", "fsdp"), None),
    )
    return jax.shard_map(
        chosen,
        mesh=mesh,
        in_specs=placed,
        out_specs=(
            P(("rep", "fsdp"), None),
            P(("rep", "fsdp"), None),
            P("fsdp"),
            P("fsdp"),
            P("fsdp", None),
            P("fsdp"),
            P("fsdp", None),
            P("fsdp"),
            P("fsdp"),
            P("fsdp"),
            P("fsdp", None),
            P("fsdp"),
            P("fsdp", None),
            P("fsdp"),
        ),
        check_vma=False,
    )
```

```python
import functools

import jax
import jax.numpy as jnp
from jax import lax
from jax.experimental import pallas as pl
from jax.experimental.pallas import tpu as pltpu
from jax.sharding import PartitionSpec as P

D = 2048
HEADS = 16
HEAD_DIM = 128
ROT = 32


epsilon = 1e-05
masked_score = -1e30
rotary_base = 10000.0


def as_sent(shard):
    return jax.tree.map(lambda a: a.astype(jnp.bfloat16) if a.dtype == jnp.float32 else a, shard)


def norm_rows(rows, gain, shift):
    centre = jnp.mean(rows, -1, keepdims=True)
    centred = rows - centre
    inverse = lax.rsqrt(jnp.mean(centred * centred, -1, keepdims=True) + epsilon)
    normalized = centred * inverse
    return (normalized * gain.astype(jnp.float32) + shift.astype(jnp.float32), normalized, inverse)


def norm_back(normed_grad, normalized, inverse, gain):
    scaled = normed_grad * gain.astype(jnp.float32)
    row_grad = inverse * (
        scaled
        - jnp.mean(scaled, -1, keepdims=True)
        - normalized * jnp.mean(scaled * normalized, -1, keepdims=True)
    )
    return (row_grad, jnp.sum(normed_grad * normalized, 0), jnp.sum(normed_grad, 0))


def rotary_tables(segment):
    length = segment.shape[-1]
    places = jnp.arange(length, dtype=jnp.int32)
    earlier = jnp.sum((segment[..., None, :] < segment[..., :, None]).astype(jnp.int32), -1)
    position = (places - earlier).astype(jnp.float32)
    exponent = jnp.arange(ROT // 2, dtype=jnp.float32) * 2.0 / ROT
    frequency = jnp.power(jnp.float32(rotary_base), -exponent)
    angle = position[..., None] * frequency
    return (jnp.cos(angle), jnp.sin(angle))


def turn(heads, cosine, sine, sign):
    half = ROT // 2
    front = heads[..., :half]
    behind = heads[..., half:ROT]
    cos_wide = cosine[..., None, :]
    sin_wide = sine[..., None, :] * sign
    return jnp.concatenate(
        [
            front * cos_wide - behind * sin_wide,
            behind * cos_wide + front * sin_wide,
            heads[..., ROT:],
        ],
        -1,
    )


def gelu_slope(values):
    return (
        0.5 * (1.0 + lax.erf(values * 0.7071067811865476))
        + values * jnp.exp(-0.5 * values * values) * 0.3989422804014327
    )


def attention_inputs(rows, weights, cosine, sine):
    gain, shift, joined_weight, joined_bias = (weights[0], weights[1], weights[2], weights[3])
    normed, normalized, inverse = norm_rows(rows, gain, shift)
    normed_low = normed.astype(jnp.bfloat16)
    joined = jnp.dot(
        normed_low, joined_weight, preferred_element_type=jnp.float32
    ) + joined_bias.astype(jnp.float32)
    length = rows.shape[0]
    split = joined.reshape(length, 3, HEADS, HEAD_DIM)
    queries = turn(split[:, 0], cosine, sine, 1.0).astype(jnp.bfloat16)
    keys = turn(split[:, 1], cosine, sine, 1.0).astype(jnp.bfloat16)
    values = split[:, 2].astype(jnp.bfloat16)
    return (normed_low, normalized, inverse, queries, keys, values)


def score_block(queries, keys, allowed):
    scores = jnp.einsum(
        "thd,shd->hts", queries, keys, preferred_element_type=jnp.float32
    ) * HEAD_DIM ** (-0.5)
    return jnp.where(allowed[None], scores, masked_score)


def feedforward_inputs(rows, weights):
    gain, shift, expand_weight, expand_bias = (weights[0], weights[1], weights[2], weights[3])
    normed, normalized, inverse = norm_rows(rows, gain, shift)
    normed_low = normed.astype(jnp.bfloat16)
    expanded = jnp.dot(
        normed_low, expand_weight, preferred_element_type=jnp.float32
    ) + expand_bias.astype(jnp.float32)
    return (normed_low, normalized, inverse, expanded)


def body(
    layer_input,
    segment,
    live_mask,
    attention_gain,
    attention_shift,
    joined_weight,
    joined_bias,
    output_weight,
    output_bias,
    feedforward_gain,
    feedforward_shift,
    expand_weight,
    expand_bias,
    shrink_weight,
    shrink_bias,
    cotangent,
):
    rows = layer_input.astype(jnp.float32)
    seg_row = segment[0]
    live_rows = live_mask[0].astype(jnp.float32)[:, None]
    length = seg_row.shape[0]
    cosine, sine = rotary_tables(seg_row)
    places = jnp.arange(length, dtype=jnp.int32)
    allowed = (seg_row[:, None] == seg_row[None, :]) & (places[None, :] <= places[:, None])
    attention_parts = (
        attention_gain,
        attention_shift,
        joined_weight,
        joined_bias,
        output_weight,
        output_bias,
    )
    feedforward_parts = (
        feedforward_gain,
        feedforward_shift,
        expand_weight,
        expand_bias,
        shrink_weight,
        shrink_bias,
    )
    attention_full = (
        lax.all_gather(attention_gain, "fsdp", axis=0, tiled=True),
        lax.all_gather(attention_shift, "fsdp", axis=0, tiled=True),
        lax.all_gather(joined_weight, "fsdp", axis=0, tiled=True),
        lax.all_gather(joined_bias, "fsdp", axis=0, tiled=True),
        lax.all_gather(output_weight, "fsdp", axis=0, tiled=True),
        lax.all_gather(output_bias, "fsdp", axis=0, tiled=True),
    )
    feedforward_full = (
        lax.all_gather(feedforward_gain, "fsdp", axis=0, tiled=True),
        lax.all_gather(feedforward_shift, "fsdp", axis=0, tiled=True),
        lax.all_gather(expand_weight, "fsdp", axis=0, tiled=True),
        lax.all_gather(expand_bias, "fsdp", axis=0, tiled=True),
        lax.all_gather(shrink_weight, "fsdp", axis=0, tiled=True),
        lax.all_gather(shrink_bias, "fsdp", axis=0, tiled=True),
    )
    normed_one, normalized_one, inverse_one, queries, keys, values = attention_inputs(
        rows, attention_full, cosine, sine
    )
    scores = score_block(queries, keys, allowed)
    top = jnp.max(scores, -1, keepdims=True)
    expo = jnp.exp(scores - top)
    total = jnp.sum(expo, -1, keepdims=True)
    log_total = top + jnp.log(total)
    probs_low = (expo / total).astype(jnp.bfloat16)
    mixed = jnp.einsum("hts,shd->thd", probs_low, values, preferred_element_type=jnp.float32)
    mixed = mixed.reshape(length, D).astype(jnp.bfloat16)
    attended = jnp.dot(
        mixed, attention_full[4], preferred_element_type=jnp.float32
    ) + attention_full[5].astype(jnp.float32)
    normed_two, normalized_two, inverse_two, expanded = feedforward_inputs(rows, feedforward_full)
    activated = jax.nn.gelu(expanded, approximate=False).astype(jnp.bfloat16)
    shrunk = jnp.dot(
        activated, feedforward_full[4], preferred_element_type=jnp.float32
    ) + feedforward_full[5].astype(jnp.float32)
    layer_output = (rows + live_rows * (attended + shrunk)).astype(jnp.bfloat16)
    seed_rows = cotangent.astype(jnp.float32)
    branch_grad = (live_rows * seed_rows).astype(jnp.bfloat16)
    branch_total = jnp.sum(branch_grad.astype(jnp.float32), 0)
    feedforward_back = lax.all_gather(
        as_sent(lax.optimization_barrier((feedforward_parts, layer_output))[0]),
        "fsdp",
        axis=0,
        tiled=True,
    )
    normed_two, normalized_two, inverse_two, expanded = feedforward_inputs(rows, feedforward_back)
    activated = jax.nn.gelu(expanded, approximate=False).astype(jnp.bfloat16)
    shrink_weight_grad = jnp.einsum(
        "tf,td->fd", activated, branch_grad, preferred_element_type=jnp.float32
    )
    activated_grad = jnp.einsum(
        "td,fd->tf", branch_grad, feedforward_back[4], preferred_element_type=jnp.float32
    )
    expanded_grad = (activated_grad * gelu_slope(expanded)).astype(jnp.bfloat16)
    expand_bias_grad = jnp.sum(expanded_grad.astype(jnp.float32), 0)
    expand_weight_grad = jnp.einsum(
        "td,tf->df", normed_two, expanded_grad, preferred_element_type=jnp.float32
    )
    normed_two_grad = jnp.einsum(
        "tf,df->td", expanded_grad, feedforward_back[2], preferred_element_type=jnp.float32
    )
    rows_grad_two, ff_gain_grad, ff_shift_grad = norm_back(
        normed_two_grad, normalized_two, inverse_two, feedforward_back[0]
    )
    ff_terms = (
        ff_gain_grad,
        ff_shift_grad,
        expand_weight_grad,
        expand_bias_grad,
        shrink_weight_grad,
        branch_total,
    )
    ff_parts = (
        lax.psum_scatter(ff_terms[0], "fsdp", scatter_dimension=0, tiled=True),
        lax.psum_scatter(ff_terms[1], "fsdp", scatter_dimension=0, tiled=True),
        lax.psum_scatter(ff_terms[2], "fsdp", scatter_dimension=0, tiled=True),
        lax.psum_scatter(ff_terms[3], "fsdp", scatter_dimension=0, tiled=True),
        lax.psum_scatter(ff_terms[4], "fsdp", scatter_dimension=0, tiled=True),
        lax.psum_scatter(ff_terms[5], "fsdp", scatter_dimension=0, tiled=True),
    )
    attention_back = lax.all_gather(
        as_sent(lax.optimization_barrier((attention_parts, layer_output))[0]),
        "fsdp",
        axis=0,
        tiled=True,
    )
    normed_one, normalized_one, inverse_one, queries, keys, values = attention_inputs(
        rows, attention_back, cosine, sine
    )
    scores = score_block(queries, keys, allowed)
    probs = jnp.exp(scores - log_total)
    probs_low = probs.astype(jnp.bfloat16)
    mixed = jnp.einsum("hts,shd->thd", probs_low, values, preferred_element_type=jnp.float32)
    mixed = mixed.reshape(length, D).astype(jnp.bfloat16)
    output_weight_grad = jnp.einsum(
        "td,te->de", mixed, branch_grad, preferred_element_type=jnp.float32
    )
    mixed_grad = jnp.einsum(
        "te,de->td", branch_grad, attention_back[4], preferred_element_type=jnp.float32
    )
    mixed_grad = mixed_grad.astype(jnp.bfloat16).reshape(length, HEADS, HEAD_DIM)
    value_grad = jnp.einsum(
        "hts,thd->shd", probs_low, mixed_grad, preferred_element_type=jnp.float32
    )
    probs_grad = jnp.einsum("thd,shd->hts", mixed_grad, values, preferred_element_type=jnp.float32)
    scores_grad = (probs * (probs_grad - jnp.sum(probs_grad * probs, -1, keepdims=True))).astype(
        jnp.bfloat16
    )
    query_grad = jnp.einsum(
        "hts,shd->thd", scores_grad, keys, preferred_element_type=jnp.float32
    ) * HEAD_DIM ** (-0.5)
    key_grad = jnp.einsum(
        "hts,thd->shd", scores_grad, queries, preferred_element_type=jnp.float32
    ) * HEAD_DIM ** (-0.5)
    query_grad = turn(query_grad, cosine, sine, -1.0)
    key_grad = turn(key_grad, cosine, sine, -1.0)
    joined_grad = jnp.concatenate(
        [query_grad.reshape(length, D), key_grad.reshape(length, D), value_grad.reshape(length, D)],
        1,
    ).astype(jnp.bfloat16)
    joined_bias_grad = jnp.sum(joined_grad.astype(jnp.float32), 0)
    joined_weight_grad = jnp.einsum(
        "td,te->de", normed_one, joined_grad, preferred_element_type=jnp.float32
    )
    normed_one_grad = jnp.einsum(
        "te,de->td", joined_grad, attention_back[2], preferred_element_type=jnp.float32
    )
    rows_grad_one, at_gain_grad, at_shift_grad = norm_back(
        normed_one_grad, normalized_one, inverse_one, attention_back[0]
    )
    at_terms = (
        at_gain_grad,
        at_shift_grad,
        joined_weight_grad,
        joined_bias_grad,
        output_weight_grad,
        branch_total,
    )
    at_parts = (
        lax.psum_scatter(at_terms[0], "fsdp", scatter_dimension=0, tiled=True),
        lax.psum_scatter(at_terms[1], "fsdp", scatter_dimension=0, tiled=True),
        lax.psum_scatter(at_terms[2], "fsdp", scatter_dimension=0, tiled=True),
        lax.psum_scatter(at_terms[3], "fsdp", scatter_dimension=0, tiled=True),
        lax.psum_scatter(at_terms[4], "fsdp", scatter_dimension=0, tiled=True),
        lax.psum_scatter(at_terms[5], "fsdp", scatter_dimension=0, tiled=True),
    )
    input_grad = (seed_rows + rows_grad_one + rows_grad_two).astype(jnp.bfloat16)
    summed = (
        lax.psum(at_parts[0].astype(jnp.bfloat16), "rep").astype(jnp.float32),
        lax.psum(at_parts[1].astype(jnp.bfloat16), "rep").astype(jnp.float32),
        lax.psum(at_parts[2].astype(jnp.bfloat16), "rep").astype(jnp.float32),
        lax.psum(at_parts[3].astype(jnp.bfloat16), "rep").astype(jnp.float32),
        lax.psum(at_parts[4].astype(jnp.bfloat16), "rep").astype(jnp.float32),
        lax.psum(at_parts[5].astype(jnp.bfloat16), "rep").astype(jnp.float32),
        lax.psum(ff_parts[0].astype(jnp.bfloat16), "rep").astype(jnp.float32),
        lax.psum(ff_parts[1].astype(jnp.bfloat16), "rep").astype(jnp.float32),
        lax.psum(ff_parts[2].astype(jnp.bfloat16), "rep").astype(jnp.float32),
        lax.psum(ff_parts[3].astype(jnp.bfloat16), "rep").astype(jnp.float32),
        lax.psum(ff_parts[4].astype(jnp.bfloat16), "rep").astype(jnp.float32),
        lax.psum(ff_parts[5].astype(jnp.bfloat16), "rep").astype(jnp.float32),
    )
    return (
        layer_output,
        input_grad,
        summed[0],
        summed[1],
        summed[2],
        summed[3],
        summed[4],
        summed[5],
        summed[6],
        summed[7],
        summed[8],
        summed[9],
        summed[10],
        summed[11],
    )


MESH = pl.DeviceIdType.MESH
bf = jnp.bfloat16
f32 = jnp.float32


def gather_kernel(x_ref, bg_ref, sm_ref, jw_ref, ew_ref, X, BG, SM, WJ, WE,
       tmp, su, sd, sy, ss, rx, bu, bd, by, bs, rb, sw, rw, sxw, rxw, lsem, ssm, rsm):
    r = lax.axis_index("rep"); f = lax.axis_index("fsdp")
    z = f // 4; y = (f // 2) % 2; c = f % 2
    sib = z * 4 + y * 2 + (1 - c)
    yp = z * 4 + (1 - y) * 2 + c
    barrier = pltpu.get_barrier_semaphore()
    @pl.loop(1, 16)
    def _(k):
        pl.semaphore_signal(barrier, inc=1, device_id=(r, (f + k) % 16), device_id_type=MESH)
    pl.semaphore_signal(barrier, inc=1, device_id=(1 - r, f), device_id_type=MESH)
    pl.semaphore_wait(barrier, 16)

    def rc(src, dst, s, q, dev):
        return pltpu.make_async_remote_copy(src_ref=src, dst_ref=dst, send_sem=s, recv_sem=q, device_id=dev, device_id_type=MESH)

    def gather(own, OUT, su, sd, sy, ss, rr):
        def item(i):
            return OUT.at[i]
        def up(i, src=None):
            return rc(item(i) if src is None else src, item(i), su.at[i], rr.at[i], (r, f + 4))
        def dn(i, src=None):
            return rc(item(i) if src is None else src, item(i), sd.at[i], rr.at[i], (r, f - 4))
        def ac(i, src=None):
            return rc(item(i) if src is None else src, item(i), sy.at[i], rr.at[i], (r, yp))
        def sb(i, src=None):
            return rc(item(i) if src is None else src, item(i), ss.at[i], rr.at[i], (r, sib))
        def begin():
            pl.when(z < 3)(lambda: up(f, own).start())
            pl.when(z > 0)(lambda: dn(f, own).start())
            ac(f, own).start()
            sb(f, own).start()
        def step(s):
            @pl.when(z - s >= 0)
            def _():
                i = f - 4 * s
                up(i).wait_recv()
                pl.when(z < 3)(lambda: up(i).start())
                ac(i).start()
                sb(i).start()
            @pl.when(z + s <= 3)
            def _():
                i = f + 4 * s
                dn(i).wait_recv()
                pl.when(z > 0)(lambda: dn(i).start())
                ac(i).start()
                sb(i).start()
        def ystep(s):
            if s == 0:
                ac(yp).wait_recv(); sb(yp).start()
            else:
                @pl.when(z - s >= 0)
                def _():
                    i = yp - 4 * s
                    ac(i).wait_recv(); sb(i).start()
                @pl.when(z + s <= 3)
                def _():
                    i = yp + 4 * s
                    ac(i).wait_recv(); sb(i).start()
        def finish():
            @pl.loop(0, 8)
            def _(k):
                i = 2 * k + (1 - c)
                sb(i).wait_recv()
            @pl.loop(0, 8)
            def _(k):
                i = 2 * k + c
                sb(i).wait_send()
            @pl.loop(0, 4)
            def _(k):
                i = k * 4 + y * 2 + c
                ac(i).wait_send()
                pl.when((k <= z) & (z < 3))(lambda: up(i).wait_send())
                pl.when((k >= z) & (z > 0))(lambda: dn(i).wait_send())
        return begin, step, ystep, finish

    xb, xs, xy, xf = gather(x_ref, X, su, sd, sy, ss, rx)
    gb, gs, gy, gf = gather(bg_ref, BG, bu, bd, by, bs, rb)

    def wpieces(src_dev, dst_dev, src_is_arg):
        rows = pl.ds(pl.multiple_of(128 * src_dev + 64 * r, 64), 64)
        out = []
        for t in range(3):
            if src_is_arg:
                s = jw_ref.at[pl.ds(pl.multiple_of(64 * r, 64), 64), pl.ds(pl.multiple_of(2048 * t + 128 * dst_dev, 128), 128)]
            else:
                s = WJ.at[rows, pl.ds(128 * t, 128)]
            out.append((s, WJ.at[rows, pl.ds(128 * t, 128)]))
        if src_is_arg:
            s = ew_ref.at[pl.ds(pl.multiple_of(64 * r, 64), 64), pl.ds(pl.multiple_of(512 * dst_dev, 512), 512)]
        else:
            s = WE.at[rows]
        out.append((s, WE.at[rows]))
        return out

    a = pltpu.make_async_copy(x_ref, tmp.at[0], lsem.at[0]); a.start()
    b = pltpu.make_async_copy(bg_ref, tmp.at[1], lsem.at[1]); b.start()
    xb()
    @pl.loop(1, 16)
    def _(k):
        fd = (f + k) % 16
        rc(sm_ref, SM.at[f], ssm.at[fd], rsm.at[f], (r, fd)).start()
        for t, (s, d) in enumerate(wpieces(f, fd, True)):
            rc(s, d, sw.at[fd, t], rw.at[f, t], (r, fd)).start()
    for t, (s, d) in enumerate(wpieces(f, f, True)):
        rc(s, d, sxw.at[f, t], rxw.at[f, t], (1 - r, f)).start()
        pltpu.make_async_copy(s, d, rw.at[f, t]).start()
    own_small = pltpu.make_async_copy(sm_ref, SM.at[f], rsm.at[f])
    own_small.start()
    a.wait(); b.wait()
    a2 = pltpu.make_async_copy(tmp.at[0], X.at[f], lsem.at[0]); a2.start()
    b2 = pltpu.make_async_copy(tmp.at[1], BG.at[f], lsem.at[1]); b2.start()
    def fwd(lo, hi):
        @pl.loop(lo, hi)
        def _(k):
            fs = (f + 16 - k) % 16
            for t, (s, d) in enumerate(wpieces(fs, f, False)):
                rc(s, d, sw.at[fs, t], rw.at[fs, t], (r, f)).wait_recv()
                rc(s, d, sxw.at[fs, t], rxw.at[fs, t], (1 - r, f)).start()
    xs(1); xy(0); fwd(1, 5)
    xs(2); xy(1); fwd(5, 9)
    xs(3); xy(2); fwd(9, 13)
    gb()
    xy(3); fwd(13, 16)
    for t, (s, d) in enumerate(wpieces(f, f, True)):
        pltpu.make_async_copy(s, d, rw.at[f, t]).wait()
    xf()
    for s in (1, 2, 3):
        gs(s)
        gy(s - 1)
    gy(3)
    rows_of = lambda src: pl.ds(pl.multiple_of(128 * src + 64 * (1 - r), 64), 64)
    @pl.loop(0, 16)
    def _(fs):
        for t in range(4):
            d = WJ.at[rows_of(fs), pl.ds(128 * t, 128)] if t < 3 else WE.at[rows_of(fs)]
            q = rc(d, d, sxw.at[fs, t], rxw.at[fs, t], (1 - r, f))
            q.wait_recv()
            q.wait_send()
        @pl.when(fs != f)
        def _():
            for t, (s, d) in enumerate(wpieces(f, fs, True)):
                rc(s, d, sw.at[fs, t], rw.at[f, t], (r, fs)).wait_send()
    gf()
    own_small.wait()
    @pl.loop(1, 16)
    def _(k):
        fs = (f + k) % 16
        other = rc(sm_ref, SM.at[fs], ssm.at[fs], rsm.at[fs], (r, fs))
        other.wait_recv()
        other.wait_send()
    a2.wait(); b2.wait()

def gather_all(x, bg, sm, jw, ew):
    D = pltpu.SemaphoreType.DMA
    hbm = pl.BlockSpec(memory_space=pl.ANY)
    return pl.pallas_call(
        gather_kernel,
        out_shape=(jax.ShapeDtypeStruct((16, 128, 2048), bf), jax.ShapeDtypeStruct((16, 128, 2048), bf), jax.ShapeDtypeStruct((16, 16, 128), bf),
                   jax.ShapeDtypeStruct((2048, 384), bf), jax.ShapeDtypeStruct((2048, 512), bf)),
        in_specs=[hbm] * 5, out_specs=(hbm,) * 5,
        scratch_shapes=[pltpu.VMEM((2, 128, 2048), bf)] + [D((16,))] * 10 + [D((16, 4))] * 4 + [D((2,)), D((16,)), D((16,))],
        compiler_params=pltpu.CompilerParams(collective_id=0, has_side_effects=True, vmem_limit_bytes=60 << 20),
    )(x, bg, sm, jw, ew)


def reduce_kernel(P1, P2, OS, JE, SO1, SO2, OSo, JW, EW, L, A, B, CO, CI, HB, RX, LOS, ROS,
       sl, sa, ra, sb, rb, sc, rco, rci, sx, rx, so, ro, so2, ro2, sw, rw, sf, rf, lsem):
    r = lax.axis_index("rep"); f = lax.axis_index("fsdp")
    z = f // 4; y = (f // 2) % 2; c = f % 2
    sib = (r, z * 4 + y * 2 + (1 - c))
    yp = (r, z * 4 + (1 - y) * 2 + c)
    xp = (1 - r, f)
    lower = z <= 1
    zz = jnp.where(lower, z, 3 - z)
    def phys(q):
        return jnp.where(lower, q, 3 - q)
    f_in = (r, jnp.where(lower, f + 4, f - 4))
    f_out = (r, jnp.where(lower, f - 4, f + 4))
    barrier = pltpu.get_barrier_semaphore()
    @pl.loop(1, 16)
    def _(k):
        pl.semaphore_signal(barrier, inc=1, device_id=(r, (f + k) % 16), device_id_type=MESH)
    pl.semaphore_signal(barrier, inc=1, device_id=xp, device_id_type=MESH)
    pl.semaphore_wait(barrier, 16)

    def rc(src, dst, s, q, dev):
        return pltpu.make_async_remote_copy(src_ref=src, dst_ref=dst, send_sem=s, recv_sem=q, device_id=dev, device_id_type=MESH)
    def lc(src, dst, s):
        return pltpu.make_async_copy(src, dst, s)

    def add_into(dst, src, rows):
        @pl.loop(0, rows // 16)
        def _(i):
            w = pl.ds(pl.multiple_of(i * 16, 16), 16)
            dst[w] = (dst[w].astype(f32) + src[w].astype(f32)).astype(bf)

    def reducer(n, PP, SO):
        def a_send(k):
            return rc(PP.at[2 * k + 1 - c], A.at[n, k], sa.at[n, k], ra.at[n, k], sib)
        def a_load(k):
            return lc(PP.at[2 * k + c], L.at[n, k], sl.at[n, k])
        def b_send(zp):
            return rc(L.at[n, zp * 2 + 1 - y], B.at[n, zp], sb.at[n, zp], rb.at[n, zp], yp)
        def order():
            return (3, 0, 2, 1)
        def begin():
            for yy in (1 - y, y):
                for q in order():
                    k = phys(q) * 2 + yy
                    a_send(k).start()
                    a_load(k).start()
        def prep(k):
            a_load(k).wait()
            a_send(k).wait_recv()
            add_into(L.at[n, k], A.at[n, k], 128)
        def far():
            for q in order():
                prep(phys(q) * 2 + 1 - y)
                b_send(phys(q)).start()
        def near(q):
            zp = phys(q)
            k = zp * 2 + y
            prep(k)
            b_send(zp).wait_recv()
            add_into(L.at[n, k], B.at[n, zp], 128)
        def to_in(q):
            zp = phys(q)
            return zp, L.at[n, zp * 2 + y]
        def recv(buf, q, sem):
            zp = phys(q)
            rc(buf.at[n, zp], buf.at[n, zp], sc.at[n, zp], sem.at[n, zp], f_in).wait_recv()
            return buf.at[n, zp]
        def send(q, buf, sem, dev):
            zp = phys(q)
            return rc(L.at[n, zp * 2 + y], buf.at[n, zp], sc.at[n, zp], sem.at[n, zp], dev)
        def step(q):
            near(q)
            zp = phys(q)
            k = zp * 2 + y
            @pl.when(zz == 0)
            def _():
                if q > 0:
                    send(q, CO, rco, f_in).start()
            @pl.when(zz == 1)
            def _():
                if q >= 2:
                    add_into(L.at[n, k], recv(CO, q, rco), 128)
                    send(q, CI, rci, f_in).start()
                if q == 0:
                    add_into(L.at[n, k], recv(CI, q, rci), 128)
                    send(q, CI, rci, f_out).start()
        def last():
            def total(q, bufs):
                k = phys(q) * 2 + y
                @pl.loop(0, 8)
                def _(i):
                    w = pl.ds(pl.multiple_of(i * 16, 16), 16)
                    v = L[n, k, w].astype(f32)
                    for b in bufs:
                        v = v + b[w].astype(f32)
                    SO[w] = v
            @pl.when(zz == 0)
            def _():
                total(0, [recv(CI, 0, rci)])
            @pl.when(zz == 1)
            def _():
                total(1, [recv(CO, 1, rco), recv(CI, 1, rci)])
        def drain():
            @pl.loop(0, 8)
            def _(k):
                a_send(k).wait_send()
            @pl.loop(0, 4)
            def _(zp):
                b_send(zp).wait_send()
            for q in range(4):
                if q > 0:
                    pl.when(zz == 0)(lambda: send(q, CO, rco, f_in).wait_send())
                if q != 1:
                    pl.when(zz == 1)(lambda: send(q, CI, rci, f_in).wait_send())
        return begin, far, step, last, drain

    R1 = reducer(0, P1, SO1)
    R2 = reducer(1, P2, SO2)

    def x1(g):
        return rc(JE.at[pl.ds(4 * g, 4), 1 - r], RX.at[pl.ds(4 * g, 4)], sx.at[g], rx.at[g], xp)
    def hb_load():
        return lc(JE.at[:, r], HB, lsem.at[0])
    rr = pl.ds(pl.multiple_of(64 * r, 64), 64)
    def dst(fs, t):
        if t < 3:
            return JW.at[rr, pl.ds(pl.multiple_of(2048 * t + 128 * fs, 128), 128)]
        return EW.at[rr, pl.ds(pl.multiple_of(512 * fs, 512), 512)]
    def srcp(fd, t):
        return HB.at[fd, :, pl.ds(128 * t, 128)] if t < 3 else HB.at[fd, :, pl.ds(384, 512)]
    def dsto(fs, t):
        ro_ = pl.ds(pl.multiple_of(64 * (1 - r), 64), 64)
        if t < 3:
            return JW.at[ro_, pl.ds(pl.multiple_of(2048 * t + 128 * fs, 128), 128)]
        return EW.at[ro_, pl.ds(pl.multiple_of(512 * fs, 512), 512)]
    def je_group(g):
        if g == 0: hb_load().wait()
        x1(g).wait_recv()
        @pl.loop(0, 4)
        def _(j):
            fd = 4 * g + j
            add_into(HB.at[fd], RX.at[fd], 64)
            @pl.when(fd != f)
            def _():
                for t in range(4):
                    rc(srcp(fd, t), dst(f, t), sw.at[fd, t], rw.at[f, t], (r, fd)).start()
            @pl.when(fd == f)
            def _():
                for t in range(4):
                    lc(srcp(fd, t), dst(f, t), sw.at[fd, t]).start()
                    rc(srcp(fd, t), dst(f, t), sf.at[fd, t], rf.at[f, t], xp).start()
    def fwd_group(g):
        @pl.loop(4 * g, 4 * g + 4)
        def _(fs):
            @pl.when(fs != f)
            def _():
                for t in range(4):
                    rc(dst(fs, t), dst(fs, t), sw.at[fs, t], rw.at[fs, t], xp).wait_recv()
                    rc(dst(fs, t), dst(fs, t), sf.at[fs, t], rf.at[fs, t], xp).start()
    def je_drain():
        for g in range(4):
            x1(g).wait_send()
        @pl.loop(0, 16)
        def _(fs):
            for t in range(4):
                rc(dsto(fs, t), dsto(fs, t), sf.at[fs, t], rf.at[fs, t], xp).wait_recv()
                rc(dsto(fs, t), dsto(fs, t), sf.at[fs, t], rf.at[fs, t], xp).wait_send()
            @pl.when(fs != f)
            def _():
                for t in range(4):
                    rc(srcp(fs, t), dst(f, t), sw.at[fs, t], rw.at[f, t], xp).wait_send()
            @pl.when(fs == f)
            def _():
                for t in range(4):
                    lc(srcp(fs, t), dst(f, t), sw.at[fs, t]).wait()

    def o1(j):
        return rc(OS.at[1 - r, j], ROS.at[j], so.at[j], ro.at[j], xp)
    def o2(j):
        return rc(LOS.at[j], OSo.at[r, j], so2.at[j], ro2.at[j], xp)
    def o2r(j):
        return rc(LOS.at[j], OSo.at[1 - r, j], so2.at[j], ro2.at[j], xp)
    def os_load():
        return lc(OS.at[r], LOS, lsem.at[1])
    def os_store(j):
        return lc(LOS.at[j], OSo.at[r, j], lsem.at[2 + j])
    def os_step(j):
        if j == 0: os_load().wait()
        o1(j).wait_recv()
        add_into(LOS.at[j], ROS.at[j], 64)
        o2(j).start()
        os_store(j).start()
    def os_drain():
        for j in range(5):
            o1(j).wait_send(); o2(j).wait_send(); o2r(j).wait_recv(); os_store(j).wait()

    hb_load().start()
    for g in range(4): x1(g).start()
    os_load().start()
    for j in range(5): o1(j).start()
    R1[0]()
    R1[1]()
    R2[0]()
    R1[2](3)
    je_group(0)
    R1[2](0)
    je_group(1)
    R1[2](2); R2[1]()
    je_group(2)
    R1[2](1)
    je_group(3)
    os_step(0); os_step(1)
    R1[3](); R2[2](3)
    os_step(2); os_step(3); os_step(4)
    fwd_group(0)
    R2[2](0)
    fwd_group(1)
    R2[2](2)
    fwd_group(2)
    R2[2](1)
    fwd_group(3)
    R2[3]()
    je_drain(); os_drain()
    R1[4](); R2[4]()

def reduce_all(p1, p2, os_, je):
    D = pltpu.SemaphoreType.DMA
    hbm = pl.BlockSpec(memory_space=pl.ANY)
    vm = pl.BlockSpec(memory_space=pltpu.VMEM)
    S = jax.ShapeDtypeStruct
    return pl.pallas_call(
        reduce_kernel,
        out_shape=(S((128, 2048), f32), S((128, 2048), f32), S((2, 5, 64, 2048), bf), S((128, 6144), bf), S((128, 8192), bf)),
        in_specs=[hbm] * 4, out_specs=(vm, vm, hbm, hbm, hbm),
        scratch_shapes=[
            pltpu.VMEM((2, 8, 128, 2048), bf), pltpu.VMEM((2, 8, 128, 2048), bf), pltpu.VMEM((2, 4, 128, 2048), bf),
            pltpu.VMEM((2, 4, 128, 2048), bf), pltpu.VMEM((2, 4, 128, 2048), bf),
            pltpu.VMEM((16, 64, 896), bf), pltpu.VMEM((16, 64, 896), bf),
            pltpu.VMEM((5, 64, 2048), bf), pltpu.VMEM((5, 64, 2048), bf),
            D((2, 8)), D((2, 8)), D((2, 8)), D((2, 4)), D((2, 4)), D((2, 4)), D((2, 4)), D((2, 4)),
            D((4,)), D((4,)), D((5,)), D((5,)), D((5,)), D((5,)),
            D((16, 4)), D((16, 4)), D((16, 4)), D((16, 4)), D((8,))],
        compiler_params=pltpu.CompilerParams(collective_id=1, has_side_effects=True, vmem_limit_bytes=60 << 20),
    )(p1, p2, os_, je)


def wide(a):
    return a.astype(jnp.float32)


def normalize(rows):
    centre = jnp.mean(rows, -1, keepdims=True)
    centred = rows - centre
    inverse = lax.rsqrt(jnp.mean(centred * centred, -1, keepdims=True) + epsilon)
    return (centred * inverse, inverse)


def head_body(
    n,
    layer_input,
    segment,
    live_mask,
    attention_gain,
    attention_shift,
    joined_weight,
    joined_bias,
    output_weight,
    output_bias,
    feedforward_gain,
    feedforward_shift,
    expand_weight,
    expand_bias,
    shrink_weight,
    shrink_bias,
    cotangent,
):
    me = lax.axis_index("fsdp")
    own = layer_input.shape[0]
    width = layer_input.shape[1]
    part = width // n
    third = joined_bias.shape[0]
    piece = expand_weight.shape[1] // n
    heads = HEADS // n
    cols = heads * HEAD_DIM
    tokens = own * n
    low = jnp.bfloat16
    live_rows = wide(live_mask[0])[:, None]
    seeds = wide(cotangent)
    branch_own = (live_rows * seeds).astype(low)
    small = jnp.concatenate(
        [
            attention_gain,
            attention_shift,
            feedforward_gain,
            feedforward_shift,
            output_bias,
            shrink_bias,
            joined_bias,
            segment[0].astype(low),
        ]
    )
    small = jnp.pad(small, (0, 2048 - small.shape[0])).reshape(16, 128)
    rows_all, branch_all, small_all, weight_j, weight_e = gather_all(
        layer_input, branch_own, small, joined_weight, expand_weight
    )
    small_all = small_all.reshape(n, 2048)
    rows = wide(rows_all).reshape(tokens, width)
    branch = branch_all.reshape(tokens, width)
    gain_one, shift_one, gain_two, shift_two, bias_o, bias_s = (
        wide(small_all[:, k * part : (k + 1) * part]).reshape(width) for k in range(6)
    )
    bias_j = wide(small_all[:, 6 * part : 6 * part + third]).reshape(3, n, cols)
    bias_j = lax.dynamic_index_in_dim(bias_j, me, 1, keepdims=False).reshape(3 * cols)
    seg_all = small_all[:, 6 * part + third : 6 * part + third + own]

    weight_os = jnp.concatenate([output_weight, shrink_weight], 0)

    normalized, inverse = normalize(rows)
    normed_one = (normalized * gain_one + shift_one).astype(low)
    normed_two = (normalized * gain_two + shift_two).astype(low)
    joined = jnp.dot(normed_one, weight_j, preferred_element_type=jnp.float32) + bias_j
    seg_int = seg_all.astype(jnp.int32)
    cosine, sine = rotary_tables(seg_int)
    places = jnp.arange(own, dtype=jnp.int32)
    allowed = (seg_int[:, :, None] == seg_int[:, None, :]) & (
        places[None, None, :] <= places[None, :, None]
    )
    split = joined.reshape(n, own, 3, heads, HEAD_DIM)
    queries = turn(split[:, :, 0], cosine, sine, 1.0).astype(low)
    keys = turn(split[:, :, 1], cosine, sine, 1.0).astype(low)
    values = split[:, :, 2].astype(low)
    scale = HEAD_DIM ** (-0.5)
    scores = (
        jnp.einsum("bthd,bshd->bhts", queries, keys, preferred_element_type=jnp.float32) * scale
    )
    scores = jnp.where(allowed[:, None], scores, masked_score)
    top = jnp.max(scores, -1, keepdims=True)
    expo = jnp.exp(scores - top)
    probs = expo / jnp.sum(expo, -1, keepdims=True)
    probs_low = probs.astype(low)
    mixed = jnp.einsum("bhts,bshd->bthd", probs_low, values, preferred_element_type=jnp.float32)
    mixed = mixed.reshape(tokens, cols).astype(low)
    expanded = jnp.dot(normed_two, weight_e, preferred_element_type=jnp.float32) + wide(expand_bias)
    activated = jax.nn.gelu(expanded, approximate=False).astype(low)
    slope = gelu_slope(expanded)
    inner = jnp.concatenate([mixed, activated], 1)
    partial = jnp.dot(inner, weight_os, preferred_element_type=jnp.float32).astype(low)

    grad_os = jnp.einsum("tf,td->fd", inner, branch, preferred_element_type=jnp.float32)
    inner_grad = jnp.einsum("td,fd->tf", branch, weight_os, preferred_element_type=jnp.float32)
    expanded_grad = (inner_grad[:, cols:] * slope).astype(low)
    mixed_grad = inner_grad[:, :cols].astype(low).reshape(n, own, heads, HEAD_DIM)
    value_grad = jnp.einsum(
        "bhts,bthd->bshd", probs_low, mixed_grad, preferred_element_type=jnp.float32
    )
    probs_grad = jnp.einsum(
        "bthd,bshd->bhts", mixed_grad, values, preferred_element_type=jnp.float32
    )
    scores_grad = (probs * (probs_grad - jnp.sum(probs_grad * probs, -1, keepdims=True))).astype(low)
    query_grad = (
        jnp.einsum("bhts,bshd->bthd", scores_grad, keys, preferred_element_type=jnp.float32) * scale
    )
    key_grad = (
        jnp.einsum("bhts,bthd->bshd", scores_grad, queries, preferred_element_type=jnp.float32)
        * scale
    )
    query_grad = turn(query_grad, cosine, sine, -1.0)
    key_grad = turn(key_grad, cosine, sine, -1.0)
    joined_grad = jnp.concatenate(
        [a.reshape(tokens, cols) for a in (query_grad, key_grad, value_grad)], 1
    ).astype(low)
    grad_j = jnp.einsum("td,te->de", normed_one, joined_grad, preferred_element_type=jnp.float32)
    grad_e = jnp.einsum("td,tf->df", normed_two, expanded_grad, preferred_element_type=jnp.float32)
    back_one = jnp.einsum("te,de->td", joined_grad, weight_j, preferred_element_type=jnp.float32)
    back_two = jnp.einsum("tf,df->td", expanded_grad, weight_e, preferred_element_type=jnp.float32)
    hat = (back_one * gain_one + back_two * gain_two).astype(low)
    grads = jnp.concatenate([grad_j, grad_e], 1).astype(low)
    summed, hat_own, rest_os, joined_weight_grad, expand_weight_grad = reduce_all(
        partial.reshape(n, own, width),
        hat.reshape(n, own, width),
        grad_os.astype(low).reshape(2, 5, 64, width),
        grads.reshape(n, 2, part // 2, 3 * cols + piece),
    )
    rest_os = wide(rest_os).reshape(cols + piece, width)
    layer_output = (
        wide(layer_input) + live_rows * (summed + (bias_o + bias_s))
    ).astype(low)

    rows_own = wide(layer_input)
    normalized_own, inverse_own = normalize(rows_own)
    row_grad = inverse_own * (
        hat_own
        - jnp.mean(hat_own, -1, keepdims=True)
        - normalized_own * jnp.mean(hat_own * normalized_own, -1, keepdims=True)
    )
    input_grad = (seeds + row_grad).astype(low)

    vectors = jnp.stack(
        [
            jnp.sum(back_one * normalized, 0),
            jnp.sum(back_one, 0),
            jnp.sum(back_two * normalized, 0),
            jnp.sum(back_two, 0),
        ]
    )
    bias_j_grad = jnp.sum(wide(joined_grad), 0).reshape(3, 1, cols)
    bias_j_grad = jnp.where(
        lax.broadcasted_iota(jnp.int32, (3, n, cols), 1) == me, bias_j_grad, 0.0
    ).reshape(-1)
    branch_sum = jnp.sum(wide(branch_own), 0)
    small_sums = lax.psum(
        jnp.concatenate([vectors.reshape(-1), branch_sum, bias_j_grad]), ("rep", "fsdp")
    )
    pieces = small_sums[: 5 * width].reshape(5, n, part)
    pieces = lax.dynamic_index_in_dim(pieces, me, 1, keepdims=False)
    joined_bias_grad = lax.dynamic_slice(small_sums, (5 * width + me * third,), (third,))
    expand_bias_grad = jnp.sum(wide(expanded_grad), 0)
    expand_bias_grad = wide(lax.psum(expand_bias_grad.astype(low), "rep"))
    return (
        layer_output,
        input_grad,
        pieces[0],
        pieces[1],
        wide(joined_weight_grad),
        joined_bias_grad,
        rest_os[:cols],
        pieces[4],
        pieces[2],
        pieces[3],
        wide(expand_weight_grad),
        expand_bias_grad,
        rest_os[cols:],
        pieces[4],
    )


def solution(mesh):
    n = mesh.shape["fsdp"]
    chosen = functools.partial(head_body, n) if n == HEADS else body
    placed = (
        P(("rep", "fsdp"), None),
        P(("rep", "fsdp"), None),
        P(("rep", "fsdp"), None),
        P("fsdp"),
        P("fsdp"),
        P("fsdp", None),
        P("fsdp"),
        P("fsdp", None),
        P("fsdp"),
        P("fsdp"),
        P("fsdp"),
        P("fsdp", None),
        P("fsdp"),
        P("fsdp", None),
        P("fsdp"),
        P(("rep", "fsdp"), None),
    )
    return jax.shard_map(
        chosen,
        mesh=mesh,
        in_specs=placed,
        out_specs=(
            P(("rep", "fsdp"), None),
            P(("rep", "fsdp"), None),
            P("fsdp"),
            P("fsdp"),
            P("fsdp", None),
            P("fsdp"),
            P("fsdp", None),
            P("fsdp"),
            P("fsdp"),
            P("fsdp"),
            P("fsdp", None),
            P("fsdp"),
            P("fsdp", None),
            P("fsdp"),
        ),
        check_vma=False,
    )
```

```python
import functools

import jax
import jax.numpy as jnp
import numpy as np
from jax import lax
from jax.experimental import pallas as pl
from jax.experimental.pallas import tpu as pltpu
from jax.sharding import PartitionSpec as P

D = 2048
HEADS = 16
HEAD_DIM = 128
ROT = 32


epsilon = 1e-05
masked_score = -1e30
rotary_base = 10000.0


def as_sent(shard):
    return jax.tree.map(lambda a: a.astype(jnp.bfloat16) if a.dtype == jnp.float32 else a, shard)


def norm_rows(rows, gain, shift):
    centre = jnp.mean(rows, -1, keepdims=True)
    centred = rows - centre
    inverse = lax.rsqrt(jnp.mean(centred * centred, -1, keepdims=True) + epsilon)
    normalized = centred * inverse
    return (normalized * gain.astype(jnp.float32) + shift.astype(jnp.float32), normalized, inverse)


def norm_back(normed_grad, normalized, inverse, gain):
    scaled = normed_grad * gain.astype(jnp.float32)
    row_grad = inverse * (
        scaled
        - jnp.mean(scaled, -1, keepdims=True)
        - normalized * jnp.mean(scaled * normalized, -1, keepdims=True)
    )
    return (row_grad, jnp.sum(normed_grad * normalized, 0), jnp.sum(normed_grad, 0))


def rotary_tables(segment):
    length = segment.shape[-1]
    places = jnp.arange(length, dtype=jnp.int32)
    earlier = jnp.sum((segment[..., None, :] < segment[..., :, None]).astype(jnp.int32), -1)
    position = (places - earlier).astype(jnp.float32)
    exponent = jnp.arange(ROT // 2, dtype=jnp.float32) * 2.0 / ROT
    frequency = jnp.power(jnp.float32(rotary_base), -exponent)
    angle = position[..., None] * frequency
    return (jnp.cos(angle), jnp.sin(angle))


def turn(heads, cosine, sine, sign):
    half = ROT // 2
    front = heads[..., :half]
    behind = heads[..., half:ROT]
    cos_wide = cosine[..., None, :]
    sin_wide = sine[..., None, :] * sign
    return jnp.concatenate(
        [
            front * cos_wide - behind * sin_wide,
            behind * cos_wide + front * sin_wide,
            heads[..., ROT:],
        ],
        -1,
    )


def gelu_slope(values):
    return (
        0.5 * (1.0 + lax.erf(values * 0.7071067811865476))
        + values * jnp.exp(-0.5 * values * values) * 0.3989422804014327
    )


def attention_inputs(rows, weights, cosine, sine):
    gain, shift, joined_weight, joined_bias = (weights[0], weights[1], weights[2], weights[3])
    normed, normalized, inverse = norm_rows(rows, gain, shift)
    normed_low = normed.astype(jnp.bfloat16)
    joined = jnp.dot(
        normed_low, joined_weight, preferred_element_type=jnp.float32
    ) + joined_bias.astype(jnp.float32)
    length = rows.shape[0]
    split = joined.reshape(length, 3, HEADS, HEAD_DIM)
    queries = turn(split[:, 0], cosine, sine, 1.0).astype(jnp.bfloat16)
    keys = turn(split[:, 1], cosine, sine, 1.0).astype(jnp.bfloat16)
    values = split[:, 2].astype(jnp.bfloat16)
    return (normed_low, normalized, inverse, queries, keys, values)


def score_block(queries, keys, allowed):
    scores = jnp.einsum(
        "thd,shd->hts", queries, keys, preferred_element_type=jnp.float32
    ) * HEAD_DIM ** (-0.5)
    return jnp.where(allowed[None], scores, masked_score)


def feedforward_inputs(rows, weights):
    gain, shift, expand_weight, expand_bias = (weights[0], weights[1], weights[2], weights[3])
    normed, normalized, inverse = norm_rows(rows, gain, shift)
    normed_low = normed.astype(jnp.bfloat16)
    expanded = jnp.dot(
        normed_low, expand_weight, preferred_element_type=jnp.float32
    ) + expand_bias.astype(jnp.float32)
    return (normed_low, normalized, inverse, expanded)


def body(
    layer_input,
    segment,
    live_mask,
    attention_gain,
    attention_shift,
    joined_weight,
    joined_bias,
    output_weight,
    output_bias,
    feedforward_gain,
    feedforward_shift,
    expand_weight,
    expand_bias,
    shrink_weight,
    shrink_bias,
    cotangent,
):
    rows = layer_input.astype(jnp.float32)
    seg_row = segment[0]
    live_rows = live_mask[0].astype(jnp.float32)[:, None]
    length = seg_row.shape[0]
    cosine, sine = rotary_tables(seg_row)
    places = jnp.arange(length, dtype=jnp.int32)
    allowed = (seg_row[:, None] == seg_row[None, :]) & (places[None, :] <= places[:, None])
    attention_parts = (
        attention_gain,
        attention_shift,
        joined_weight,
        joined_bias,
        output_weight,
        output_bias,
    )
    feedforward_parts = (
        feedforward_gain,
        feedforward_shift,
        expand_weight,
        expand_bias,
        shrink_weight,
        shrink_bias,
    )
    attention_full = (
        lax.all_gather(attention_gain, "fsdp", axis=0, tiled=True),
        lax.all_gather(attention_shift, "fsdp", axis=0, tiled=True),
        lax.all_gather(joined_weight, "fsdp", axis=0, tiled=True),
        lax.all_gather(joined_bias, "fsdp", axis=0, tiled=True),
        lax.all_gather(output_weight, "fsdp", axis=0, tiled=True),
        lax.all_gather(output_bias, "fsdp", axis=0, tiled=True),
    )
    feedforward_full = (
        lax.all_gather(feedforward_gain, "fsdp", axis=0, tiled=True),
        lax.all_gather(feedforward_shift, "fsdp", axis=0, tiled=True),
        lax.all_gather(expand_weight, "fsdp", axis=0, tiled=True),
        lax.all_gather(expand_bias, "fsdp", axis=0, tiled=True),
        lax.all_gather(shrink_weight, "fsdp", axis=0, tiled=True),
        lax.all_gather(shrink_bias, "fsdp", axis=0, tiled=True),
    )
    normed_one, normalized_one, inverse_one, queries, keys, values = attention_inputs(
        rows, attention_full, cosine, sine
    )
    scores = score_block(queries, keys, allowed)
    top = jnp.max(scores, -1, keepdims=True)
    expo = jnp.exp(scores - top)
    total = jnp.sum(expo, -1, keepdims=True)
    log_total = top + jnp.log(total)
    probs_low = (expo / total).astype(jnp.bfloat16)
    mixed = jnp.einsum("hts,shd->thd", probs_low, values, preferred_element_type=jnp.float32)
    mixed = mixed.reshape(length, D).astype(jnp.bfloat16)
    attended = jnp.dot(
        mixed, attention_full[4], preferred_element_type=jnp.float32
    ) + attention_full[5].astype(jnp.float32)
    normed_two, normalized_two, inverse_two, expanded = feedforward_inputs(rows, feedforward_full)
    activated = jax.nn.gelu(expanded, approximate=False).astype(jnp.bfloat16)
    shrunk = jnp.dot(
        activated, feedforward_full[4], preferred_element_type=jnp.float32
    ) + feedforward_full[5].astype(jnp.float32)
    layer_output = (rows + live_rows * (attended + shrunk)).astype(jnp.bfloat16)
    seed_rows = cotangent.astype(jnp.float32)
    branch_grad = (live_rows * seed_rows).astype(jnp.bfloat16)
    branch_total = jnp.sum(branch_grad.astype(jnp.float32), 0)
    feedforward_back = lax.all_gather(
        as_sent(lax.optimization_barrier((feedforward_parts, layer_output))[0]),
        "fsdp",
        axis=0,
        tiled=True,
    )
    normed_two, normalized_two, inverse_two, expanded = feedforward_inputs(rows, feedforward_back)
    activated = jax.nn.gelu(expanded, approximate=False).astype(jnp.bfloat16)
    shrink_weight_grad = jnp.einsum(
        "tf,td->fd", activated, branch_grad, preferred_element_type=jnp.float32
    )
    activated_grad = jnp.einsum(
        "td,fd->tf", branch_grad, feedforward_back[4], preferred_element_type=jnp.float32
    )
    expanded_grad = (activated_grad * gelu_slope(expanded)).astype(jnp.bfloat16)
    expand_bias_grad = jnp.sum(expanded_grad.astype(jnp.float32), 0)
    expand_weight_grad = jnp.einsum(
        "td,tf->df", normed_two, expanded_grad, preferred_element_type=jnp.float32
    )
    normed_two_grad = jnp.einsum(
        "tf,df->td", expanded_grad, feedforward_back[2], preferred_element_type=jnp.float32
    )
    rows_grad_two, ff_gain_grad, ff_shift_grad = norm_back(
        normed_two_grad, normalized_two, inverse_two, feedforward_back[0]
    )
    ff_terms = (
        ff_gain_grad,
        ff_shift_grad,
        expand_weight_grad,
        expand_bias_grad,
        shrink_weight_grad,
        branch_total,
    )
    ff_parts = (
        lax.psum_scatter(ff_terms[0], "fsdp", scatter_dimension=0, tiled=True),
        lax.psum_scatter(ff_terms[1], "fsdp", scatter_dimension=0, tiled=True),
        lax.psum_scatter(ff_terms[2], "fsdp", scatter_dimension=0, tiled=True),
        lax.psum_scatter(ff_terms[3], "fsdp", scatter_dimension=0, tiled=True),
        lax.psum_scatter(ff_terms[4], "fsdp", scatter_dimension=0, tiled=True),
        lax.psum_scatter(ff_terms[5], "fsdp", scatter_dimension=0, tiled=True),
    )
    attention_back = lax.all_gather(
        as_sent(lax.optimization_barrier((attention_parts, layer_output))[0]),
        "fsdp",
        axis=0,
        tiled=True,
    )
    normed_one, normalized_one, inverse_one, queries, keys, values = attention_inputs(
        rows, attention_back, cosine, sine
    )
    scores = score_block(queries, keys, allowed)
    probs = jnp.exp(scores - log_total)
    probs_low = probs.astype(jnp.bfloat16)
    mixed = jnp.einsum("hts,shd->thd", probs_low, values, preferred_element_type=jnp.float32)
    mixed = mixed.reshape(length, D).astype(jnp.bfloat16)
    output_weight_grad = jnp.einsum(
        "td,te->de", mixed, branch_grad, preferred_element_type=jnp.float32
    )
    mixed_grad = jnp.einsum(
        "te,de->td", branch_grad, attention_back[4], preferred_element_type=jnp.float32
    )
    mixed_grad = mixed_grad.astype(jnp.bfloat16).reshape(length, HEADS, HEAD_DIM)
    value_grad = jnp.einsum(
        "hts,thd->shd", probs_low, mixed_grad, preferred_element_type=jnp.float32
    )
    probs_grad = jnp.einsum("thd,shd->hts", mixed_grad, values, preferred_element_type=jnp.float32)
    scores_grad = (probs * (probs_grad - jnp.sum(probs_grad * probs, -1, keepdims=True))).astype(
        jnp.bfloat16
    )
    query_grad = jnp.einsum(
        "hts,shd->thd", scores_grad, keys, preferred_element_type=jnp.float32
    ) * HEAD_DIM ** (-0.5)
    key_grad = jnp.einsum(
        "hts,thd->shd", scores_grad, queries, preferred_element_type=jnp.float32
    ) * HEAD_DIM ** (-0.5)
    query_grad = turn(query_grad, cosine, sine, -1.0)
    key_grad = turn(key_grad, cosine, sine, -1.0)
    joined_grad = jnp.concatenate(
        [query_grad.reshape(length, D), key_grad.reshape(length, D), value_grad.reshape(length, D)],
        1,
    ).astype(jnp.bfloat16)
    joined_bias_grad = jnp.sum(joined_grad.astype(jnp.float32), 0)
    joined_weight_grad = jnp.einsum(
        "td,te->de", normed_one, joined_grad, preferred_element_type=jnp.float32
    )
    normed_one_grad = jnp.einsum(
        "te,de->td", joined_grad, attention_back[2], preferred_element_type=jnp.float32
    )
    rows_grad_one, at_gain_grad, at_shift_grad = norm_back(
        normed_one_grad, normalized_one, inverse_one, attention_back[0]
    )
    at_terms = (
        at_gain_grad,
        at_shift_grad,
        joined_weight_grad,
        joined_bias_grad,
        output_weight_grad,
        branch_total,
    )
    at_parts = (
        lax.psum_scatter(at_terms[0], "fsdp", scatter_dimension=0, tiled=True),
        lax.psum_scatter(at_terms[1], "fsdp", scatter_dimension=0, tiled=True),
        lax.psum_scatter(at_terms[2], "fsdp", scatter_dimension=0, tiled=True),
        lax.psum_scatter(at_terms[3], "fsdp", scatter_dimension=0, tiled=True),
        lax.psum_scatter(at_terms[4], "fsdp", scatter_dimension=0, tiled=True),
        lax.psum_scatter(at_terms[5], "fsdp", scatter_dimension=0, tiled=True),
    )
    input_grad = (seed_rows + rows_grad_one + rows_grad_two).astype(jnp.bfloat16)
    summed = (
        lax.psum(at_parts[0].astype(jnp.bfloat16), "rep").astype(jnp.float32),
        lax.psum(at_parts[1].astype(jnp.bfloat16), "rep").astype(jnp.float32),
        lax.psum(at_parts[2].astype(jnp.bfloat16), "rep").astype(jnp.float32),
        lax.psum(at_parts[3].astype(jnp.bfloat16), "rep").astype(jnp.float32),
        lax.psum(at_parts[4].astype(jnp.bfloat16), "rep").astype(jnp.float32),
        lax.psum(at_parts[5].astype(jnp.bfloat16), "rep").astype(jnp.float32),
        lax.psum(ff_parts[0].astype(jnp.bfloat16), "rep").astype(jnp.float32),
        lax.psum(ff_parts[1].astype(jnp.bfloat16), "rep").astype(jnp.float32),
        lax.psum(ff_parts[2].astype(jnp.bfloat16), "rep").astype(jnp.float32),
        lax.psum(ff_parts[3].astype(jnp.bfloat16), "rep").astype(jnp.float32),
        lax.psum(ff_parts[4].astype(jnp.bfloat16), "rep").astype(jnp.float32),
        lax.psum(ff_parts[5].astype(jnp.bfloat16), "rep").astype(jnp.float32),
    )
    return (
        layer_output,
        input_grad,
        summed[0],
        summed[1],
        summed[2],
        summed[3],
        summed[4],
        summed[5],
        summed[6],
        summed[7],
        summed[8],
        summed[9],
        summed[10],
        summed[11],
    )


MESH = pl.DeviceIdType.MESH
bf = jnp.bfloat16
f32 = jnp.float32
WIDE = 2048
TOK = 2048


def ds(start, size):
    return pl.ds(pl.multiple_of(start, size), size)


def mm(a, b, ca, cb):
    return lax.dot_general(a, b, (((ca,), (cb,)), ((), ())), preferred_element_type=f32)


def layer_kernel(
    x_ref, bg_ref, sm_ref, jw_ref, ew_ref, wo_ref, ws_ref, ct_ref, st_ref, eb_ref,
    SO1, SO2, OSo, JWo, EWo, FIN, SMO,
    X, BG, WJ, WE, WOS, INNER, QKV, SLOPE, CT, ST, PR, L1, RING, A1, B1, C1, C2X,
    JB, RX, OSB, ROS, STAGE, T1, SM, SMF, CV, GBR, COL, VC, VEC, VR, TOT, TX, BSUM,
    su, sd, sy, ss, rx_, bu, bd, by, bs, rb_, sw, rw, sxw, rxw, ssm, rsm,
    sa, ra, sbb, rbb, sc, rc_, sx, rxx, so, ro, so2, ro2, sg, rg, sf, rf, sv, rv, st_, rt_, lsem, ready,
):
    r = lax.axis_index("rep")
    f = lax.axis_index("fsdp")
    z = f // 4
    y = (f // 2) % 2
    c = f % 2
    sib = (r, z * 4 + y * 2 + (1 - c))
    yo = z * 4 + (1 - y) * 2 + c
    yp = (r, yo)
    xp = (1 - r, f)
    lower = z <= 1
    zz = jnp.where(lower, z, 3 - z)

    def phys(q):
        return jnp.where(lower, q, 3 - q)

    f_in = (r, jnp.where(lower, f + 4, f - 4))
    f_out = (r, jnp.where(lower, f - 4, f + 4))

    barrier = pltpu.get_barrier_semaphore()

    @pl.loop(1, 16)
    def _(k):
        pl.semaphore_signal(barrier, inc=1, device_id=(r, (f + k) % 16), device_id_type=MESH)

    pl.semaphore_signal(barrier, inc=1, device_id=xp, device_id_type=MESH)
    pl.semaphore_wait(barrier, 16)

    def rc(src, dst, s, q, dev):
        return pltpu.make_async_remote_copy(
            src_ref=src, dst_ref=dst, send_sem=s, recv_sem=q, device_id=dev, device_id_type=MESH
        )

    def lc(src, dst, s):
        return pltpu.make_async_copy(src, dst, s)

    def gather(own, OUT, su, sd, sy, ss, rr):
        def item(i):
            return OUT.at[ds(128 * i, 128)]

        def up(i, src=None):
            return rc(item(i) if src is None else src, item(i), su.at[i], rr.at[i], (r, f + 4))

        def dn(i, src=None):
            return rc(item(i) if src is None else src, item(i), sd.at[i], rr.at[i], (r, f - 4))

        def ac(i, src=None):
            return rc(item(i) if src is None else src, item(i), sy.at[i], rr.at[i], yp)

        def sb(i, src=None):
            return rc(item(i) if src is None else src, item(i), ss.at[i], rr.at[i], sib)

        def begin():
            pl.when(z < 3)(lambda: up(f, own).start())
            pl.when(z > 0)(lambda: dn(f, own).start())
            ac(f, own).start()
            sb(f, own).start()

        def step(s):
            @pl.when(z - s >= 0)
            def _():
                i = f - 4 * s
                up(i).wait_recv()
                pl.when(z < 3)(lambda: up(i).start())
                ac(i).start()
                sb(i).start()

            @pl.when(z + s <= 3)
            def _():
                i = f + 4 * s
                dn(i).wait_recv()
                pl.when(z > 0)(lambda: dn(i).start())
                ac(i).start()
                sb(i).start()

        def ystep(s):
            if s == 0:
                ac(yo).wait_recv()
                sb(yo).start()
            else:
                @pl.when(z - s >= 0)
                def _():
                    ac(yo - 4 * s).wait_recv()
                    sb(yo - 4 * s).start()

                @pl.when(z + s <= 3)
                def _():
                    ac(yo + 4 * s).wait_recv()
                    sb(yo + 4 * s).start()

        def finish():
            @pl.loop(0, 8)
            def _(k):
                sb(2 * k + (1 - c)).wait_recv()

            @pl.loop(0, 8)
            def _(k):
                sb(2 * k + c).wait_send()

            @pl.loop(0, 4)
            def _(k):
                i = k * 4 + y * 2 + c
                ac(i).wait_send()
                pl.when((k <= z) & (z < 3))(lambda: up(i).wait_send())
                pl.when((k >= z) & (z > 0))(lambda: dn(i).wait_send())

        return begin, step, ystep, finish

    xb, xs, xy, xf = gather(x_ref, X, su, sd, sy, ss, rx_)
    gb, gs, gy, gf = gather(bg_ref, BG, bu, bd, by, bs, rb_)

    def wpieces(src, dst, from_arg):
        rows = ds(128 * src + 64 * r, 64)
        out = []
        for t in range(3):
            d = WJ.at[rows, pl.ds(128 * t, 128)]
            out.append((jw_ref.at[ds(64 * r, 64), ds(2048 * t + 128 * dst, 128)] if from_arg else d, d))
        d = WE.at[rows]
        out.append((ew_ref.at[ds(64 * r, 64), ds(512 * dst, 512)] if from_arg else d, d))
        return out

    def fwd(lo, hi):
        @pl.loop(lo, hi)
        def _(k):
            fs = (f + 16 - k) % 16
            for t, (s, d) in enumerate(wpieces(fs, f, False)):
                rc(s, d, sw.at[fs, t], rw.at[fs, t], (r, f)).wait_recv()
                rc(s, d, sxw.at[fs, t], rxw.at[fs, t], xp).start()

    own_x = lc(x_ref, X.at[ds(128 * f, 128)], lsem.at[0])
    own_b = lc(bg_ref, BG.at[ds(128 * f, 128)], lsem.at[1])
    load_o = lc(wo_ref, WOS.at[pl.ds(0, 128)], lsem.at[2])
    load_s = lc(ws_ref, WOS.at[pl.ds(128, 512)], lsem.at[3])
    own_s = lc(sm_ref, SM.at[f], lsem.at[4])
    xb()
    for cp in (own_x, own_b, load_o, load_s, own_s):
        cp.start()

    @pl.loop(1, 16)
    def _(k):
        fd = (f + k) % 16
        rc(sm_ref, SM.at[f], ssm.at[fd], rsm.at[f], (r, fd)).start()
        for t, (s, d) in enumerate(wpieces(f, fd, True)):
            rc(s, d, sw.at[fd, t], rw.at[f, t], (r, fd)).start()

    for t, (s, d) in enumerate(wpieces(f, f, True)):
        rc(s, d, sxw.at[f, t], rxw.at[f, t], xp).start()
        lc(s, d, rw.at[f, t]).start()
    xs(1)
    xy(0)
    fwd(1, 5)
    xs(2)
    xy(1)
    fwd(5, 9)
    xs(3)
    xy(2)
    fwd(9, 13)
    gb()
    xy(3)
    own_s.wait()

    @pl.loop(1, 16)
    def _(k):
        fs = (f + k) % 16
        other = rc(sm_ref, SM.at[fs], ssm.at[fs], rsm.at[fs], (r, fs))
        other.wait_recv()
        other.wait_send()

    @pl.loop(0, 16)
    def _(i):
        SMF[ds(16 * i, 16)] = SM[i].astype(f32)

    send_small = lc(SMF, SMO, lsem.at[4])
    send_small.start()

    @pl.loop(0, 16)
    def _(i):
        rows = ds(128 * i, 128)
        place = jnp.broadcast_to(SMF[pl.ds(16 * i + 10, 1)], (128, 128)).T
        pick = (place == lax.broadcasted_iota(jnp.int32, (128, 128), 1).astype(f32)).astype(f32)
        hi = lax.Precision.HIGHEST
        CT[rows] = jnp.dot(pick, ct_ref[...], precision=hi, preferred_element_type=f32)
        ST[rows] = jnp.dot(pick, st_ref[...], precision=hi, preferred_element_type=f32)

    fwd(13, 16)
    own_x.wait()
    xf()

    @pl.loop(0, 16)
    def _(i):
        @pl.loop(0, 8, unroll=2)
        def _(k):
            w = ds(128 * i + 16 * k, 16)
            v = X[w].astype(f32)
            v = v - jnp.mean(v, -1, keepdims=True)
            v = v * lax.rsqrt(jnp.mean(v * v, -1, keepdims=True) + epsilon)
            X[w] = v.astype(bf)

        @pl.when(i == 8)
        def _():
            gs(1)
            gy(0)

    gs(2)
    gy(1)

    for t, (s, d) in enumerate(wpieces(f, f, True)):
        lc(s, d, rw.at[f, t]).wait()
    other_half = lambda src: ds(128 * src + 64 * (1 - r), 64)

    @pl.loop(0, 16)
    def _(fs):
        for t in range(4):
            d = WJ.at[other_half(fs), pl.ds(128 * t, 128)] if t < 3 else WE.at[other_half(fs)]
            cp = rc(d, d, sxw.at[fs, t], rxw.at[fs, t], xp)
            cp.wait_recv()
            cp.wait_send()

    load_o.wait()
    load_s.wait()

    def columns(j):
        for v in range(4):
            COL[v] = jnp.broadcast_to(SMF[pl.ds(16 * j + v, 1)], (128, 128)).T

    def fold(v):
        return v[:8] + v[8:]

    CV[...] = jnp.zeros_like(CV)

    @pl.loop(0, 16)
    def _(j):
        columns(j)

        @pl.loop(0, 8)
        def _(k):
            w = ds(128 * j + 16 * k, 16)
            cw = ds(16 * k, 16)
            g1, s1, g2, s2 = (COL[v, cw] for v in range(4))
            for t in range(3):
                l = pl.ds(128 * t, 128)
                v = WJ[w, l].astype(f32)
                CV[:, l] += fold(v * s1)
                WJ[w, l] = (v * g1).astype(bf)
            for t in range(4):
                l = pl.ds(128 * t, 128)
                lo = pl.ds(384 + 128 * t, 128)
                v = WE[w, l].astype(f32)
                CV[:, lo] += fold(v * s2)
                WE[w, l] = (v * g2).astype(bf)

    CV[...] = jnp.broadcast_to(jnp.sum(CV[...], 0, keepdims=True), CV.shape)
    for t in range(3):
        place = (16 * t + f) // 3 * 16 + 6 + (16 * t + f) % 3
        CV[:, pl.ds(128 * t, 128)] += SMF[pl.ds(place, 1)]
    CV[:, pl.ds(384, 512)] += eb_ref[...]

    lane = lax.broadcasted_iota(jnp.int32, (16, 128), 1)

    def swap(v, ln):
        return jnp.where(ln < 16, pltpu.roll(v, 112, 1), pltpu.roll(v, 16, 1))

    @pl.loop(0, 4)
    def _(i):
        rows = ds(512 * i, 512)
        T1[:, pl.ds(0, 384)] = mm(X[rows], WJ[...], 1, 0)
        T1[:, pl.ds(384, 512)] = mm(X[rows], WE[...], 1, 0)

        @pl.loop(0, 32, unroll=2)
        def _(k):
            w = ds(16 * k, 16)
            gw = ds(512 * i + 16 * k, 16)
            cos, sin = CT[gw], ST[gw]
            for t in range(2):
                l = pl.ds(128 * t, 128)
                v = T1[w, l] + CV[0:1, l]
                QKV[gw, l] = (v * cos + swap(v, lane) * sin).astype(bf)
            l = pl.ds(256, 128)
            QKV[gw, l] = (T1[w, l] + CV[0:1, l]).astype(bf)
            for t in range(4):
                l = pl.ds(384 + 128 * t, 128)
                v = T1[w, l] + CV[0:1, l]
                part = 0.5 * (1.0 + lax.erf(v * 0.7071067811865476))
                INNER[gw, pl.ds(128 + 128 * t, 128)] = (v * part).astype(bf)
                SLOPE[gw, pl.ds(128 * t, 128)] = (
                    part + v * jnp.exp(-0.5 * v * v) * 0.3989422804014327
                ).astype(bf)

        @pl.when(i == 1)
        def _():
            gs(3)
            gy(2)

        @pl.when(i == 3)
        def _():
            gy(3)

    scale = HEAD_DIM ** (-0.5)
    down = lax.broadcasted_iota(jnp.int32, (128, 128), 0)
    across = lax.broadcasted_iota(jnp.int32, (128, 128), 1)

    @pl.loop(0, 16, unroll=2)
    def _(i):
        rows = ds(128 * i, 128)
        q = QKV[rows, pl.ds(0, 128)]
        k = QKV[rows, pl.ds(128, 128)]
        v = QKV[rows, pl.ds(256, 128)]
        seg = jnp.broadcast_to(SMF[pl.ds(16 * i + 9, 1)], (128, 128))
        s = mm(q, k, 1, 1) * scale
        s = jnp.where((seg == seg.T) & (across <= down), s, masked_score)
        e = jnp.exp(s - jnp.max(s, -1, keepdims=True))
        p = e / jnp.sum(e, -1, keepdims=True)
        PR[rows] = p
        INNER[rows, pl.ds(0, 128)] = mm(p.astype(bf), v, 1, 0).astype(bf)

    def add_into(dst, src, rows):
        @pl.loop(0, rows // 16)
        def _(i):
            w = ds(i * 16, 16)
            dst[w] = (dst[w].astype(f32) + src[w].astype(f32)).astype(bf)

    def reducer(n, sent, own, AA, BB, CC, CX, SO):
        def a_send(k):
            return rc(sent(k), AA(k), sa.at[n, k], ra.at[n, k], sib)

        def b_send(zp):
            return rc(own(zp * 2 + 1 - y), BB(zp), sbb.at[n, zp], rbb.at[n, zp], yp)

        def prep(k):
            a_send(k).wait_recv()
            add_into(own(k), AA(k), 128)

        def far():
            for q in (3, 0, 2, 1):
                prep(phys(q) * 2 + 1 - y)
                b_send(phys(q)).start()

        def near(q):
            zp = phys(q)
            k = zp * 2 + y
            prep(k)
            b_send(zp).wait_recv()
            add_into(own(k), BB(zp), 128)

        def got(q, extra=False):
            zp = phys(q)
            buf = CX if extra else CC(zp)
            slot = 4 if extra else zp
            rc(buf, buf, sc.at[n, zp], rc_.at[n, slot], f_in).wait_recv()
            return buf

        def send(q, dev, extra=False):
            zp = phys(q)
            return rc(
                own(zp * 2 + y), CX if extra else CC(zp), sc.at[n, zp], rc_.at[n, 4 if extra else zp], dev
            )

        def step(q):
            near(q)
            zp = phys(q)
            k = zp * 2 + y

            @pl.when(zz == 0)
            def _():
                if q > 0:
                    send(q, f_in).start()

            @pl.when(zz == 1)
            def _():
                if q >= 2:
                    add_into(own(k), got(q), 128)
                    send(q, f_in, q == 2).start()
                if q == 0:
                    add_into(own(k), got(q), 128)
                    send(q, f_out).start()

        def total(q, bufs):
            k = phys(q) * 2 + y

            @pl.loop(0, 8)
            def _(i):
                w = ds(i * 16, 16)
                v = own(k)[w].astype(f32)
                for b in bufs:
                    v = v + b[w].astype(f32)
                STAGE[w] = v

        def last():
            @pl.when(zz == 0)
            def _():
                total(0, [got(0)])

            @pl.when(zz == 1)
            def _():
                total(1, [got(1), got(1, True)])

            cp = lc(STAGE, SO, lsem.at[5])
            cp.start()
            cp.wait()

        def drain(first=0):
            @pl.loop(first, 8)
            def _(k):
                a_send(k).wait_send()

            @pl.loop(0, 4)
            def _(zp):
                b_send(zp).wait_send()

            for q in range(4):
                if q > 0:
                    pl.when(zz == 0)(lambda: send(q, f_in).wait_send())
                if q >= 2:
                    pl.when(zz == 1)(lambda: send(q, f_in, q == 2).wait_send())
                if q == 0:
                    pl.when(zz == 1)(lambda: send(q, f_out).wait_send())

        return a_send, far, step, last, drain

    R1 = reducer(
        0, lambda k: RING.at[k % 3], lambda k: L1.at[k], lambda k: A1.at[k], lambda k: B1.at[k],
        lambda k: C1.at[k], C1.at[4], SO1,
    )
    R2 = reducer(
        1,
        lambda k: BG.at[ds(128 * (2 * k + 1 - c), 128)],
        lambda k: BG.at[ds(128 * (2 * k + c), 128)],
        lambda k: X.at[ds(128 * k, 128)],
        lambda k: X.at[ds(1024 + 128 * k, 128)],
        lambda k: X.at[ds(1536 + 128 * k, 128)],
        C2X,
        SO2,
    )

    @pl.loop(0, 8)
    def _(b):
        res = mm(INNER[ds(256 * b, 256)], WOS[...], 1, 0)

        @pl.when(b >= 3)
        def _():
            R1[0](b - 3).wait_send()

        for side in range(2):
            @pl.when(c == side)
            def _():
                L1[b] = res[128 * side : 128 * side + 128].astype(bf)
                RING[b % 3] = res[128 - 128 * side : 256 - 128 * side].astype(bf)

        R1[0](b).start()

    own_b.wait()
    gf()

    half = ds(320 * r, 320)
    away = ds(320 * (1 - r), 320)

    def o1(j):
        return rc(OSB.at[j, away], ROS.at[j], so.at[j], ro.at[j], xp)

    def o2(j):
        return rc(OSB.at[j, half], OSo.at[half, ds(512 * j, 512)], so2.at[j], ro2.at[j], xp)

    def o2r(j):
        return rc(OSB.at[j, half], OSo.at[away, ds(512 * j, 512)], so2.at[j], ro2.at[j], xp)

    def os_store(j):
        return lc(OSB.at[j, half], OSo.at[half, ds(512 * j, 512)], lsem.at[6 + j])

    def os_step(j):
        o1(j).wait_recv()
        add_into(OSB.at[j, half], ROS.at[j], 320)
        o2(j).start()
        os_store(j).start()

    def os_drain():
        for j in range(4):
            o1(j).wait_send()
            o2(j).wait_send()
            o2r(j).wait_recv()
            os_store(j).wait()

    @pl.loop(0, 4)
    def _(j):
        OSB[j] = mm(INNER[...], BG[:, ds(512 * j, 512)], 0, 0).astype(bf)
        o1(j).start()

    R1[1]()

    GBR[...] = jnp.zeros_like(GBR)
    VEC[...] = jnp.zeros_like(VEC)
    TOT[...] = jnp.zeros_like(TOT)
    mine = BG[:, ds(128 * f, 128)].astype(f32)
    BSUM[...] = jnp.sum(mine, 0, keepdims=True)

    def fold_rows(v, rows):
        return jnp.sum(v.reshape(rows // 8, 8, v.shape[-1]), 0)

    @pl.loop(0, 4)
    def _(i):
        rows = ds(512 * i, 512)
        T1[:, pl.ds(0, 640)] = mm(BG[rows], WOS[...], 1, 1)

        @pl.loop(0, 32, unroll=2)
        def _(k):
            w = ds(16 * k, 16)
            gw = ds(512 * i + 16 * k, 16)
            INNER[gw, pl.ds(0, 128)] = T1[w, pl.ds(0, 128)].astype(bf)
            e = (T1[w, pl.ds(128, 512)] * SLOPE[gw].astype(f32)).astype(bf)
            SLOPE[gw] = e
            GBR[:, pl.ds(384, 512)] += fold(e.astype(f32))

    os_step(0)
    R1[2](3)
    os_step(1)
    R1[2](0)

    lane_b = lax.broadcasted_iota(jnp.int32, (128, 128), 1)

    @pl.loop(0, 16, unroll=2)
    def _(i):
        rows = ds(128 * i, 128)
        q = QKV[rows, pl.ds(0, 128)]
        k = QKV[rows, pl.ds(128, 128)]
        v = QKV[rows, pl.ds(256, 128)]
        p = PR[rows]
        mg = INNER[rows, pl.ds(0, 128)]
        vg = mm(p.astype(bf), mg, 0, 0)
        pg = mm(mg, v, 1, 1)
        sgr = (p * (pg - jnp.sum(pg * p, -1, keepdims=True))).astype(bf)
        cos, sin = CT[rows], ST[rows]
        qg = mm(sgr, k, 1, 0) * scale
        kg = mm(sgr, q, 0, 0) * scale
        for t, g in enumerate((qg, kg, vg)):
            if t < 2:
                g = g * cos - swap(g, lane_b) * sin
            g = g.astype(bf)
            l = pl.ds(128 * t, 128)
            QKV[rows, l] = g
            GBR[:, l] += fold_rows(g.astype(f32), 128)

    os_step(2)
    R1[2](2)
    os_step(3)
    R1[2](1)
    GBR[...] = jnp.broadcast_to(jnp.sum(GBR[...], 0, keepdims=True), GBR.shape)

    keep = ds(64 * r, 64)
    give = ds(64 * (1 - r), 64)

    def x1(g):
        return rc(JB.at[ds(4 * g, 4), give], RX.at[ds(4 * g, 4)], sx.at[g], rxx.at[g], xp)

    def place_of(fs, t, rows):
        if t < 3:
            return JWo.at[rows, ds(2048 * t + 128 * fs, 128)]
        return EWo.at[rows, ds(512 * fs, 512)]

    def piece_of(fd, t):
        return JB.at[fd, keep, pl.ds(128 * t, 128)] if t < 3 else JB.at[fd, keep, pl.ds(384, 512)]

    def je_group(g):
        x1(g).wait_recv()

        @pl.loop(0, 4)
        def _(j):
            fd = 4 * g + j
            add_into(JB.at[fd, keep], RX.at[fd], 64)

            @pl.when(fd != f)
            def _():
                for t in range(4):
                    rc(piece_of(fd, t), place_of(f, t, keep), sg.at[fd, t], rg.at[f, t], (r, fd)).start()

            @pl.when(fd == f)
            def _():
                for t in range(4):
                    lc(piece_of(fd, t), place_of(f, t, keep), sg.at[fd, t]).start()
                    rc(piece_of(fd, t), place_of(f, t, keep), sf.at[fd, t], rf.at[f, t], xp).start()

    def fwd_group(g):
        @pl.loop(4 * g, 4 * g + 4)
        def _(fs):
            @pl.when(fs != f)
            def _():
                for t in range(4):
                    d = place_of(fs, t, keep)
                    rc(d, d, sg.at[fs, t], rg.at[fs, t], xp).wait_recv()
                    rc(d, d, sf.at[fs, t], rf.at[fs, t], xp).start()

    def je_drain():
        for g in range(4):
            x1(g).wait_send()

        @pl.loop(0, 16)
        def _(fs):
            for t in range(4):
                d = place_of(fs, t, give)
                cp = rc(d, d, sf.at[fs, t], rf.at[fs, t], xp)
                cp.wait_recv()
                cp.wait_send()

            @pl.when(fs != f)
            def _():
                for t in range(4):
                    rc(piece_of(fs, t), place_of(f, t, keep), sg.at[fs, t], rg.at[f, t], xp).wait_send()

            @pl.when(fs == f)
            def _():
                for t in range(4):
                    lc(piece_of(fs, t), place_of(f, t, keep), sg.at[fs, t]).wait()

    @pl.loop(0, 4)
    def _(i):
        left = X[:, ds(512 * i, 512)]
        T1[:, pl.ds(0, 384)] = mm(left, QKV[...], 0, 0)
        T1[:, pl.ds(384, 512)] = mm(left, SLOPE[...], 0, 0)

        @pl.loop(0, 4)
        def _(s):
            j = 4 * i + s
            columns(j)

            @pl.loop(0, 8)
            def _(k):
                w = ds(128 * s + 16 * k, 16)
                gw = ds(128 * j + 16 * k, 16)
                cw = ds(16 * k, 16)
                for b, (first, count, W) in enumerate(((0, 3, WJ), (384, 4, WE))):
                    g, sh = COL[2 * b, cw], COL[2 * b + 1, cw]
                    a1 = jnp.zeros((16, 128), f32)
                    a2 = jnp.zeros((16, 128), f32)
                    for t in range(count):
                        l = pl.ds(first + 128 * t, 128)
                        m = T1[w, l]
                        bias = GBR[0:1, l]
                        JB[j, cw, l] = (g * m + sh * bias).astype(bf)
                        wt = W[gw, pl.ds(128 * t, 128)].astype(f32)
                        a1 = a1 + wt * m
                        a2 = a2 + wt * bias
                    VC[2 * b, cw] = jnp.sum(a1, -1, keepdims=True) / g
                    VC[2 * b + 1, cw] = jnp.sum(a2, -1, keepdims=True) / g

            for v in range(4):
                VEC[j, pl.ds(v, 1)] = VC[v].T[0:1]

        x1(i).start()

    def tile(fd, src):
        return rc(VEC.at[fd], VR.at[src], sv.at[fd], rv.at[src], (r, fd))

    for t in range(3):
        VEC[(16 * t + f) // 3, pl.ds(4 + (16 * t + f) % 3, 1)] = GBR[0:1, pl.ds(128 * t, 128)]
    TOT[pl.ds(7, 1)] = BSUM[...]
    for t in range(4):
        TOT[pl.ds(8 + t, 1)] = GBR[0:1, pl.ds(384 + 128 * t, 128)]

    @pl.loop(1, 16)
    def _(k):
        tile((f + k) % 16, f).start()

    VR[f] = VEC[f]
    R1[3]()

    for dev in (sib, yp, f_in):
        pl.semaphore_signal(ready, inc=1, device_id=dev, device_id_type=MESH)

    @pl.when(zz == 1)
    def _():
        pl.semaphore_signal(ready, inc=1, device_id=f_out, device_id_type=MESH)
        pl.semaphore_wait(ready, 4)

    @pl.when(zz == 0)
    def _():
        pl.semaphore_wait(ready, 3)

    @pl.loop(0, 8)
    def _(b):
        rows = ds(256 * b, 256)
        BG[rows] = (mm(QKV[rows], WJ[...], 1, 1) + mm(SLOPE[rows], WE[...], 1, 1)).astype(bf)
        R2[0](b).start()

    def total_rep():
        return rc(TOT, TX, st_, rt_, xp)

    @pl.loop(1, 16)
    def _(k):
        tile(f, (f + k) % 16).wait_recv()

    TOT[pl.ds(0, 7)] = jnp.sum(VR[...], 0)[0:7]
    total_rep().start()
    je_group(0)
    je_group(1)
    R2[1]()
    je_group(2)
    je_group(3)
    R2[2](3)
    fwd_group(0)
    R2[2](0)
    fwd_group(1)
    R2[2](2)
    fwd_group(2)
    R2[2](1)
    fwd_group(3)
    R2[3]()
    R1[4](5)
    R2[4]()
    send_small.wait()

    @pl.loop(1, 16)
    def _(k):
        fd = (f + k) % 16
        for t, (s, d) in enumerate(wpieces(f, fd, True)):
            rc(s, d, sw.at[fd, t], rw.at[f, t], (r, fd)).wait_send()

    @pl.loop(1, 16)
    def _(k):
        tile((f + k) % 16, f).wait_send()

    total_rep().wait_recv()
    total_rep().wait_send()
    FIN[...] = TOT[...] + TX[...]
    os_drain()
    je_drain()


def layer_call(x, bg, sm, jw, ew, wo, ws, ct, st, eb):
    S = jax.ShapeDtypeStruct
    D = pltpu.SemaphoreType.DMA
    V = pltpu.VMEM
    hbm = pl.BlockSpec(memory_space=pl.ANY)
    vm = pl.BlockSpec(memory_space=pltpu.VMEM)
    return pl.pallas_call(
        layer_kernel,
        out_shape=(
            S((128, WIDE), f32), S((128, WIDE), f32), S((640, WIDE), bf), S((128, 3 * WIDE), bf),
            S((128, 4 * WIDE), bf), S((16, 128), f32), S((256, 128), f32),
        ),
        in_specs=[hbm] * 7 + [vm] * 3,
        out_specs=(hbm, hbm, hbm, hbm, hbm, vm, hbm),
        scratch_shapes=[
            V((TOK, WIDE), bf), V((TOK, WIDE), bf), V((WIDE, 384), bf), V((WIDE, 512), bf), V((640, WIDE), bf),
            V((TOK, 640), bf), V((TOK, 384), bf), V((TOK, 512), bf), V((TOK, 128), f32), V((TOK, 128), f32),
            V((TOK, 128), f32), V((8, 128, WIDE), bf), V((3, 128, WIDE), bf), V((8, 128, WIDE), bf),
            V((4, 128, WIDE), bf), V((5, 128, WIDE), bf), V((128, WIDE), bf),
            V((16, 128, 896), bf), V((16, 64, 896), bf), V((4, 640, 512), bf), V((4, 320, 512), bf),
            V((128, WIDE), f32), V((512, 896), f32), V((16, 16, 128), bf), V((256, 128), f32),
            V((8, 896), f32), V((8, 896), f32), V((4, 128, 128), f32), V((4, 128, 128), f32),
            V((16, 8, 128), f32), V((16, 8, 128), f32), V((16, 128), f32), V((16, 128), f32), V((1, 128), f32),
        ]
        + [D((16,))] * 10 + [D((16, 4))] * 4 + [D((16,))] * 2
        + [D((2, 8))] * 2 + [D((2, 4))] * 3 + [D((2, 5))] + [D((4,))] * 6 + [D((16, 4))] * 4
        + [D((16,))] * 2 + [D, D] + [D((12,)), pltpu.SemaphoreType.REGULAR],
        compiler_params=pltpu.CompilerParams(
            collective_id=0, has_side_effects=True, vmem_limit_bytes=67043328
        ),
    )(x, bg, sm, jw, ew, wo, ws, ct, st, eb)


def wide(a):
    return a.astype(f32)


def turn_tables(length):
    place = np.arange(length, dtype=np.float32)[:, None]
    power = np.arange(ROT // 2, dtype=np.float32) * np.float32(2.0) / np.float32(ROT)
    angle = place * np.power(np.float32(rotary_base), -power)
    cosine, sine = (np.cos(angle), np.sin(angle))
    rest = HEAD_DIM - ROT
    ct = np.concatenate([cosine, cosine, np.ones((length, rest))], 1)
    st = np.concatenate([-sine, sine, np.zeros((length, rest))], 1)
    return (jnp.asarray(ct, f32), jnp.asarray(st, f32))


def head_body(
    n,
    layer_input,
    segment,
    live_mask,
    attention_gain,
    attention_shift,
    joined_weight,
    joined_bias,
    output_weight,
    output_bias,
    feedforward_gain,
    feedforward_shift,
    expand_weight,
    expand_bias,
    shrink_weight,
    shrink_bias,
    cotangent,
):
    own, width = layer_input.shape
    part = width // n
    live_rows = wide(live_mask[0])[:, None]
    seeds = wide(cotangent)
    branch_own = (live_rows * seeds).astype(bf)
    seg = segment[0]
    places = jnp.arange(own, dtype=jnp.int32)
    earlier = jnp.sum((seg[None, :] < seg[:, None]).astype(jnp.int32), -1)
    lines = (
        attention_gain.reshape(1, part),
        attention_shift.reshape(1, part),
        feedforward_gain.reshape(1, part),
        feedforward_shift.reshape(1, part),
        output_bias.reshape(1, part),
        shrink_bias.reshape(1, part),
        joined_bias.reshape(3, part),
        segment.astype(bf),
        (places - earlier).astype(bf).reshape(1, own),
    )
    row = lax.broadcasted_iota(jnp.int32, (16, 128), 0)
    small = jnp.zeros((16, 128), bf)
    at = 0
    for item in lines:
        for k in range(item.shape[0]):
            small = jnp.where(row == at, item[k : k + 1], small)
            at += 1
    ct, st = turn_tables(own)
    summed, hat_own, os_grad, joined_grad, expand_grad, sums, small_all = layer_call(
        layer_input, branch_own, small, joined_weight, expand_weight, output_weight, shrink_weight,
        ct, st, wide(expand_bias).reshape(1, -1),
    )
    small_all = small_all.reshape(n, 16, part)
    bias = (small_all[:, 4] + small_all[:, 5]).reshape(width)
    rows_own = wide(layer_input)
    layer_output = (rows_own + live_rows * (summed + bias)).astype(bf)
    centred = rows_own - jnp.mean(rows_own, -1, keepdims=True)
    inverse = lax.rsqrt(jnp.mean(centred * centred, -1, keepdims=True) + epsilon)
    normalized = centred * inverse
    row_grad = inverse * (
        hat_own
        - jnp.mean(hat_own, -1, keepdims=True)
        - normalized * jnp.mean(hat_own * normalized, -1, keepdims=True)
    )
    input_grad = (seeds + row_grad).astype(bf)

    os_grad = wide(os_grad)
    return (
        layer_output,
        input_grad,
        sums[0],
        sums[1],
        wide(joined_grad),
        sums[4:7].reshape(-1),
        os_grad[:part],
        sums[7],
        sums[2],
        sums[3],
        wide(expand_grad),
        sums[8:12].reshape(-1),
        os_grad[part:],
        sums[7],
    )


def solution(mesh):
    n = mesh.shape["fsdp"]
    fits = n == HEADS and mesh.shape["rep"] == 2
    chosen = functools.partial(head_body, n) if fits else body
    placed = (
        P(("rep", "fsdp"), None),
        P(("rep", "fsdp"), None),
        P(("rep", "fsdp"), None),
        P("fsdp"),
        P("fsdp"),
        P("fsdp", None),
        P("fsdp"),
        P("fsdp", None),
        P("fsdp"),
        P("fsdp"),
        P("fsdp"),
        P("fsdp", None),
        P("fsdp"),
        P("fsdp", None),
        P("fsdp"),
        P(("rep", "fsdp"), None),
    )
    return jax.shard_map(
        chosen,
        mesh=mesh,
        in_specs=placed,
        out_specs=(
            P(("rep", "fsdp"), None),
            P(("rep", "fsdp"), None),
            P("fsdp"),
            P("fsdp"),
            P("fsdp", None),
            P("fsdp"),
            P("fsdp", None),
            P("fsdp"),
            P("fsdp"),
            P("fsdp"),
            P("fsdp", None),
            P("fsdp"),
            P("fsdp", None),
            P("fsdp"),
        ),
        check_vma=False,
    )
```

```python
import functools

import jax
import jax.numpy as jnp
import numpy as np
from jax import lax
from jax.experimental import pallas as pl
from jax.experimental.pallas import tpu as pltpu
from jax.sharding import PartitionSpec as P

D = 2048
HEADS = 16
HEAD_DIM = 128
ROT = 32


epsilon = 1e-05
masked_score = -1e30
rotary_base = 10000.0


def as_sent(shard):
    return jax.tree.map(lambda a: a.astype(jnp.bfloat16) if a.dtype == jnp.float32 else a, shard)


def norm_rows(rows, gain, shift):
    centre = jnp.mean(rows, -1, keepdims=True)
    centred = rows - centre
    inverse = lax.rsqrt(jnp.mean(centred * centred, -1, keepdims=True) + epsilon)
    normalized = centred * inverse
    return (normalized * gain.astype(jnp.float32) + shift.astype(jnp.float32), normalized, inverse)


def norm_back(normed_grad, normalized, inverse, gain):
    scaled = normed_grad * gain.astype(jnp.float32)
    row_grad = inverse * (
        scaled
        - jnp.mean(scaled, -1, keepdims=True)
        - normalized * jnp.mean(scaled * normalized, -1, keepdims=True)
    )
    return (row_grad, jnp.sum(normed_grad * normalized, 0), jnp.sum(normed_grad, 0))


def rotary_tables(segment):
    length = segment.shape[-1]
    places = jnp.arange(length, dtype=jnp.int32)
    earlier = jnp.sum((segment[..., None, :] < segment[..., :, None]).astype(jnp.int32), -1)
    position = (places - earlier).astype(jnp.float32)
    exponent = jnp.arange(ROT // 2, dtype=jnp.float32) * 2.0 / ROT
    frequency = jnp.power(jnp.float32(rotary_base), -exponent)
    angle = position[..., None] * frequency
    return (jnp.cos(angle), jnp.sin(angle))


def turn(heads, cosine, sine, sign):
    half = ROT // 2
    front = heads[..., :half]
    behind = heads[..., half:ROT]
    cos_wide = cosine[..., None, :]
    sin_wide = sine[..., None, :] * sign
    return jnp.concatenate(
        [
            front * cos_wide - behind * sin_wide,
            behind * cos_wide + front * sin_wide,
            heads[..., ROT:],
        ],
        -1,
    )


def gelu_slope(values):
    return (
        0.5 * (1.0 + lax.erf(values * 0.7071067811865476))
        + values * jnp.exp(-0.5 * values * values) * 0.3989422804014327
    )


def attention_inputs(rows, weights, cosine, sine):
    gain, shift, joined_weight, joined_bias = (weights[0], weights[1], weights[2], weights[3])
    normed, normalized, inverse = norm_rows(rows, gain, shift)
    normed_low = normed.astype(jnp.bfloat16)
    joined = jnp.dot(
        normed_low, joined_weight, preferred_element_type=jnp.float32
    ) + joined_bias.astype(jnp.float32)
    length = rows.shape[0]
    split = joined.reshape(length, 3, HEADS, HEAD_DIM)
    queries = turn(split[:, 0], cosine, sine, 1.0).astype(jnp.bfloat16)
    keys = turn(split[:, 1], cosine, sine, 1.0).astype(jnp.bfloat16)
    values = split[:, 2].astype(jnp.bfloat16)
    return (normed_low, normalized, inverse, queries, keys, values)


def score_block(queries, keys, allowed):
    scores = jnp.einsum(
        "thd,shd->hts", queries, keys, preferred_element_type=jnp.float32
    ) * HEAD_DIM ** (-0.5)
    return jnp.where(allowed[None], scores, masked_score)


def feedforward_inputs(rows, weights):
    gain, shift, expand_weight, expand_bias = (weights[0], weights[1], weights[2], weights[3])
    normed, normalized, inverse = norm_rows(rows, gain, shift)
    normed_low = normed.astype(jnp.bfloat16)
    expanded = jnp.dot(
        normed_low, expand_weight, preferred_element_type=jnp.float32
    ) + expand_bias.astype(jnp.float32)
    return (normed_low, normalized, inverse, expanded)


def body(
    layer_input,
    segment,
    live_mask,
    attention_gain,
    attention_shift,
    joined_weight,
    joined_bias,
    output_weight,
    output_bias,
    feedforward_gain,
    feedforward_shift,
    expand_weight,
    expand_bias,
    shrink_weight,
    shrink_bias,
    cotangent,
):
    rows = layer_input.astype(jnp.float32)
    seg_row = segment[0]
    live_rows = live_mask[0].astype(jnp.float32)[:, None]
    length = seg_row.shape[0]
    cosine, sine = rotary_tables(seg_row)
    places = jnp.arange(length, dtype=jnp.int32)
    allowed = (seg_row[:, None] == seg_row[None, :]) & (places[None, :] <= places[:, None])
    attention_parts = (
        attention_gain,
        attention_shift,
        joined_weight,
        joined_bias,
        output_weight,
        output_bias,
    )
    feedforward_parts = (
        feedforward_gain,
        feedforward_shift,
        expand_weight,
        expand_bias,
        shrink_weight,
        shrink_bias,
    )
    attention_full = (
        lax.all_gather(attention_gain, "fsdp", axis=0, tiled=True),
        lax.all_gather(attention_shift, "fsdp", axis=0, tiled=True),
        lax.all_gather(joined_weight, "fsdp", axis=0, tiled=True),
        lax.all_gather(joined_bias, "fsdp", axis=0, tiled=True),
        lax.all_gather(output_weight, "fsdp", axis=0, tiled=True),
        lax.all_gather(output_bias, "fsdp", axis=0, tiled=True),
    )
    feedforward_full = (
        lax.all_gather(feedforward_gain, "fsdp", axis=0, tiled=True),
        lax.all_gather(feedforward_shift, "fsdp", axis=0, tiled=True),
        lax.all_gather(expand_weight, "fsdp", axis=0, tiled=True),
        lax.all_gather(expand_bias, "fsdp", axis=0, tiled=True),
        lax.all_gather(shrink_weight, "fsdp", axis=0, tiled=True),
        lax.all_gather(shrink_bias, "fsdp", axis=0, tiled=True),
    )
    normed_one, normalized_one, inverse_one, queries, keys, values = attention_inputs(
        rows, attention_full, cosine, sine
    )
    scores = score_block(queries, keys, allowed)
    top = jnp.max(scores, -1, keepdims=True)
    expo = jnp.exp(scores - top)
    total = jnp.sum(expo, -1, keepdims=True)
    log_total = top + jnp.log(total)
    probs_low = (expo / total).astype(jnp.bfloat16)
    mixed = jnp.einsum("hts,shd->thd", probs_low, values, preferred_element_type=jnp.float32)
    mixed = mixed.reshape(length, D).astype(jnp.bfloat16)
    attended = jnp.dot(
        mixed, attention_full[4], preferred_element_type=jnp.float32
    ) + attention_full[5].astype(jnp.float32)
    normed_two, normalized_two, inverse_two, expanded = feedforward_inputs(rows, feedforward_full)
    activated = jax.nn.gelu(expanded, approximate=False).astype(jnp.bfloat16)
    shrunk = jnp.dot(
        activated, feedforward_full[4], preferred_element_type=jnp.float32
    ) + feedforward_full[5].astype(jnp.float32)
    layer_output = (rows + live_rows * (attended + shrunk)).astype(jnp.bfloat16)
    seed_rows = cotangent.astype(jnp.float32)
    branch_grad = (live_rows * seed_rows).astype(jnp.bfloat16)
    branch_total = jnp.sum(branch_grad.astype(jnp.float32), 0)
    feedforward_back = lax.all_gather(
        as_sent(lax.optimization_barrier((feedforward_parts, layer_output))[0]),
        "fsdp",
        axis=0,
        tiled=True,
    )
    normed_two, normalized_two, inverse_two, expanded = feedforward_inputs(rows, feedforward_back)
    activated = jax.nn.gelu(expanded, approximate=False).astype(jnp.bfloat16)
    shrink_weight_grad = jnp.einsum(
        "tf,td->fd", activated, branch_grad, preferred_element_type=jnp.float32
    )
    activated_grad = jnp.einsum(
        "td,fd->tf", branch_grad, feedforward_back[4], preferred_element_type=jnp.float32
    )
    expanded_grad = (activated_grad * gelu_slope(expanded)).astype(jnp.bfloat16)
    expand_bias_grad = jnp.sum(expanded_grad.astype(jnp.float32), 0)
    expand_weight_grad = jnp.einsum(
        "td,tf->df", normed_two, expanded_grad, preferred_element_type=jnp.float32
    )
    normed_two_grad = jnp.einsum(
        "tf,df->td", expanded_grad, feedforward_back[2], preferred_element_type=jnp.float32
    )
    rows_grad_two, ff_gain_grad, ff_shift_grad = norm_back(
        normed_two_grad, normalized_two, inverse_two, feedforward_back[0]
    )
    ff_terms = (
        ff_gain_grad,
        ff_shift_grad,
        expand_weight_grad,
        expand_bias_grad,
        shrink_weight_grad,
        branch_total,
    )
    ff_parts = (
        lax.psum_scatter(ff_terms[0], "fsdp", scatter_dimension=0, tiled=True),
        lax.psum_scatter(ff_terms[1], "fsdp", scatter_dimension=0, tiled=True),
        lax.psum_scatter(ff_terms[2], "fsdp", scatter_dimension=0, tiled=True),
        lax.psum_scatter(ff_terms[3], "fsdp", scatter_dimension=0, tiled=True),
        lax.psum_scatter(ff_terms[4], "fsdp", scatter_dimension=0, tiled=True),
        lax.psum_scatter(ff_terms[5], "fsdp", scatter_dimension=0, tiled=True),
    )
    attention_back = lax.all_gather(
        as_sent(lax.optimization_barrier((attention_parts, layer_output))[0]),
        "fsdp",
        axis=0,
        tiled=True,
    )
    normed_one, normalized_one, inverse_one, queries, keys, values = attention_inputs(
        rows, attention_back, cosine, sine
    )
    scores = score_block(queries, keys, allowed)
    probs = jnp.exp(scores - log_total)
    probs_low = probs.astype(jnp.bfloat16)
    mixed = jnp.einsum("hts,shd->thd", probs_low, values, preferred_element_type=jnp.float32)
    mixed = mixed.reshape(length, D).astype(jnp.bfloat16)
    output_weight_grad = jnp.einsum(
        "td,te->de", mixed, branch_grad, preferred_element_type=jnp.float32
    )
    mixed_grad = jnp.einsum(
        "te,de->td", branch_grad, attention_back[4], preferred_element_type=jnp.float32
    )
    mixed_grad = mixed_grad.astype(jnp.bfloat16).reshape(length, HEADS, HEAD_DIM)
    value_grad = jnp.einsum(
        "hts,thd->shd", probs_low, mixed_grad, preferred_element_type=jnp.float32
    )
    probs_grad = jnp.einsum("thd,shd->hts", mixed_grad, values, preferred_element_type=jnp.float32)
    scores_grad = (probs * (probs_grad - jnp.sum(probs_grad * probs, -1, keepdims=True))).astype(
        jnp.bfloat16
    )
    query_grad = jnp.einsum(
        "hts,shd->thd", scores_grad, keys, preferred_element_type=jnp.float32
    ) * HEAD_DIM ** (-0.5)
    key_grad = jnp.einsum(
        "hts,thd->shd", scores_grad, queries, preferred_element_type=jnp.float32
    ) * HEAD_DIM ** (-0.5)
    query_grad = turn(query_grad, cosine, sine, -1.0)
    key_grad = turn(key_grad, cosine, sine, -1.0)
    joined_grad = jnp.concatenate(
        [query_grad.reshape(length, D), key_grad.reshape(length, D), value_grad.reshape(length, D)],
        1,
    ).astype(jnp.bfloat16)
    joined_bias_grad = jnp.sum(joined_grad.astype(jnp.float32), 0)
    joined_weight_grad = jnp.einsum(
        "td,te->de", normed_one, joined_grad, preferred_element_type=jnp.float32
    )
    normed_one_grad = jnp.einsum(
        "te,de->td", joined_grad, attention_back[2], preferred_element_type=jnp.float32
    )
    rows_grad_one, at_gain_grad, at_shift_grad = norm_back(
        normed_one_grad, normalized_one, inverse_one, attention_back[0]
    )
    at_terms = (
        at_gain_grad,
        at_shift_grad,
        joined_weight_grad,
        joined_bias_grad,
        output_weight_grad,
        branch_total,
    )
    at_parts = (
        lax.psum_scatter(at_terms[0], "fsdp", scatter_dimension=0, tiled=True),
        lax.psum_scatter(at_terms[1], "fsdp", scatter_dimension=0, tiled=True),
        lax.psum_scatter(at_terms[2], "fsdp", scatter_dimension=0, tiled=True),
        lax.psum_scatter(at_terms[3], "fsdp", scatter_dimension=0, tiled=True),
        lax.psum_scatter(at_terms[4], "fsdp", scatter_dimension=0, tiled=True),
        lax.psum_scatter(at_terms[5], "fsdp", scatter_dimension=0, tiled=True),
    )
    input_grad = (seed_rows + rows_grad_one + rows_grad_two).astype(jnp.bfloat16)
    summed = (
        lax.psum(at_parts[0].astype(jnp.bfloat16), "rep").astype(jnp.float32),
        lax.psum(at_parts[1].astype(jnp.bfloat16), "rep").astype(jnp.float32),
        lax.psum(at_parts[2].astype(jnp.bfloat16), "rep").astype(jnp.float32),
        lax.psum(at_parts[3].astype(jnp.bfloat16), "rep").astype(jnp.float32),
        lax.psum(at_parts[4].astype(jnp.bfloat16), "rep").astype(jnp.float32),
        lax.psum(at_parts[5].astype(jnp.bfloat16), "rep").astype(jnp.float32),
        lax.psum(ff_parts[0].astype(jnp.bfloat16), "rep").astype(jnp.float32),
        lax.psum(ff_parts[1].astype(jnp.bfloat16), "rep").astype(jnp.float32),
        lax.psum(ff_parts[2].astype(jnp.bfloat16), "rep").astype(jnp.float32),
        lax.psum(ff_parts[3].astype(jnp.bfloat16), "rep").astype(jnp.float32),
        lax.psum(ff_parts[4].astype(jnp.bfloat16), "rep").astype(jnp.float32),
        lax.psum(ff_parts[5].astype(jnp.bfloat16), "rep").astype(jnp.float32),
    )
    return (
        layer_output,
        input_grad,
        summed[0],
        summed[1],
        summed[2],
        summed[3],
        summed[4],
        summed[5],
        summed[6],
        summed[7],
        summed[8],
        summed[9],
        summed[10],
        summed[11],
    )


MESH = pl.DeviceIdType.MESH
bf = jnp.bfloat16
f32 = jnp.float32
WIDE = 2048
TOK = 2048


def ds(start, size):
    return pl.ds(pl.multiple_of(start, size), size)


def mm(a, b, ca, cb):
    return lax.dot_general(a, b, (((ca,), (cb,)), ((), ())), preferred_element_type=f32)


def layer_kernel(
    x_ref, bg_ref, sm_ref, jw_ref, ew_ref, wo_ref, ws_ref, ct_ref, eb_ref,
    SO1, SO2, OSo, JWo, EWo, FIN, SMO,
    X, BG, WJ, WE, WOS, INNER, QKV, SLOPE, CT, PR, L1, RING, A1, B1, C1, A2,
    JB, RX, OSB, ROS, T1, SM, SMF, CV, GBR, VEC, VR, TOT, TX, BSUM,
    su, sd, sy, ss, rx_, bu, bd, by, bs, rb_, sw, rw, sxw, rxw, ssm, rsm,
    sa, ra, sbb, rbb, sc, rc_, sx, rxx, so, ro, so2, ro2, sg, rg, sf, rf, sv, rv, st_, rt_, lsem, ready,
):
    r = lax.axis_index("rep")
    f = lax.axis_index("fsdp")
    z = f // 4
    y = (f // 2) % 2
    c = f % 2
    sib = (r, z * 4 + y * 2 + (1 - c))
    yo = z * 4 + (1 - y) * 2 + c
    yp = (r, yo)
    xp = (1 - r, f)
    lower = z <= 1
    zz = jnp.where(lower, z, 3 - z)

    def phys(q):
        return jnp.where(lower, q, 3 - q)

    f_in = (r, jnp.where(lower, f + 4, f - 4))
    f_out = (r, jnp.where(lower, f - 4, f + 4))

    barrier = pltpu.get_barrier_semaphore()

    @pl.loop(1, 16)
    def _(k):
        pl.semaphore_signal(barrier, inc=1, device_id=(r, (f + k) % 16), device_id_type=MESH)

    pl.semaphore_signal(barrier, inc=1, device_id=xp, device_id_type=MESH)
    pl.semaphore_wait(barrier, 16)

    def rc(src, dst, s, q, dev):
        return pltpu.make_async_remote_copy(
            src_ref=src, dst_ref=dst, send_sem=s, recv_sem=q, device_id=dev, device_id_type=MESH
        )

    def lc(src, dst, s):
        return pltpu.make_async_copy(src, dst, s)

    def gather(own, OUT, su, sd, sy, ss, rr):
        def item(i):
            return OUT.at[ds(128 * i, 128)]

        def up(i, src=None):
            return rc(item(i) if src is None else src, item(i), su.at[i], rr.at[i], (r, f + 4))

        def dn(i, src=None):
            return rc(item(i) if src is None else src, item(i), sd.at[i], rr.at[i], (r, f - 4))

        def ac(i, src=None):
            return rc(item(i) if src is None else src, item(i), sy.at[i], rr.at[i], yp)

        def sb(i, src=None):
            return rc(item(i) if src is None else src, item(i), ss.at[i], rr.at[i], sib)

        def begin_z():
            pl.when(z < 3)(lambda: up(f, own).start())
            pl.when(z > 0)(lambda: dn(f, own).start())

        def begin_y():
            ac(f, own).start()
            sb(f, own).start()

        def step(s):
            @pl.when(z - s >= 0)
            def _():
                i = f - 4 * s
                up(i).wait_recv()
                pl.when(z < 3)(lambda: up(i).start())
                ac(i).start()
                sb(i).start()

            @pl.when(z + s <= 3)
            def _():
                i = f + 4 * s
                dn(i).wait_recv()
                pl.when(z > 0)(lambda: dn(i).start())
                ac(i).start()
                sb(i).start()

        def ystep(s):
            @pl.when(z - s >= 0)
            def _():
                ac(yo - 4 * s).wait_recv()
                sb(yo - 4 * s).start()

            @pl.when((s > 0) & (z + s <= 3))
            def _():
                ac(yo + 4 * s).wait_recv()
                sb(yo + 4 * s).start()

        def landed(q):
            for v in range(2):
                sb(4 * q + 2 * v + 1 - c).wait_recv()

        def finish():
            @pl.loop(0, 8)
            def _(k):
                sb(2 * k + c).wait_send()

            @pl.loop(0, 4)
            def _(k):
                i = k * 4 + y * 2 + c
                ac(i).wait_send()
                pl.when((k <= z) & (z < 3))(lambda: up(i).wait_send())
                pl.when((k >= z) & (z > 0))(lambda: dn(i).wait_send())

        return begin_z, begin_y, step, ystep, landed, finish

    xz, xo, xs, xy, xl, xf = gather(x_ref, X, su, sd, sy, ss, rx_)
    gz, go, gs, gy, gl, gf = gather(bg_ref, BG, bu, bd, by, bs, rb_)

    def wpieces(src, dst, from_arg):
        rows = ds(128 * src + 64 * r, 64)
        out = []
        for t in range(3):
            d = WJ.at[rows, pl.ds(128 * t, 128)]
            out.append((jw_ref.at[ds(64 * r, 64), ds(2048 * t + 128 * dst, 128)] if from_arg else d, d))
        d = WE.at[rows]
        out.append((ew_ref.at[ds(64 * r, 64), ds(512 * dst, 512)] if from_arg else d, d))
        return out

    def fwd(lo, hi):
        @pl.loop(lo, hi)
        def _(k):
            fs = (f + 16 - k) % 16
            for t, (s, d) in enumerate(wpieces(fs, f, False)):
                rc(s, d, sw.at[fs, t], rw.at[fs, t], (r, f)).wait_recv()
                rc(s, d, sxw.at[fs, t], rxw.at[fs, t], xp).start()

    own_x = lc(x_ref, X.at[ds(128 * f, 128)], lsem.at[0])
    own_b = lc(bg_ref, BG.at[ds(128 * f, 128)], lsem.at[1])
    load_o = lc(wo_ref, WOS.at[pl.ds(0, 128)], lsem.at[2])
    load_s = lc(ws_ref, WOS.at[pl.ds(128, 512)], lsem.at[3])
    own_s = lc(sm_ref, SM.at[f], lsem.at[4])
    def wsend(lo, hi):
        @pl.loop(lo, hi)
        def _(k):
            fd = (f + k) % 16
            for t, (s, d) in enumerate(wpieces(f, fd, True)):
                rc(s, d, sw.at[fd, t], rw.at[f, t], (r, fd)).start()

    def ssend():
        @pl.loop(1, 16)
        def _(k):
            fd = (f + k) % 16
            rc(sm_ref, SM.at[f], ssm.at[fd], rsm.at[f], (r, fd)).start()

    def wown():
        for t, (s, d) in enumerate(wpieces(f, f, True)):
            rc(s, d, sxw.at[f, t], rxw.at[f, t], xp).start()
            lc(s, d, rw.at[f, t]).start()

    for cp in (own_x, own_b, load_o, load_s, own_s):
        cp.start()
    ssend()
    wsend(1, 16)
    wown()
    xo()
    xz()
    go()
    fwd(1, 9)
    own_s.wait()

    @pl.loop(1, 16)
    def _(k):
        fs = (f + k) % 16
        other = rc(sm_ref, SM.at[fs], ssm.at[fs], rsm.at[fs], (r, fs))
        other.wait_recv()
        other.wait_send()

    @pl.loop(0, 16)
    def _(i):
        SMF[ds(16 * i, 16)] = SM[i].astype(f32)

    send_small = lc(SMF, SMO, lsem.at[4])
    send_small.start()

    @pl.loop(0, 16)
    def _(i):
        rows = ds(128 * i, 128)
        place = jnp.broadcast_to(SMF[pl.ds(16 * i + 10, 1)], (128, 128)).T
        pick = (place == lax.broadcasted_iota(jnp.int32, (128, 128), 1).astype(f32)).astype(f32)
        hi = lax.Precision.HIGHEST
        CT[rows] = jnp.dot(pick, ct_ref[...], precision=hi, preferred_element_type=f32)

    fwd(9, 16)
    xs(1)

    for t, (s, d) in enumerate(wpieces(f, f, True)):
        lc(s, d, rw.at[f, t]).wait()
    other_half = lambda src: ds(128 * src + 64 * (1 - r), 64)

    @pl.loop(0, 16)
    def _(fs):
        for t in range(4):
            d = WJ.at[other_half(fs), pl.ds(128 * t, 128)] if t < 3 else WE.at[other_half(fs)]
            cp = rc(d, d, sxw.at[fs, t], rxw.at[fs, t], xp)
            cp.wait_recv()
            cp.wait_send()

    load_o.wait()
    load_s.wait()

    def columns(j):
        for v in range(4):
            PR[pl.ds(128 * v, 128)] = jnp.broadcast_to(SMF[pl.ds(16 * j + v, 1)], (128, 128)).T

    def fold(v):
        return v[:8] + v[8:]

    CV[...] = jnp.zeros_like(CV)

    @pl.loop(0, 16)
    def _(j):
        columns(j)

        @pl.loop(0, 8)
        def _(k):
            w = ds(128 * j + 16 * k, 16)
            cw = ds(16 * k, 16)
            g1, s1, g2, s2 = (PR[ds(128 * v + 16 * k, 16)] for v in range(4))
            for t in range(3):
                l = pl.ds(128 * t, 128)
                v = WJ[w, l].astype(f32)
                CV[:, l] += fold(v * s1)
                WJ[w, l] = (v * g1).astype(bf)
            for t in range(4):
                l = pl.ds(128 * t, 128)
                lo = pl.ds(384 + 128 * t, 128)
                v = WE[w, l].astype(f32)
                CV[:, lo] += fold(v * s2)
                WE[w, l] = (v * g2).astype(bf)

    CV[...] = jnp.broadcast_to(jnp.sum(CV[...], 0, keepdims=True), CV.shape)
    for t in range(3):
        place = (16 * t + f) // 3 * 16 + 6 + (16 * t + f) % 3
        CV[:, pl.ds(128 * t, 128)] += SMF[pl.ds(place, 1)]
    CV[:, pl.ds(384, 512)] += eb_ref[...]

    lane = lax.broadcasted_iota(jnp.int32, (16, 128), 1)

    def angles(v, ln):
        return jnp.where(ln < 32, v, 1.0), jnp.where(ln < 32, pltpu.roll(v, 96, 1), 0.0)

    def swap(v, ln):
        return jnp.where(ln < 16, pltpu.roll(v, 112, 1), pltpu.roll(v, 16, 1))

    scale = HEAD_DIM ** (-0.5)
    down = lax.broadcasted_iota(jnp.int32, (128, 128), 0)
    across = lax.broadcasted_iota(jnp.int32, (128, 128), 1)

    own_x.wait()

    @pl.loop(0, 4)
    def _(p):
        i = phys(jnp.where((zz == 1) & (p < 2), 1 - p, p))
        rows = ds(512 * i, 512)
        pl.when((p > 0) & (p < 3))(lambda: xs(p + 1))
        @pl.when(p == 1)
        def _():
            gz()

        xy(p)
        xl(i)
        T1[:, pl.ds(0, 384)] = mm(X[rows], WJ[...], 1, 0)
        T1[:, pl.ds(384, 512)] = mm(X[rows], WE[...], 1, 0)

        @pl.loop(0, 32, unroll=2)
        def _(k):
            w = ds(16 * k, 16)
            gw = ds(512 * i + 16 * k, 16)
            cos, sin = angles(CT[gw], lane)
            for t in range(2):
                l = pl.ds(128 * t, 128)
                v = T1[w, l] + CV[0:1, l]
                QKV[gw, l] = (v * cos + swap(v, lane) * sin).astype(bf)
            l = pl.ds(256, 128)
            QKV[gw, l] = (T1[w, l] + CV[0:1, l]).astype(bf)
            for t in range(4):
                l = pl.ds(384 + 128 * t, 128)
                v = T1[w, l] + CV[0:1, l]
                part = 0.5 * (1.0 + lax.erf(v * 0.7071067811865476))
                INNER[gw, pl.ds(128 + 128 * t, 128)] = (v * part).astype(bf)
                SLOPE[gw, pl.ds(128 * t, 128)] = (
                    part + v * jnp.exp(-0.5 * v * v) * 0.3989422804014327
                ).astype(bf)

        @pl.loop(0, 4, unroll=2)
        def _(j):
            slot = 4 * i + j
            rows = ds(128 * slot, 128)
            q = QKV[rows, pl.ds(0, 128)]
            k = QKV[rows, pl.ds(128, 128)]
            v = QKV[rows, pl.ds(256, 128)]
            seg = jnp.broadcast_to(SMF[pl.ds(16 * slot + 9, 1)], (128, 128))
            s = mm(q, k, 1, 1) * scale
            s = jnp.where((seg == seg.T) & (across <= down), s, masked_score)
            e = jnp.exp(s - jnp.max(s, -1, keepdims=True))
            p = e / jnp.sum(e, -1, keepdims=True)
            PR[rows] = p
            INNER[rows, pl.ds(0, 128)] = mm(p.astype(bf), v, 1, 0).astype(bf)

        @pl.when(p == 2)
        def _():
            gs(1)
            gy(0)

        @pl.when(p == 3)
        def _():
            gs(2)
            gy(1)


    xf()

    def add_into(dst, src, rows):
        @pl.loop(0, rows // 16)
        def _(i):
            w = ds(i * 16, 16)
            dst[w] = (dst[w].astype(f32) + src[w].astype(f32)).astype(bf)

    def reducer(n, sent, own, AA, BB, CC, CX, SO):
        def a_send(k):
            return rc(sent(k), AA(k), sa.at[n, k], ra.at[n, k], sib)

        def b_send(zp):
            return rc(own(zp * 2 + 1 - y), BB(zp), sbb.at[n, zp], rbb.at[n, zp], yp)

        def prep(k):
            a_send(k).wait_recv()
            add_into(own(k), AA(k), 128)

        def far(*turns):
            for q in turns or (3, 0, 2, 1):
                prep(phys(q) * 2 + 1 - y)
                b_send(phys(q)).start()

        def near(q):
            zp = phys(q)
            k = zp * 2 + y
            prep(k)
            b_send(zp).wait_recv()
            add_into(own(k), BB(zp), 128)

        def got(q, extra=False):
            zp = phys(q)
            buf = CX if extra else CC(zp)
            slot = 4 if extra else zp
            rc(buf, buf, sc.at[n, zp], rc_.at[n, slot], f_in).wait_recv()
            return buf

        def send(q, dev, extra=False):
            zp = phys(q)
            return rc(
                own(zp * 2 + y), CX if extra else CC(zp), sc.at[n, zp], rc_.at[n, 4 if extra else zp], dev
            )

        def step(q):
            near(q)
            if q > 0:
                pl.when(zz == 0)(lambda: send(q, f_in).start())

        def relay(q):
            k = phys(q) * 2 + y

            @pl.when(zz == 1)
            def _():
                if q >= 2:
                    add_into(own(k), got(q), 128)
                    send(q, f_in, q == 2).start()
                if q == 0:
                    add_into(own(k), got(q), 128)
                    send(q, f_out).start()

        def total(q, bufs):
            k = phys(q) * 2 + y

            @pl.loop(0, 8)
            def _(i):
                w = ds(i * 16, 16)
                v = own(k)[w].astype(f32)
                for b in bufs:
                    v = v + b[w].astype(f32)
                for l, n in enumerate((896, 896, 256)):
                    T1[ds(128 * l + 16 * i, 16), pl.ds(0, n)] = v[:, 896 * l : 896 * l + n]

        def last():
            @pl.when(zz == 0)
            def _():
                total(0, [got(0)])

            @pl.when(zz == 1)
            def _():
                total(1, [got(1), got(1, True)])

            cps = [
                lc(T1.at[pl.ds(128 * l, 128), pl.ds(0, n)], SO.at[:, pl.ds(896 * l, n)], lsem.at[at])
                for l, n, at in ((0, 896, 5), (1, 896, 10), (2, 256, 11))
            ]
            for cp in cps:
                cp.start()
            for cp in cps:
                cp.wait()

        def drain(first=0):
            @pl.loop(first, 8)
            def _(k):
                a_send(k).wait_send()

            @pl.loop(0, 4)
            def _(zp):
                b_send(zp).wait_send()

            for q in range(4):
                if q > 0:
                    pl.when(zz == 0)(lambda: send(q, f_in).wait_send())
                if q >= 2:
                    pl.when(zz == 1)(lambda: send(q, f_in, q == 2).wait_send())
                if q == 0:
                    pl.when(zz == 1)(lambda: send(q, f_out).wait_send())

        return a_send, far, step, last, drain, relay

    R1 = reducer(
        0, lambda k: RING.at[k % 3], lambda k: L1.at[k], lambda k: A1.at[k], lambda k: B1.at[k],
        lambda k: C1.at[k], C1.at[4], SO1,
    )
    R2 = reducer(
        1,
        lambda k: BG.at[ds(128 * (2 * k + 1 - c), 128)],
        lambda k: BG.at[ds(128 * (2 * k + c), 128)],
        lambda k: A2.at[k],
        lambda k: RING.at[k],
        lambda k: WOS.at[ds(128 * k, 128)],
        WOS.at[pl.ds(512, 128)],
        SO2,
    )

    @pl.loop(0, 8)
    def _(b):
        res = mm(INNER[ds(256 * b, 256)], WOS[...], 1, 0)

        @pl.when(b >= 3)
        def _():
            R1[0](b - 3).wait_send()

        for side in range(2):
            @pl.when(c == side)
            def _():
                L1[b] = res[128 * side : 128 * side + 128].astype(bf)
                RING[b % 3] = res[128 - 128 * side : 256 - 128 * side].astype(bf)

        R1[0](b).start()

        @pl.when(b == 2)
        def _():
            gs(3)
            gy(2)

    gy(3)
    own_b.wait()
    for q in range(4):
        gl(q)
    gf()

    half = ds(320 * r, 320)
    away = ds(320 * (1 - r), 320)

    def o1(j):
        return rc(OSB.at[j, away], ROS.at[j], so.at[j], ro.at[j], xp)

    def o2(j):
        return rc(OSB.at[j, half], OSo.at[half, ds(512 * j, 512)], so2.at[j], ro2.at[j], xp)

    def o2r(j):
        return rc(OSB.at[j, half], OSo.at[away, ds(512 * j, 512)], so2.at[j], ro2.at[j], xp)

    def os_store(j):
        return lc(OSB.at[j, half], OSo.at[half, ds(512 * j, 512)], lsem.at[6 + j])

    def os_step(j):
        o1(j).wait_recv()
        add_into(OSB.at[j, half], ROS.at[j], 320)
        o2(j).start()
        os_store(j).start()

    def os_drain():
        for j in range(4):
            o1(j).wait_send()
            o2(j).wait_send()
            o2r(j).wait_recv()
            os_store(j).wait()

    @pl.loop(0, 4)
    def _(j):
        OSB[j] = mm(INNER[...], BG[:, ds(512 * j, 512)], 0, 0).astype(bf)
        o1(j).start()

    R1[1]()

    GBR[...] = jnp.zeros_like(GBR)
    VEC[...] = jnp.zeros_like(VEC)
    TOT[...] = jnp.zeros_like(TOT)
    mine = BG[:, ds(128 * f, 128)].astype(f32)
    BSUM[...] = jnp.sum(mine, 0, keepdims=True)

    def fold_rows(v, rows):
        return jnp.sum(v.reshape(rows // 8, 8, v.shape[-1]), 0)

    @pl.loop(0, 4)
    def _(i):
        rows = ds(512 * i, 512)
        T1[:, pl.ds(0, 640)] = mm(BG[rows], WOS[...], 1, 1)

        @pl.loop(0, 32, unroll=2)
        def _(k):
            w = ds(16 * k, 16)
            gw = ds(512 * i + 16 * k, 16)
            INNER[gw, pl.ds(0, 128)] = T1[w, pl.ds(0, 128)].astype(bf)
            e = (T1[w, pl.ds(128, 512)] * SLOPE[gw].astype(f32)).astype(bf)
            SLOPE[gw] = e
            GBR[:, pl.ds(384, 512)] += fold(e.astype(f32))

    @pl.loop(5, 8)
    def _(b):
        R1[0](b).wait_send()

    for dev in (sib, yp, f_in):
        pl.semaphore_signal(ready, inc=1, device_id=dev, device_id_type=MESH)

    @pl.when(zz == 1)
    def _():
        pl.semaphore_signal(ready, inc=1, device_id=f_out, device_id_type=MESH)

    os_step(0)
    os_step(1)

    lane_b = lax.broadcasted_iota(jnp.int32, (128, 128), 1)

    @pl.loop(0, 16, unroll=2)
    def _(i):
        rows = ds(128 * i, 128)
        q = QKV[rows, pl.ds(0, 128)]
        k = QKV[rows, pl.ds(128, 128)]
        v = QKV[rows, pl.ds(256, 128)]
        p = PR[rows]
        mg = INNER[rows, pl.ds(0, 128)]
        vg = mm(p.astype(bf), mg, 0, 0)
        pg = mm(mg, v, 1, 1)
        sgr = (p * (pg - jnp.sum(pg * p, -1, keepdims=True))).astype(bf)
        cos, sin = angles(CT[rows], lane_b)
        qg = mm(sgr, k, 1, 0) * scale
        kg = mm(sgr, q, 0, 0) * scale
        for t, g in enumerate((qg, kg, vg)):
            if t < 2:
                g = g * cos - swap(g, lane_b) * sin
            g = g.astype(bf)
            l = pl.ds(128 * t, 128)
            QKV[rows, l] = g
            GBR[:, l] += fold_rows(g.astype(f32), 128)

    os_step(2)
    os_step(3)
    GBR[...] = jnp.broadcast_to(jnp.sum(GBR[...], 0, keepdims=True), GBR.shape)

    keep = ds(64 * r, 64)
    give = ds(64 * (1 - r), 64)

    def x1(g):
        return rc(JB.at[ds(4 * g, 4), give], RX.at[ds(4 * g, 4)], sx.at[g], rxx.at[g], xp)

    def place_of(fs, t, rows):
        if t < 3:
            return JWo.at[rows, ds(2048 * t + 128 * fs, 128)]
        return EWo.at[rows, ds(512 * fs, 512)]

    def piece_of(fd, t):
        return JB.at[fd, keep, pl.ds(128 * t, 128)] if t < 3 else JB.at[fd, keep, pl.ds(384, 512)]

    def je_group(g):
        x1(g).wait_recv()

        @pl.loop(0, 4)
        def _(j):
            fd = 4 * g + j
            add_into(JB.at[fd, keep], RX.at[fd], 64)

            @pl.when(fd != f)
            def _():
                for t in range(4):
                    rc(piece_of(fd, t), place_of(f, t, keep), sg.at[fd, t], rg.at[f, t], (r, fd)).start()

            @pl.when(fd == f)
            def _():
                for t in range(4):
                    lc(piece_of(fd, t), place_of(f, t, keep), sg.at[fd, t]).start()
                    rc(piece_of(fd, t), place_of(f, t, keep), sf.at[fd, t], rf.at[f, t], xp).start()

    def fwd_group(g):
        @pl.loop(4 * g, 4 * g + 4)
        def _(fs):
            @pl.when(fs != f)
            def _():
                for t in range(4):
                    d = place_of(fs, t, keep)
                    rc(d, d, sg.at[fs, t], rg.at[fs, t], xp).wait_recv()
                    rc(d, d, sf.at[fs, t], rf.at[fs, t], xp).start()

    def je_drain():
        for g in range(4):
            x1(g).wait_send()

        @pl.loop(0, 16)
        def _(fs):
            for t in range(4):
                d = place_of(fs, t, give)
                cp = rc(d, d, sf.at[fs, t], rf.at[fs, t], xp)
                cp.wait_recv()
                cp.wait_send()

            @pl.when(fs != f)
            def _():
                for t in range(4):
                    rc(piece_of(fs, t), place_of(f, t, keep), sg.at[fs, t], rg.at[f, t], xp).wait_send()

            @pl.when(fs == f)
            def _():
                for t in range(4):
                    lc(piece_of(fs, t), place_of(f, t, keep), sg.at[fs, t]).wait()

    @pl.when(zz == 1)
    def _():
        pl.semaphore_wait(ready, 4)

    @pl.when(zz == 0)
    def _():
        pl.semaphore_wait(ready, 3)


    @pl.loop(0, 4)
    def _(i):
        left = X[:, ds(512 * i, 512)]
        T1[:, pl.ds(0, 384)] = mm(left, QKV[...], 0, 0)
        T1[:, pl.ds(384, 512)] = mm(left, SLOPE[...], 0, 0)

        @pl.loop(0, 4)
        def _(s):
            j = 4 * i + s
            columns(j)

            @pl.loop(0, 8)
            def _(k):
                w = ds(128 * s + 16 * k, 16)
                gw = ds(128 * j + 16 * k, 16)
                cw = ds(16 * k, 16)
                for b, (first, count, W) in enumerate(((0, 3, WJ), (384, 4, WE))):
                    g, sh = (PR[ds(256 * b + 128 * v + 16 * k, 16)] for v in range(2))
                    a1 = jnp.zeros((16, 128), f32)
                    a2 = jnp.zeros((16, 128), f32)
                    for t in range(count):
                        l = pl.ds(first + 128 * t, 128)
                        m = T1[w, l]
                        bias = GBR[0:1, l]
                        JB[j, cw, l] = (g * m + sh * bias).astype(bf)
                        wt = W[gw, pl.ds(128 * t, 128)].astype(f32)
                        a1 = a1 + wt * m
                        a2 = a2 + wt * bias
                    for v, a in ((2 * b, a1), (2 * b + 1, a2)):
                        CT[ds(128 * v + 16 * k, 16)] = jnp.broadcast_to(jnp.sum(a, -1, keepdims=True) / g, (16, 128))

            for v in range(4):
                VEC[j, pl.ds(v, 1)] = CT[pl.ds(128 * v, 128)].T[0:1]

        x1(i).start()

        turn_at = phys(jnp.where(i == 0, 3, jnp.where(i == 1, 0, 4 - i)))

        @pl.loop(2 * turn_at, 2 * turn_at + 2)
        def _(b):
            part = ds(256 * b, 256)
            BG[part] = (mm(QKV[part], WJ[...], 1, 1) + mm(SLOPE[part], WE[...], 1, 1)).astype(bf)
            R2[0](b).start()

        @pl.when(i == 0)
        def _():
            R1[2](3)

        @pl.when(i == 1)
        def _():
            R1[2](0)

        @pl.when(i == 2)
        def _():
            R1[2](2)
            R1[5](3)

    def tile(fd, src):
        return rc(VEC.at[fd], VR.at[src], sv.at[fd], rv.at[src], (r, fd))

    for t in range(3):
        VEC[(16 * t + f) // 3, pl.ds(4 + (16 * t + f) % 3, 1)] = GBR[0:1, pl.ds(128 * t, 128)]
    TOT[pl.ds(7, 1)] = BSUM[...]
    for t in range(4):
        TOT[pl.ds(8 + t, 1)] = GBR[0:1, pl.ds(384 + 128 * t, 128)]

    @pl.loop(1, 16)
    def _(k):
        tile((f + k) % 16, f).start()

    VR[f] = VEC[f]
    je_group(0)
    je_group(1)
    R1[2](1)
    R1[5](2)
    R2[1](3)
    R2[1](0)

    def total_rep():
        return rc(TOT, TX, st_, rt_, xp)

    @pl.loop(1, 16)
    def _(k):
        tile(f, (f + k) % 16).wait_recv()

    TOT[pl.ds(0, 7)] = jnp.sum(VR[...], 0)[0:7]
    total_rep().start()
    R1[5](0)
    je_group(2)
    R2[1](2)
    R2[1](1)
    je_group(3)
    R1[3]()
    R2[2](3)
    R2[2](0)
    fwd_group(0)
    R2[2](2)
    R2[5](3)
    fwd_group(1)
    R2[2](1)
    R2[5](2)
    fwd_group(2)
    R2[5](0)
    fwd_group(3)
    R2[3]()
    R1[4](8)
    R2[4]()
    send_small.wait()

    @pl.loop(1, 16)
    def _(k):
        fd = (f + k) % 16
        for t, (s, d) in enumerate(wpieces(f, fd, True)):
            rc(s, d, sw.at[fd, t], rw.at[f, t], (r, fd)).wait_send()

    @pl.loop(1, 16)
    def _(k):
        tile((f + k) % 16, f).wait_send()

    total_rep().wait_recv()
    total_rep().wait_send()
    FIN[...] = TOT[...] + TX[...]
    os_drain()
    je_drain()


def layer_call(x, bg, sm, jw, ew, wo, ws, ct, eb):
    S = jax.ShapeDtypeStruct
    D = pltpu.SemaphoreType.DMA
    V = pltpu.VMEM
    hbm = pl.BlockSpec(memory_space=pl.ANY)
    vm = pl.BlockSpec(memory_space=pltpu.VMEM)
    return pl.pallas_call(
        layer_kernel,
        out_shape=(
            S((128, WIDE), f32), S((128, WIDE), f32), S((640, WIDE), bf), S((128, 3 * WIDE), bf),
            S((128, 4 * WIDE), bf), S((16, 128), f32), S((256, 128), f32),
        ),
        in_specs=[hbm] * 7 + [vm] * 2,
        out_specs=(hbm, hbm, hbm, hbm, hbm, vm, hbm),
        scratch_shapes=[
            V((TOK, WIDE), bf), V((TOK, WIDE), bf), V((WIDE, 384), bf), V((WIDE, 512), bf), V((640, WIDE), bf),
            V((TOK, 640), bf), V((TOK, 384), bf), V((TOK, 512), bf), V((TOK, 128), f32),
            V((TOK, 128), f32), V((8, 128, WIDE), bf), V((4, 128, WIDE), bf), V((8, 128, WIDE), bf),
            V((4, 128, WIDE), bf), V((5, 128, WIDE), bf), V((8, 128, WIDE), bf),
            V((16, 128, 896), bf), V((16, 64, 896), bf), V((4, 640, 512), bf), V((4, 320, 512), bf),
            V((512, 896), f32), V((16, 16, 128), bf), V((256, 128), f32),
            V((8, 896), f32), V((8, 896), f32),
            V((16, 8, 128), f32), V((16, 8, 128), f32), V((16, 128), f32), V((16, 128), f32), V((1, 128), f32),
        ]
        + [D((16,))] * 10 + [D((16, 4))] * 4 + [D((16,))] * 2
        + [D((2, 8))] * 2 + [D((2, 4))] * 3 + [D((2, 5))] + [D((4,))] * 6 + [D((16, 4))] * 4
        + [D((16,))] * 2 + [D, D] + [D((12,)), pltpu.SemaphoreType.REGULAR],
        compiler_params=pltpu.CompilerParams(
            collective_id=0, has_side_effects=True, vmem_limit_bytes=67043328
        ),
    )(x, bg, sm, jw, ew, wo, ws, ct, eb)


def wide(a):
    return a.astype(f32)


def turn_tables(length):
    place = np.arange(length, dtype=np.float32)[:, None]
    power = np.arange(ROT // 2, dtype=np.float32) * np.float32(2.0) / np.float32(ROT)
    angle = place * np.power(np.float32(rotary_base), -power)
    cosine, sine = (np.cos(angle), np.sin(angle))
    rest = np.zeros((length, HEAD_DIM - 2 * ROT))
    return jnp.asarray(np.concatenate([cosine, cosine, -sine, sine, rest], 1), f32)


def head_body(
    n,
    layer_input,
    segment,
    live_mask,
    attention_gain,
    attention_shift,
    joined_weight,
    joined_bias,
    output_weight,
    output_bias,
    feedforward_gain,
    feedforward_shift,
    expand_weight,
    expand_bias,
    shrink_weight,
    shrink_bias,
    cotangent,
):
    own, width = layer_input.shape
    part = width // n
    live_rows = wide(live_mask[0])[:, None]
    seeds = wide(cotangent)
    branch_own = (live_rows * seeds).astype(bf)
    seg = segment[0]
    places = jnp.arange(own, dtype=jnp.int32)
    earlier = jnp.sum((seg[None, :] < seg[:, None]).astype(jnp.int32), -1)
    lines = (
        attention_gain.reshape(1, part),
        attention_shift.reshape(1, part),
        feedforward_gain.reshape(1, part),
        feedforward_shift.reshape(1, part),
        output_bias.reshape(1, part),
        shrink_bias.reshape(1, part),
        joined_bias.reshape(3, part),
        segment.astype(bf),
        (places - earlier).astype(bf).reshape(1, own),
    )
    row = lax.broadcasted_iota(jnp.int32, (16, 128), 0)
    small = jnp.zeros((16, 128), bf)
    at = 0
    for item in lines:
        for k in range(item.shape[0]):
            small = jnp.where(row == at, item[k : k + 1], small)
            at += 1
    ct = turn_tables(own)
    rows_own = wide(layer_input)
    centred = rows_own - jnp.mean(rows_own, -1, keepdims=True)
    inverse = lax.rsqrt(jnp.mean(centred * centred, -1, keepdims=True) + epsilon)
    normalized = centred * inverse
    summed, hat_own, os_grad, joined_grad, expand_grad, sums, small_all = layer_call(
        normalized.astype(bf), branch_own, small, joined_weight, expand_weight, output_weight, shrink_weight,
        ct, wide(expand_bias).reshape(1, -1),
    )
    small_all = small_all.reshape(n, 16, part)
    bias = (small_all[:, 4] + small_all[:, 5]).reshape(width)
    layer_output = (rows_own + live_rows * (summed + bias)).astype(bf)
    row_grad = inverse * (
        hat_own
        - jnp.mean(hat_own, -1, keepdims=True)
        - normalized * jnp.mean(hat_own * normalized, -1, keepdims=True)
    )
    input_grad = (seeds + row_grad).astype(bf)

    os_grad = wide(os_grad)
    return (
        layer_output,
        input_grad,
        sums[0],
        sums[1],
        wide(joined_grad),
        sums[4:7].reshape(-1),
        os_grad[:part],
        sums[7],
        sums[2],
        sums[3],
        wide(expand_grad),
        sums[8:12].reshape(-1),
        os_grad[part:],
        sums[7],
    )


def solution(mesh):
    n = mesh.shape["fsdp"]
    fits = n == HEADS and mesh.shape["rep"] == 2
    chosen = functools.partial(head_body, n) if fits else body
    placed = (
        P(("rep", "fsdp"), None),
        P(("rep", "fsdp"), None),
        P(("rep", "fsdp"), None),
        P("fsdp"),
        P("fsdp"),
        P("fsdp", None),
        P("fsdp"),
        P("fsdp", None),
        P("fsdp"),
        P("fsdp"),
        P("fsdp"),
        P("fsdp", None),
        P("fsdp"),
        P("fsdp", None),
        P("fsdp"),
        P(("rep", "fsdp"), None),
    )
    return jax.shard_map(
        chosen,
        mesh=mesh,
        in_specs=placed,
        out_specs=(
            P(("rep", "fsdp"), None),
            P(("rep", "fsdp"), None),
            P("fsdp"),
            P("fsdp"),
            P("fsdp", None),
            P("fsdp"),
            P("fsdp", None),
            P("fsdp"),
            P("fsdp"),
            P("fsdp"),
            P("fsdp", None),
            P("fsdp"),
            P("fsdp", None),
            P("fsdp"),
        ),
        check_vma=False,
    )
```

```python
import functools

import jax
import jax.numpy as jnp
import numpy as np
from jax import lax
from jax.experimental import pallas as pl
from jax.experimental.pallas import tpu as pltpu
from jax.sharding import PartitionSpec as P

D = 2048
HEADS = 16
HEAD_DIM = 128
ROT = 32


epsilon = 1e-05
masked_score = -1e30
rotary_base = 10000.0


def as_sent(shard):
    return jax.tree.map(lambda a: a.astype(jnp.bfloat16) if a.dtype == jnp.float32 else a, shard)


def norm_rows(rows, gain, shift):
    centre = jnp.mean(rows, -1, keepdims=True)
    centred = rows - centre
    inverse = lax.rsqrt(jnp.mean(centred * centred, -1, keepdims=True) + epsilon)
    normalized = centred * inverse
    return (normalized * gain.astype(jnp.float32) + shift.astype(jnp.float32), normalized, inverse)


def norm_back(normed_grad, normalized, inverse, gain):
    scaled = normed_grad * gain.astype(jnp.float32)
    row_grad = inverse * (
        scaled
        - jnp.mean(scaled, -1, keepdims=True)
        - normalized * jnp.mean(scaled * normalized, -1, keepdims=True)
    )
    return (row_grad, jnp.sum(normed_grad * normalized, 0), jnp.sum(normed_grad, 0))


def rotary_tables(segment):
    length = segment.shape[-1]
    places = jnp.arange(length, dtype=jnp.int32)
    earlier = jnp.sum((segment[..., None, :] < segment[..., :, None]).astype(jnp.int32), -1)
    position = (places - earlier).astype(jnp.float32)
    exponent = jnp.arange(ROT // 2, dtype=jnp.float32) * 2.0 / ROT
    frequency = jnp.power(jnp.float32(rotary_base), -exponent)
    angle = position[..., None] * frequency
    return (jnp.cos(angle), jnp.sin(angle))


def turn(heads, cosine, sine, sign):
    half = ROT // 2
    front = heads[..., :half]
    behind = heads[..., half:ROT]
    cos_wide = cosine[..., None, :]
    sin_wide = sine[..., None, :] * sign
    return jnp.concatenate(
        [
            front * cos_wide - behind * sin_wide,
            behind * cos_wide + front * sin_wide,
            heads[..., ROT:],
        ],
        -1,
    )


def gelu_slope(values):
    return (
        0.5 * (1.0 + lax.erf(values * 0.7071067811865476))
        + values * jnp.exp(-0.5 * values * values) * 0.3989422804014327
    )


def attention_inputs(rows, weights, cosine, sine):
    gain, shift, joined_weight, joined_bias = (weights[0], weights[1], weights[2], weights[3])
    normed, normalized, inverse = norm_rows(rows, gain, shift)
    normed_low = normed.astype(jnp.bfloat16)
    joined = jnp.dot(
        normed_low, joined_weight, preferred_element_type=jnp.float32
    ) + joined_bias.astype(jnp.float32)
    length = rows.shape[0]
    split = joined.reshape(length, 3, HEADS, HEAD_DIM)
    queries = turn(split[:, 0], cosine, sine, 1.0).astype(jnp.bfloat16)
    keys = turn(split[:, 1], cosine, sine, 1.0).astype(jnp.bfloat16)
    values = split[:, 2].astype(jnp.bfloat16)
    return (normed_low, normalized, inverse, queries, keys, values)


def score_block(queries, keys, allowed):
    scores = jnp.einsum(
        "thd,shd->hts", queries, keys, preferred_element_type=jnp.float32
    ) * HEAD_DIM ** (-0.5)
    return jnp.where(allowed[None], scores, masked_score)


def feedforward_inputs(rows, weights):
    gain, shift, expand_weight, expand_bias = (weights[0], weights[1], weights[2], weights[3])
    normed, normalized, inverse = norm_rows(rows, gain, shift)
    normed_low = normed.astype(jnp.bfloat16)
    expanded = jnp.dot(
        normed_low, expand_weight, preferred_element_type=jnp.float32
    ) + expand_bias.astype(jnp.float32)
    return (normed_low, normalized, inverse, expanded)


def body(
    layer_input,
    segment,
    live_mask,
    attention_gain,
    attention_shift,
    joined_weight,
    joined_bias,
    output_weight,
    output_bias,
    feedforward_gain,
    feedforward_shift,
    expand_weight,
    expand_bias,
    shrink_weight,
    shrink_bias,
    cotangent,
):
    rows = layer_input.astype(jnp.float32)
    seg_row = segment[0]
    live_rows = live_mask[0].astype(jnp.float32)[:, None]
    length = seg_row.shape[0]
    cosine, sine = rotary_tables(seg_row)
    places = jnp.arange(length, dtype=jnp.int32)
    allowed = (seg_row[:, None] == seg_row[None, :]) & (places[None, :] <= places[:, None])
    attention_parts = (
        attention_gain,
        attention_shift,
        joined_weight,
        joined_bias,
        output_weight,
        output_bias,
    )
    feedforward_parts = (
        feedforward_gain,
        feedforward_shift,
        expand_weight,
        expand_bias,
        shrink_weight,
        shrink_bias,
    )
    attention_full = (
        lax.all_gather(attention_gain, "fsdp", axis=0, tiled=True),
        lax.all_gather(attention_shift, "fsdp", axis=0, tiled=True),
        lax.all_gather(joined_weight, "fsdp", axis=0, tiled=True),
        lax.all_gather(joined_bias, "fsdp", axis=0, tiled=True),
        lax.all_gather(output_weight, "fsdp", axis=0, tiled=True),
        lax.all_gather(output_bias, "fsdp", axis=0, tiled=True),
    )
    feedforward_full = (
        lax.all_gather(feedforward_gain, "fsdp", axis=0, tiled=True),
        lax.all_gather(feedforward_shift, "fsdp", axis=0, tiled=True),
        lax.all_gather(expand_weight, "fsdp", axis=0, tiled=True),
        lax.all_gather(expand_bias, "fsdp", axis=0, tiled=True),
        lax.all_gather(shrink_weight, "fsdp", axis=0, tiled=True),
        lax.all_gather(shrink_bias, "fsdp", axis=0, tiled=True),
    )
    normed_one, normalized_one, inverse_one, queries, keys, values = attention_inputs(
        rows, attention_full, cosine, sine
    )
    scores = score_block(queries, keys, allowed)
    top = jnp.max(scores, -1, keepdims=True)
    expo = jnp.exp(scores - top)
    total = jnp.sum(expo, -1, keepdims=True)
    log_total = top + jnp.log(total)
    probs_low = (expo / total).astype(jnp.bfloat16)
    mixed = jnp.einsum("hts,shd->thd", probs_low, values, preferred_element_type=jnp.float32)
    mixed = mixed.reshape(length, D).astype(jnp.bfloat16)
    attended = jnp.dot(
        mixed, attention_full[4], preferred_element_type=jnp.float32
    ) + attention_full[5].astype(jnp.float32)
    normed_two, normalized_two, inverse_two, expanded = feedforward_inputs(rows, feedforward_full)
    activated = jax.nn.gelu(expanded, approximate=False).astype(jnp.bfloat16)
    shrunk = jnp.dot(
        activated, feedforward_full[4], preferred_element_type=jnp.float32
    ) + feedforward_full[5].astype(jnp.float32)
    layer_output = (rows + live_rows * (attended + shrunk)).astype(jnp.bfloat16)
    seed_rows = cotangent.astype(jnp.float32)
    branch_grad = (live_rows * seed_rows).astype(jnp.bfloat16)
    branch_total = jnp.sum(branch_grad.astype(jnp.float32), 0)
    feedforward_back = lax.all_gather(
        as_sent(lax.optimization_barrier((feedforward_parts, layer_output))[0]),
        "fsdp",
        axis=0,
        tiled=True,
    )
    normed_two, normalized_two, inverse_two, expanded = feedforward_inputs(rows, feedforward_back)
    activated = jax.nn.gelu(expanded, approximate=False).astype(jnp.bfloat16)
    shrink_weight_grad = jnp.einsum(
        "tf,td->fd", activated, branch_grad, preferred_element_type=jnp.float32
    )
    activated_grad = jnp.einsum(
        "td,fd->tf", branch_grad, feedforward_back[4], preferred_element_type=jnp.float32
    )
    expanded_grad = (activated_grad * gelu_slope(expanded)).astype(jnp.bfloat16)
    expand_bias_grad = jnp.sum(expanded_grad.astype(jnp.float32), 0)
    expand_weight_grad = jnp.einsum(
        "td,tf->df", normed_two, expanded_grad, preferred_element_type=jnp.float32
    )
    normed_two_grad = jnp.einsum(
        "tf,df->td", expanded_grad, feedforward_back[2], preferred_element_type=jnp.float32
    )
    rows_grad_two, ff_gain_grad, ff_shift_grad = norm_back(
        normed_two_grad, normalized_two, inverse_two, feedforward_back[0]
    )
    ff_terms = (
        ff_gain_grad,
        ff_shift_grad,
        expand_weight_grad,
        expand_bias_grad,
        shrink_weight_grad,
        branch_total,
    )
    ff_parts = (
        lax.psum_scatter(ff_terms[0], "fsdp", scatter_dimension=0, tiled=True),
        lax.psum_scatter(ff_terms[1], "fsdp", scatter_dimension=0, tiled=True),
        lax.psum_scatter(ff_terms[2], "fsdp", scatter_dimension=0, tiled=True),
        lax.psum_scatter(ff_terms[3], "fsdp", scatter_dimension=0, tiled=True),
        lax.psum_scatter(ff_terms[4], "fsdp", scatter_dimension=0, tiled=True),
        lax.psum_scatter(ff_terms[5], "fsdp", scatter_dimension=0, tiled=True),
    )
    attention_back = lax.all_gather(
        as_sent(lax.optimization_barrier((attention_parts, layer_output))[0]),
        "fsdp",
        axis=0,
        tiled=True,
    )
    normed_one, normalized_one, inverse_one, queries, keys, values = attention_inputs(
        rows, attention_back, cosine, sine
    )
    scores = score_block(queries, keys, allowed)
    probs = jnp.exp(scores - log_total)
    probs_low = probs.astype(jnp.bfloat16)
    mixed = jnp.einsum("hts,shd->thd", probs_low, values, preferred_element_type=jnp.float32)
    mixed = mixed.reshape(length, D).astype(jnp.bfloat16)
    output_weight_grad = jnp.einsum(
        "td,te->de", mixed, branch_grad, preferred_element_type=jnp.float32
    )
    mixed_grad = jnp.einsum(
        "te,de->td", branch_grad, attention_back[4], preferred_element_type=jnp.float32
    )
    mixed_grad = mixed_grad.astype(jnp.bfloat16).reshape(length, HEADS, HEAD_DIM)
    value_grad = jnp.einsum(
        "hts,thd->shd", probs_low, mixed_grad, preferred_element_type=jnp.float32
    )
    probs_grad = jnp.einsum("thd,shd->hts", mixed_grad, values, preferred_element_type=jnp.float32)
    scores_grad = (probs * (probs_grad - jnp.sum(probs_grad * probs, -1, keepdims=True))).astype(
        jnp.bfloat16
    )
    query_grad = jnp.einsum(
        "hts,shd->thd", scores_grad, keys, preferred_element_type=jnp.float32
    ) * HEAD_DIM ** (-0.5)
    key_grad = jnp.einsum(
        "hts,thd->shd", scores_grad, queries, preferred_element_type=jnp.float32
    ) * HEAD_DIM ** (-0.5)
    query_grad = turn(query_grad, cosine, sine, -1.0)
    key_grad = turn(key_grad, cosine, sine, -1.0)
    joined_grad = jnp.concatenate(
        [query_grad.reshape(length, D), key_grad.reshape(length, D), value_grad.reshape(length, D)],
        1,
    ).astype(jnp.bfloat16)
    joined_bias_grad = jnp.sum(joined_grad.astype(jnp.float32), 0)
    joined_weight_grad = jnp.einsum(
        "td,te->de", normed_one, joined_grad, preferred_element_type=jnp.float32
    )
    normed_one_grad = jnp.einsum(
        "te,de->td", joined_grad, attention_back[2], preferred_element_type=jnp.float32
    )
    rows_grad_one, at_gain_grad, at_shift_grad = norm_back(
        normed_one_grad, normalized_one, inverse_one, attention_back[0]
    )
    at_terms = (
        at_gain_grad,
        at_shift_grad,
        joined_weight_grad,
        joined_bias_grad,
        output_weight_grad,
        branch_total,
    )
    at_parts = (
        lax.psum_scatter(at_terms[0], "fsdp", scatter_dimension=0, tiled=True),
        lax.psum_scatter(at_terms[1], "fsdp", scatter_dimension=0, tiled=True),
        lax.psum_scatter(at_terms[2], "fsdp", scatter_dimension=0, tiled=True),
        lax.psum_scatter(at_terms[3], "fsdp", scatter_dimension=0, tiled=True),
        lax.psum_scatter(at_terms[4], "fsdp", scatter_dimension=0, tiled=True),
        lax.psum_scatter(at_terms[5], "fsdp", scatter_dimension=0, tiled=True),
    )
    input_grad = (seed_rows + rows_grad_one + rows_grad_two).astype(jnp.bfloat16)
    summed = (
        lax.psum(at_parts[0].astype(jnp.bfloat16), "rep").astype(jnp.float32),
        lax.psum(at_parts[1].astype(jnp.bfloat16), "rep").astype(jnp.float32),
        lax.psum(at_parts[2].astype(jnp.bfloat16), "rep").astype(jnp.float32),
        lax.psum(at_parts[3].astype(jnp.bfloat16), "rep").astype(jnp.float32),
        lax.psum(at_parts[4].astype(jnp.bfloat16), "rep").astype(jnp.float32),
        lax.psum(at_parts[5].astype(jnp.bfloat16), "rep").astype(jnp.float32),
        lax.psum(ff_parts[0].astype(jnp.bfloat16), "rep").astype(jnp.float32),
        lax.psum(ff_parts[1].astype(jnp.bfloat16), "rep").astype(jnp.float32),
        lax.psum(ff_parts[2].astype(jnp.bfloat16), "rep").astype(jnp.float32),
        lax.psum(ff_parts[3].astype(jnp.bfloat16), "rep").astype(jnp.float32),
        lax.psum(ff_parts[4].astype(jnp.bfloat16), "rep").astype(jnp.float32),
        lax.psum(ff_parts[5].astype(jnp.bfloat16), "rep").astype(jnp.float32),
    )
    return (
        layer_output,
        input_grad,
        summed[0],
        summed[1],
        summed[2],
        summed[3],
        summed[4],
        summed[5],
        summed[6],
        summed[7],
        summed[8],
        summed[9],
        summed[10],
        summed[11],
    )


MESH = pl.DeviceIdType.MESH
bf = jnp.bfloat16
f32 = jnp.float32
WIDE = 2048
TOK = 2048


def ds(start, size):
    return pl.ds(pl.multiple_of(start, size), size)


def mm(a, b, ca, cb):
    return lax.dot_general(a, b, (((ca,), (cb,)), ((), ())), preferred_element_type=f32)


def layer_kernel(
    x_ref, bg_ref, sm_ref, jw_ref, ew_ref, wo_ref, ws_ref, ct_ref, eb_ref,
    SO1, SO2, OSo, JWo, EWo, FIN, SMO,
    X, BG, WJ, WE, WOS, INNER, QKV, SLOPE, CT, PR, L1, RING, A1, B1, C1, A2,
    JB, RX, OSB, ROS, T1, SM, SMF, CV, GBR, VEC, VR, TOT, TX, BSUM,
    su, sd, sy, ss, rx_, bu, bd, by, bs, rb_, sw, rw, sxw, rxw, ssm, rsm,
    sa, ra, sbb, rbb, sc, rc_, sx, rxx, so, ro, so2, ro2, sg, rg, sf, rf, sv, rv, st_, rt_, lsem, ready,
):
    r = lax.axis_index("rep")
    f = lax.axis_index("fsdp")
    z = f // 4
    y = (f // 2) % 2
    c = f % 2
    sib = (r, z * 4 + y * 2 + (1 - c))
    yo = z * 4 + (1 - y) * 2 + c
    yp = (r, yo)
    xp = (1 - r, f)
    lower = z <= 1
    zz = jnp.where(lower, z, 3 - z)

    def phys(q):
        return jnp.where(lower, q, 3 - q)

    f_in = (r, jnp.where(lower, f + 4, f - 4))
    f_out = (r, jnp.where(lower, f - 4, f + 4))

    barrier = pltpu.get_barrier_semaphore()

    @pl.loop(1, 16)
    def _(k):
        pl.semaphore_signal(barrier, inc=1, device_id=(r, (f + k) % 16), device_id_type=MESH)

    pl.semaphore_signal(barrier, inc=1, device_id=xp, device_id_type=MESH)
    pl.semaphore_wait(barrier, 16)

    def rc(src, dst, s, q, dev):
        return pltpu.make_async_remote_copy(
            src_ref=src, dst_ref=dst, send_sem=s, recv_sem=q, device_id=dev, device_id_type=MESH
        )

    def lc(src, dst, s):
        return pltpu.make_async_copy(src, dst, s)

    def gather(own, OUT, su, sd, sy, ss, rr):
        def item(i):
            return OUT.at[ds(128 * i, 128)]

        def up(i, src=None):
            return rc(item(i) if src is None else src, item(i), su.at[i], rr.at[i], (r, f + 4))

        def dn(i, src=None):
            return rc(item(i) if src is None else src, item(i), sd.at[i], rr.at[i], (r, f - 4))

        def ac(i, src=None):
            return rc(item(i) if src is None else src, item(i), sy.at[i], rr.at[i], yp)

        def sb(i, src=None):
            return rc(item(i) if src is None else src, item(i), ss.at[i], rr.at[i], sib)

        def begin_z():
            pl.when(z < 3)(lambda: up(f, own).start())
            pl.when(z > 0)(lambda: dn(f, own).start())

        def begin_y():
            ac(f, own).start()
            sb(f, own).start()

        def step(s):
            @pl.when(z - s >= 0)
            def _():
                i = f - 4 * s
                up(i).wait_recv()
                pl.when(z < 3)(lambda: up(i).start())
                ac(i).start()
                sb(i).start()

            @pl.when(z + s <= 3)
            def _():
                i = f + 4 * s
                dn(i).wait_recv()
                pl.when(z > 0)(lambda: dn(i).start())
                ac(i).start()
                sb(i).start()

        def ystep(s):
            @pl.when(z - s >= 0)
            def _():
                ac(yo - 4 * s).wait_recv()
                sb(yo - 4 * s).start()

            @pl.when((s > 0) & (z + s <= 3))
            def _():
                ac(yo + 4 * s).wait_recv()
                sb(yo + 4 * s).start()

        def landed(q):
            for v in range(2):
                sb(4 * q + 2 * v + 1 - c).wait_recv()

        def finish():
            @pl.loop(0, 8)
            def _(k):
                sb(2 * k + c).wait_send()

            @pl.loop(0, 4)
            def _(k):
                i = k * 4 + y * 2 + c
                ac(i).wait_send()
                pl.when((k <= z) & (z < 3))(lambda: up(i).wait_send())
                pl.when((k >= z) & (z > 0))(lambda: dn(i).wait_send())

        return begin_z, begin_y, step, ystep, landed, finish

    xz, xo, xs, xy, xl, xf = gather(x_ref, X, su, sd, sy, ss, rx_)
    gz, go, gs, gy, gl, gf = gather(bg_ref, BG, bu, bd, by, bs, rb_)

    def wpieces(src, dst, from_arg):
        rows = ds(128 * src + 64 * r, 64)
        out = []
        for t in range(3):
            d = WJ.at[rows, pl.ds(128 * t, 128)]
            out.append((jw_ref.at[ds(64 * r, 64), ds(2048 * t + 128 * dst, 128)] if from_arg else d, d))
        d = WE.at[rows]
        out.append((ew_ref.at[ds(64 * r, 64), ds(512 * dst, 512)] if from_arg else d, d))
        return out

    def fwd(lo, hi):
        @pl.loop(lo, hi)
        def _(k):
            fs = (f + 16 - k) % 16
            for t, (s, d) in enumerate(wpieces(fs, f, False)):
                rc(s, d, sw.at[fs, t], rw.at[fs, t], (r, f)).wait_recv()
                rc(s, d, sxw.at[fs, t], rxw.at[fs, t], xp).start()

    own_x = lc(x_ref, X.at[ds(128 * f, 128)], lsem.at[0])
    own_b = lc(bg_ref, BG.at[ds(128 * f, 128)], lsem.at[1])
    load_o = lc(wo_ref, WOS.at[pl.ds(0, 128)], lsem.at[2])
    load_s = lc(ws_ref, WOS.at[pl.ds(128, 512)], lsem.at[3])
    own_s = lc(sm_ref, SM.at[f], lsem.at[4])
    def wsend(lo, hi):
        @pl.loop(lo, hi)
        def _(k):
            fd = (f + k) % 16
            for t, (s, d) in enumerate(wpieces(f, fd, True)):
                rc(s, d, sw.at[fd, t], rw.at[f, t], (r, fd)).start()

    def ssend():
        @pl.loop(1, 16)
        def _(k):
            fd = (f + k) % 16
            rc(sm_ref, SM.at[f], ssm.at[fd], rsm.at[f], (r, fd)).start()

    def wown():
        for t, (s, d) in enumerate(wpieces(f, f, True)):
            rc(s, d, sxw.at[f, t], rxw.at[f, t], xp).start()
            lc(s, d, rw.at[f, t]).start()

    for cp in (own_x, own_b, load_o, load_s, own_s):
        cp.start()
    ssend()
    wsend(1, 16)
    wown()
    xo()
    xz()
    go()
    fwd(1, 13)
    own_s.wait()

    @pl.loop(1, 16)
    def _(k):
        fs = (f + k) % 16
        other = rc(sm_ref, SM.at[fs], ssm.at[fs], rsm.at[fs], (r, fs))
        other.wait_recv()
        other.wait_send()

    @pl.loop(0, 16)
    def _(i):
        SMF[ds(16 * i, 16)] = SM[i].astype(f32)

    send_small = lc(SMF, SMO, lsem.at[4])
    send_small.start()

    @pl.loop(0, 16)
    def _(i):
        rows = ds(128 * i, 128)
        place = jnp.broadcast_to(SMF[pl.ds(16 * i + 10, 1)], (128, 128)).T
        pick = (place == lax.broadcasted_iota(jnp.int32, (128, 128), 1).astype(f32)).astype(f32)
        hi = lax.Precision.HIGHEST
        CT[rows] = jnp.dot(pick, ct_ref[...], precision=hi, preferred_element_type=f32)

    fwd(13, 16)
    xs(1)

    for t, (s, d) in enumerate(wpieces(f, f, True)):
        lc(s, d, rw.at[f, t]).wait()
    other_half = lambda src: ds(128 * src + 64 * (1 - r), 64)

    @pl.loop(0, 16)
    def _(fs):
        for t in range(4):
            d = WJ.at[other_half(fs), pl.ds(128 * t, 128)] if t < 3 else WE.at[other_half(fs)]
            cp = rc(d, d, sxw.at[fs, t], rxw.at[fs, t], xp)
            cp.wait_recv()
            cp.wait_send()

    load_o.wait()
    load_s.wait()

    def columns(j):
        for v in range(4):
            PR[pl.ds(128 * v, 128)] = jnp.broadcast_to(SMF[pl.ds(16 * j + v, 1)], (128, 128)).T

    def fold(v):
        return v[:8] + v[8:]

    CV[...] = jnp.zeros_like(CV)

    @pl.loop(0, 16)
    def _(j):
        columns(j)

        @pl.loop(0, 8)
        def _(k):
            w = ds(128 * j + 16 * k, 16)
            cw = ds(16 * k, 16)
            g1, s1, g2, s2 = (PR[ds(128 * v + 16 * k, 16)] for v in range(4))
            for t in range(3):
                l = pl.ds(128 * t, 128)
                v = WJ[w, l].astype(f32)
                CV[:, l] += fold(v * s1)
                WJ[w, l] = (v * g1).astype(bf)
            for t in range(4):
                l = pl.ds(128 * t, 128)
                lo = pl.ds(384 + 128 * t, 128)
                v = WE[w, l].astype(f32)
                CV[:, lo] += fold(v * s2)
                WE[w, l] = (v * g2).astype(bf)

    CV[...] = jnp.broadcast_to(jnp.sum(CV[...], 0, keepdims=True), CV.shape)
    for t in range(3):
        place = (16 * t + f) // 3 * 16 + 6 + (16 * t + f) % 3
        CV[:, pl.ds(128 * t, 128)] += SMF[pl.ds(place, 1)]
    CV[:, pl.ds(384, 512)] += eb_ref[...]

    lane = lax.broadcasted_iota(jnp.int32, (16, 128), 1)

    def angles(v, ln):
        return jnp.where(ln < 32, v, 1.0), jnp.where(ln < 32, pltpu.roll(v, 96, 1), 0.0)

    def swap(v, ln):
        return jnp.where(ln < 16, pltpu.roll(v, 112, 1), pltpu.roll(v, 16, 1))

    scale = HEAD_DIM ** (-0.5)
    down = lax.broadcasted_iota(jnp.int32, (128, 128), 0)
    across = lax.broadcasted_iota(jnp.int32, (128, 128), 1)

    own_x.wait()

    @pl.loop(0, 4)
    def _(p):
        i = phys(jnp.where((zz == 1) & (p < 2), 1 - p, p))
        rows = ds(512 * i, 512)
        pl.when((p > 0) & (p < 3))(lambda: xs(p + 1))
        @pl.when(p == 1)
        def _():
            gz()

        xy(p)
        xl(i)
        T1[:, pl.ds(0, 384)] = mm(X[rows], WJ[...], 1, 0)
        T1[:, pl.ds(384, 512)] = mm(X[rows], WE[...], 1, 0)

        @pl.loop(0, 32, unroll=2)
        def _(k):
            w = ds(16 * k, 16)
            gw = ds(512 * i + 16 * k, 16)
            cos, sin = angles(CT[gw], lane)
            for t in range(2):
                l = pl.ds(128 * t, 128)
                v = T1[w, l] + CV[0:1, l]
                QKV[gw, l] = (v * cos + swap(v, lane) * sin).astype(bf)
            l = pl.ds(256, 128)
            QKV[gw, l] = (T1[w, l] + CV[0:1, l]).astype(bf)
            for t in range(4):
                l = pl.ds(384 + 128 * t, 128)
                v = T1[w, l] + CV[0:1, l]
                part = 0.5 * (1.0 + lax.erf(v * 0.7071067811865476))
                INNER[gw, pl.ds(128 + 128 * t, 128)] = (v * part).astype(bf)
                SLOPE[gw, pl.ds(128 * t, 128)] = (
                    part + v * jnp.exp(-0.5 * v * v) * 0.3989422804014327
                ).astype(bf)

        @pl.loop(0, 4, unroll=2)
        def _(j):
            slot = 4 * i + j
            rows = ds(128 * slot, 128)
            q = QKV[rows, pl.ds(0, 128)]
            k = QKV[rows, pl.ds(128, 128)]
            v = QKV[rows, pl.ds(256, 128)]
            seg = jnp.broadcast_to(SMF[pl.ds(16 * slot + 9, 1)], (128, 128))
            s = mm(q, k, 1, 1) * scale
            s = jnp.where((seg == seg.T) & (across <= down), s, masked_score)
            e = jnp.exp(s - jnp.max(s, -1, keepdims=True))
            p = e / jnp.sum(e, -1, keepdims=True)
            PR[rows] = p
            INNER[rows, pl.ds(0, 128)] = mm(p.astype(bf), v, 1, 0).astype(bf)

        @pl.when(p == 2)
        def _():
            gs(1)
            gy(0)

        @pl.when(p == 3)
        def _():
            gs(2)
            gy(1)


    xf()

    def add_into(dst, src, rows):
        @pl.loop(0, rows // 16)
        def _(i):
            w = ds(i * 16, 16)
            dst[w] = (dst[w].astype(f32) + src[w].astype(f32)).astype(bf)

    def reducer(n, sent, own, AA, BB, CC, CX, SO):
        def a_send(k):
            return rc(sent(k), AA(k), sa.at[n, k], ra.at[n, k], sib)

        def b_send(zp):
            return rc(own(zp * 2 + 1 - y), BB(zp), sbb.at[n, zp], rbb.at[n, zp], yp)

        def prep(k):
            a_send(k).wait_recv()
            add_into(own(k), AA(k), 128)

        def far(*turns):
            for q in turns or (3, 0, 2, 1):
                prep(phys(q) * 2 + 1 - y)
                b_send(phys(q)).start()

        def near(q):
            zp = phys(q)
            k = zp * 2 + y
            prep(k)
            b_send(zp).wait_recv()
            add_into(own(k), BB(zp), 128)

        def got(q, extra=False):
            zp = phys(q)
            buf = CX if extra else CC(zp)
            slot = 4 if extra else zp
            rc(buf, buf, sc.at[n, zp], rc_.at[n, slot], f_in).wait_recv()
            return buf

        def send(q, dev, extra=False):
            zp = phys(q)
            return rc(
                own(zp * 2 + y), CX if extra else CC(zp), sc.at[n, zp], rc_.at[n, 4 if extra else zp], dev
            )

        def step(q):
            near(q)
            if q > 0:
                pl.when(zz == 0)(lambda: send(q, f_in).start())

        def relay(q):
            k = phys(q) * 2 + y

            @pl.when(zz == 1)
            def _():
                if q >= 2:
                    add_into(own(k), got(q), 128)
                    send(q, f_in, q == 2).start()
                if q == 0:
                    add_into(own(k), got(q), 128)
                    send(q, f_out).start()

        def total(q, bufs):
            k = phys(q) * 2 + y

            @pl.loop(0, 8)
            def _(i):
                w = ds(i * 16, 16)
                v = own(k)[w].astype(f32)
                for b in bufs:
                    v = v + b[w].astype(f32)
                for l, n in enumerate((896, 896, 256)):
                    T1[ds(128 * l + 16 * i, 16), pl.ds(0, n)] = v[:, 896 * l : 896 * l + n]

        def last():
            @pl.when(zz == 0)
            def _():
                total(0, [got(0)])

            @pl.when(zz == 1)
            def _():
                total(1, [got(1), got(1, True)])

            cps = [
                lc(T1.at[pl.ds(128 * l, 128), pl.ds(0, n)], SO.at[:, pl.ds(896 * l, n)], lsem.at[at])
                for l, n, at in ((0, 896, 5), (1, 896, 10), (2, 256, 11))
            ]
            for cp in cps:
                cp.start()
            for cp in cps:
                cp.wait()

        def drain(first=0):
            @pl.loop(first, 8)
            def _(k):
                a_send(k).wait_send()

            @pl.loop(0, 4)
            def _(zp):
                b_send(zp).wait_send()

            for q in range(4):
                if q > 0:
                    pl.when(zz == 0)(lambda: send(q, f_in).wait_send())
                if q >= 2:
                    pl.when(zz == 1)(lambda: send(q, f_in, q == 2).wait_send())
                if q == 0:
                    pl.when(zz == 1)(lambda: send(q, f_out).wait_send())

        return a_send, far, step, last, drain, relay

    R1 = reducer(
        0, lambda k: RING.at[k % 3], lambda k: L1.at[k], lambda k: A1.at[k], lambda k: B1.at[k],
        lambda k: C1.at[k], C1.at[4], SO1,
    )
    R2 = reducer(
        1,
        lambda k: BG.at[ds(128 * (2 * k + 1 - c), 128)],
        lambda k: BG.at[ds(128 * (2 * k + c), 128)],
        lambda k: A2.at[k],
        lambda k: RING.at[k],
        lambda k: WOS.at[ds(128 * k, 128)],
        WOS.at[pl.ds(512, 128)],
        SO2,
    )

    @pl.loop(0, 8)
    def _(b):
        res = mm(INNER[ds(256 * b, 256)], WOS[...], 1, 0)

        @pl.when(b >= 3)
        def _():
            R1[0](b - 3).wait_send()

        for side in range(2):
            @pl.when(c == side)
            def _():
                L1[b] = res[128 * side : 128 * side + 128].astype(bf)
                RING[b % 3] = res[128 - 128 * side : 256 - 128 * side].astype(bf)

        R1[0](b).start()

        @pl.when(b == 2)
        def _():
            gs(3)
            gy(2)

    gy(3)
    own_b.wait()
    for q in range(4):
        gl(q)
    gf()

    half = ds(320 * r, 320)
    away = ds(320 * (1 - r), 320)

    def o1(j):
        return rc(OSB.at[j, away], ROS.at[j], so.at[j], ro.at[j], xp)

    def o2(j):
        return rc(OSB.at[j, half], OSo.at[half, ds(512 * j, 512)], so2.at[j], ro2.at[j], xp)

    def o2r(j):
        return rc(OSB.at[j, half], OSo.at[away, ds(512 * j, 512)], so2.at[j], ro2.at[j], xp)

    def os_store(j):
        return lc(OSB.at[j, half], OSo.at[half, ds(512 * j, 512)], lsem.at[6 + j])

    def os_step(j):
        o1(j).wait_recv()
        add_into(OSB.at[j, half], ROS.at[j], 320)
        o2(j).start()
        os_store(j).start()

    def os_drain():
        for j in range(4):
            o1(j).wait_send()
            o2(j).wait_send()
            o2r(j).wait_recv()
            os_store(j).wait()

    @pl.loop(0, 4)
    def _(j):
        OSB[j] = mm(INNER[...], BG[:, ds(512 * j, 512)], 0, 0).astype(bf)
        o1(j).start()

    R1[1]()

    GBR[...] = jnp.zeros_like(GBR)
    VEC[...] = jnp.zeros_like(VEC)
    TOT[...] = jnp.zeros_like(TOT)
    mine = BG[:, ds(128 * f, 128)].astype(f32)
    BSUM[...] = jnp.sum(mine, 0, keepdims=True)

    def fold_rows(v, rows):
        return jnp.sum(v.reshape(rows // 8, 8, v.shape[-1]), 0)

    @pl.loop(0, 4)
    def _(i):
        rows = ds(512 * i, 512)
        T1[:, pl.ds(0, 640)] = mm(BG[rows], WOS[...], 1, 1)

        @pl.loop(0, 32, unroll=2)
        def _(k):
            w = ds(16 * k, 16)
            gw = ds(512 * i + 16 * k, 16)
            INNER[gw, pl.ds(0, 128)] = T1[w, pl.ds(0, 128)].astype(bf)
            e = (T1[w, pl.ds(128, 512)] * SLOPE[gw].astype(f32)).astype(bf)
            SLOPE[gw] = e
            GBR[:, pl.ds(384, 512)] += fold(e.astype(f32))

    @pl.loop(5, 8)
    def _(b):
        R1[0](b).wait_send()

    for dev in (sib, yp, f_in):
        pl.semaphore_signal(ready, inc=1, device_id=dev, device_id_type=MESH)

    @pl.when(zz == 1)
    def _():
        pl.semaphore_signal(ready, inc=1, device_id=f_out, device_id_type=MESH)

    os_step(0)
    os_step(1)

    lane_b = lax.broadcasted_iota(jnp.int32, (128, 128), 1)

    @pl.loop(0, 16, unroll=2)
    def _(i):
        rows = ds(128 * i, 128)
        q = QKV[rows, pl.ds(0, 128)]
        k = QKV[rows, pl.ds(128, 128)]
        v = QKV[rows, pl.ds(256, 128)]
        p = PR[rows]
        mg = INNER[rows, pl.ds(0, 128)]
        vg = mm(p.astype(bf), mg, 0, 0)
        pg = mm(mg, v, 1, 1)
        sgr = (p * (pg - jnp.sum(pg * p, -1, keepdims=True))).astype(bf)
        cos, sin = angles(CT[rows], lane_b)
        qg = mm(sgr, k, 1, 0) * scale
        kg = mm(sgr, q, 0, 0) * scale
        for t, g in enumerate((qg, kg, vg)):
            if t < 2:
                g = g * cos - swap(g, lane_b) * sin
            g = g.astype(bf)
            l = pl.ds(128 * t, 128)
            QKV[rows, l] = g
            GBR[:, l] += fold_rows(g.astype(f32), 128)

    os_step(2)
    os_step(3)
    GBR[...] = jnp.broadcast_to(jnp.sum(GBR[...], 0, keepdims=True), GBR.shape)

    keep = ds(64 * r, 64)
    give = ds(64 * (1 - r), 64)

    def x1(g):
        return rc(JB.at[ds(4 * g, 4), give], RX.at[ds(4 * g, 4)], sx.at[g], rxx.at[g], xp)

    def place_of(fs, t, rows):
        if t < 3:
            return JWo.at[rows, ds(2048 * t + 128 * fs, 128)]
        return EWo.at[rows, ds(512 * fs, 512)]

    def piece_of(fd, t):
        return JB.at[fd, keep, pl.ds(128 * t, 128)] if t < 3 else JB.at[fd, keep, pl.ds(384, 512)]

    def je_group(g):
        x1(g).wait_recv()

        @pl.loop(0, 4)
        def _(j):
            fd = 4 * g + j
            add_into(JB.at[fd, keep], RX.at[fd], 64)

            @pl.when(fd != f)
            def _():
                for t in range(4):
                    rc(piece_of(fd, t), place_of(f, t, keep), sg.at[fd, t], rg.at[f, t], (r, fd)).start()

            @pl.when(fd == f)
            def _():
                for t in range(4):
                    lc(piece_of(fd, t), place_of(f, t, keep), sg.at[fd, t]).start()
                    rc(piece_of(fd, t), place_of(f, t, keep), sf.at[fd, t], rf.at[f, t], xp).start()

    def fwd_group(g):
        @pl.loop(4 * g, 4 * g + 4)
        def _(fs):
            @pl.when(fs != f)
            def _():
                for t in range(4):
                    d = place_of(fs, t, keep)
                    rc(d, d, sg.at[fs, t], rg.at[fs, t], xp).wait_recv()
                    rc(d, d, sf.at[fs, t], rf.at[fs, t], xp).start()

    def je_drain():
        for g in range(4):
            x1(g).wait_send()

        @pl.loop(0, 16)
        def _(fs):
            for t in range(4):
                d = place_of(fs, t, give)
                cp = rc(d, d, sf.at[fs, t], rf.at[fs, t], xp)
                cp.wait_recv()
                cp.wait_send()

            @pl.when(fs != f)
            def _():
                for t in range(4):
                    rc(piece_of(fs, t), place_of(f, t, keep), sg.at[fs, t], rg.at[f, t], xp).wait_send()

            @pl.when(fs == f)
            def _():
                for t in range(4):
                    lc(piece_of(fs, t), place_of(f, t, keep), sg.at[fs, t]).wait()

    @pl.when(zz == 1)
    def _():
        pl.semaphore_wait(ready, 4)

    @pl.when(zz == 0)
    def _():
        pl.semaphore_wait(ready, 3)


    @pl.loop(0, 4)
    def _(i):
        left = X[:, ds(512 * i, 512)]
        T1[:, pl.ds(0, 384)] = mm(left, QKV[...], 0, 0)
        T1[:, pl.ds(384, 512)] = mm(left, SLOPE[...], 0, 0)

        @pl.loop(0, 4)
        def _(s):
            j = 4 * i + s
            columns(j)

            @pl.loop(0, 8)
            def _(k):
                w = ds(128 * s + 16 * k, 16)
                gw = ds(128 * j + 16 * k, 16)
                cw = ds(16 * k, 16)
                for b, (first, count, W) in enumerate(((0, 3, WJ), (384, 4, WE))):
                    g, sh = (PR[ds(256 * b + 128 * v + 16 * k, 16)] for v in range(2))
                    a1 = jnp.zeros((16, 128), f32)
                    a2 = jnp.zeros((16, 128), f32)
                    for t in range(count):
                        l = pl.ds(first + 128 * t, 128)
                        m = T1[w, l]
                        bias = GBR[0:1, l]
                        JB[j, cw, l] = (g * m + sh * bias).astype(bf)
                        wt = W[gw, pl.ds(128 * t, 128)].astype(f32)
                        a1 = a1 + wt * m
                        a2 = a2 + wt * bias
                    for v, a in ((2 * b, a1), (2 * b + 1, a2)):
                        CT[ds(128 * v + 16 * k, 16)] = jnp.broadcast_to(jnp.sum(a, -1, keepdims=True) / g, (16, 128))

            for v in range(4):
                VEC[j, pl.ds(v, 1)] = CT[pl.ds(128 * v, 128)].T[0:1]

        x1(i).start()

        turn_at = phys(jnp.where(i == 0, 3, jnp.where(i == 1, 0, 4 - i)))

        @pl.loop(2 * turn_at, 2 * turn_at + 2)
        def _(b):
            part = ds(256 * b, 256)
            BG[part] = (mm(QKV[part], WJ[...], 1, 1) + mm(SLOPE[part], WE[...], 1, 1)).astype(bf)
            R2[0](b).start()

        @pl.when(i == 0)
        def _():
            R1[2](3)

        @pl.when(i == 1)
        def _():
            R1[2](0)

        @pl.when(i == 2)
        def _():
            R1[2](2)
            R1[5](3)

    def tile(fd, src):
        return rc(VEC.at[fd], VR.at[src], sv.at[fd], rv.at[src], (r, fd))

    for t in range(3):
        VEC[(16 * t + f) // 3, pl.ds(4 + (16 * t + f) % 3, 1)] = GBR[0:1, pl.ds(128 * t, 128)]
    TOT[pl.ds(7, 1)] = BSUM[...]
    for t in range(4):
        TOT[pl.ds(8 + t, 1)] = GBR[0:1, pl.ds(384 + 128 * t, 128)]

    @pl.loop(1, 16)
    def _(k):
        tile((f + k) % 16, f).start()

    VR[f] = VEC[f]
    je_group(0)
    R2[1](3)
    R2[1](0)
    je_group(1)
    R1[2](1)
    R1[5](2)

    def total_rep():
        return rc(TOT, TX, st_, rt_, xp)

    @pl.loop(1, 16)
    def _(k):
        tile(f, (f + k) % 16).wait_recv()

    TOT[pl.ds(0, 7)] = jnp.sum(VR[...], 0)[0:7]
    total_rep().start()
    R2[1](2)
    R2[1](1)
    R1[5](0)
    je_group(2)
    je_group(3)
    R1[3]()
    R2[2](3)
    fwd_group(0)
    R2[2](0)
    fwd_group(1)
    R2[2](2)
    R2[5](3)
    fwd_group(2)
    R2[2](1)
    R2[5](2)
    R2[5](0)
    fwd_group(3)
    R2[3]()
    R1[4](8)
    R2[4]()
    send_small.wait()

    @pl.loop(1, 16)
    def _(k):
        fd = (f + k) % 16
        for t, (s, d) in enumerate(wpieces(f, fd, True)):
            rc(s, d, sw.at[fd, t], rw.at[f, t], (r, fd)).wait_send()

    @pl.loop(1, 16)
    def _(k):
        tile((f + k) % 16, f).wait_send()

    total_rep().wait_recv()
    total_rep().wait_send()
    FIN[...] = TOT[...] + TX[...]
    os_drain()
    je_drain()


def layer_call(x, bg, sm, jw, ew, wo, ws, ct, eb):
    S = jax.ShapeDtypeStruct
    D = pltpu.SemaphoreType.DMA
    V = pltpu.VMEM
    hbm = pl.BlockSpec(memory_space=pl.ANY)
    vm = pl.BlockSpec(memory_space=pltpu.VMEM)
    return pl.pallas_call(
        layer_kernel,
        out_shape=(
            S((128, WIDE), f32), S((128, WIDE), f32), S((640, WIDE), bf), S((128, 3 * WIDE), bf),
            S((128, 4 * WIDE), bf), S((16, 128), f32), S((256, 128), f32),
        ),
        in_specs=[hbm] * 7 + [vm] * 2,
        out_specs=(hbm, hbm, hbm, hbm, hbm, vm, hbm),
        scratch_shapes=[
            V((TOK, WIDE), bf), V((TOK, WIDE), bf), V((WIDE, 384), bf), V((WIDE, 512), bf), V((640, WIDE), bf),
            V((TOK, 640), bf), V((TOK, 384), bf), V((TOK, 512), bf), V((TOK, 128), f32),
            V((TOK, 128), f32), V((8, 128, WIDE), bf), V((4, 128, WIDE), bf), V((8, 128, WIDE), bf),
            V((4, 128, WIDE), bf), V((5, 128, WIDE), bf), V((8, 128, WIDE), bf),
            V((16, 128, 896), bf), V((16, 64, 896), bf), V((4, 640, 512), bf), V((4, 320, 512), bf),
            V((512, 896), f32), V((16, 16, 128), bf), V((256, 128), f32),
            V((8, 896), f32), V((8, 896), f32),
            V((16, 8, 128), f32), V((16, 8, 128), f32), V((16, 128), f32), V((16, 128), f32), V((1, 128), f32),
        ]
        + [D((16,))] * 10 + [D((16, 4))] * 4 + [D((16,))] * 2
        + [D((2, 8))] * 2 + [D((2, 4))] * 3 + [D((2, 5))] + [D((4,))] * 6 + [D((16, 4))] * 4
        + [D((16,))] * 2 + [D, D] + [D((12,)), pltpu.SemaphoreType.REGULAR],
        compiler_params=pltpu.CompilerParams(
            collective_id=0, has_side_effects=True, vmem_limit_bytes=67043328
        ),
    )(x, bg, sm, jw, ew, wo, ws, ct, eb)


def wide(a):
    return a.astype(f32)


def turn_tables(length):
    place = np.arange(length, dtype=np.float32)[:, None]
    power = np.arange(ROT // 2, dtype=np.float32) * np.float32(2.0) / np.float32(ROT)
    angle = place * np.power(np.float32(rotary_base), -power)
    cosine, sine = (np.cos(angle), np.sin(angle))
    rest = np.zeros((length, HEAD_DIM - 2 * ROT))
    return jnp.asarray(np.concatenate([cosine, cosine, -sine, sine, rest], 1), f32)


def head_body(
    n,
    layer_input,
    segment,
    live_mask,
    attention_gain,
    attention_shift,
    joined_weight,
    joined_bias,
    output_weight,
    output_bias,
    feedforward_gain,
    feedforward_shift,
    expand_weight,
    expand_bias,
    shrink_weight,
    shrink_bias,
    cotangent,
):
    own, width = layer_input.shape
    part = width // n
    live_rows = wide(live_mask[0])[:, None]
    seeds = wide(cotangent)
    branch_own = (live_rows * seeds).astype(bf)
    seg = segment[0]
    places = jnp.arange(own, dtype=jnp.int32)
    earlier = jnp.sum((seg[None, :] < seg[:, None]).astype(jnp.int32), -1)
    lines = (
        attention_gain.reshape(1, part),
        attention_shift.reshape(1, part),
        feedforward_gain.reshape(1, part),
        feedforward_shift.reshape(1, part),
        output_bias.reshape(1, part),
        shrink_bias.reshape(1, part),
        joined_bias.reshape(3, part),
        segment.astype(bf),
        (places - earlier).astype(bf).reshape(1, own),
    )
    row = lax.broadcasted_iota(jnp.int32, (16, 128), 0)
    small = jnp.zeros((16, 128), bf)
    at = 0
    for item in lines:
        for k in range(item.shape[0]):
            small = jnp.where(row == at, item[k : k + 1], small)
            at += 1
    ct = turn_tables(own)
    rows_own = wide(layer_input)
    centred = rows_own - jnp.mean(rows_own, -1, keepdims=True)
    inverse = lax.rsqrt(jnp.mean(centred * centred, -1, keepdims=True) + epsilon)
    normalized = centred * inverse
    summed, hat_own, os_grad, joined_grad, expand_grad, sums, small_all = layer_call(
        normalized.astype(bf), branch_own, small, joined_weight, expand_weight, output_weight, shrink_weight,
        ct, wide(expand_bias).reshape(1, -1),
    )
    small_all = small_all.reshape(n, 16, part)
    bias = (small_all[:, 4] + small_all[:, 5]).reshape(width)
    layer_output = (rows_own + live_rows * (summed + bias)).astype(bf)
    row_grad = inverse * (
        hat_own
        - jnp.mean(hat_own, -1, keepdims=True)
        - normalized * jnp.mean(hat_own * normalized, -1, keepdims=True)
    )
    input_grad = (seeds + row_grad).astype(bf)

    return (
        layer_output,
        input_grad,
        sums[0],
        sums[1],
        wide(joined_grad),
        sums[4:7].reshape(-1),
        wide(os_grad[:part]),
        sums[7],
        sums[2],
        sums[3],
        wide(expand_grad),
        sums[8:12].reshape(-1),
        wide(os_grad[part:]),
        sums[7],
    )


def solution(mesh):
    n = mesh.shape["fsdp"]
    fits = n == HEADS and mesh.shape["rep"] == 2
    chosen = functools.partial(head_body, n) if fits else body
    placed = (
        P(("rep", "fsdp"), None),
        P(("rep", "fsdp"), None),
        P(("rep", "fsdp"), None),
        P("fsdp"),
        P("fsdp"),
        P("fsdp", None),
        P("fsdp"),
        P("fsdp", None),
        P("fsdp"),
        P("fsdp"),
        P("fsdp"),
        P("fsdp", None),
        P("fsdp"),
        P("fsdp", None),
        P("fsdp"),
        P(("rep", "fsdp"), None),
    )
    return jax.shard_map(
        chosen,
        mesh=mesh,
        in_specs=placed,
        out_specs=(
            P(("rep", "fsdp"), None),
            P(("rep", "fsdp"), None),
            P("fsdp"),
            P("fsdp"),
            P("fsdp", None),
            P("fsdp"),
            P("fsdp", None),
            P("fsdp"),
            P("fsdp"),
            P("fsdp"),
            P("fsdp", None),
            P("fsdp"),
            P("fsdp", None),
            P("fsdp"),
        ),
        check_vma=False,
    )
```

```python
import functools

import jax
import jax.numpy as jnp
import numpy as np
from jax import lax
from jax.experimental import pallas as pl
from jax.experimental.pallas import tpu as pltpu
from jax.sharding import PartitionSpec as P

D = 2048
HEADS = 16
HEAD_DIM = 128
ROT = 32


epsilon = 1e-05
masked_score = -1e30
rotary_base = 10000.0


def as_sent(shard):
    return jax.tree.map(lambda a: a.astype(jnp.bfloat16) if a.dtype == jnp.float32 else a, shard)


def norm_rows(rows, gain, shift):
    centre = jnp.mean(rows, -1, keepdims=True)
    centred = rows - centre
    inverse = lax.rsqrt(jnp.mean(centred * centred, -1, keepdims=True) + epsilon)
    normalized = centred * inverse
    return (normalized * gain.astype(jnp.float32) + shift.astype(jnp.float32), normalized, inverse)


def norm_back(normed_grad, normalized, inverse, gain):
    scaled = normed_grad * gain.astype(jnp.float32)
    row_grad = inverse * (
        scaled
        - jnp.mean(scaled, -1, keepdims=True)
        - normalized * jnp.mean(scaled * normalized, -1, keepdims=True)
    )
    return (row_grad, jnp.sum(normed_grad * normalized, 0), jnp.sum(normed_grad, 0))


def rotary_tables(segment):
    length = segment.shape[-1]
    places = jnp.arange(length, dtype=jnp.int32)
    earlier = jnp.sum((segment[..., None, :] < segment[..., :, None]).astype(jnp.int32), -1)
    position = (places - earlier).astype(jnp.float32)
    exponent = jnp.arange(ROT // 2, dtype=jnp.float32) * 2.0 / ROT
    frequency = jnp.power(jnp.float32(rotary_base), -exponent)
    angle = position[..., None] * frequency
    return (jnp.cos(angle), jnp.sin(angle))


def turn(heads, cosine, sine, sign):
    half = ROT // 2
    front = heads[..., :half]
    behind = heads[..., half:ROT]
    cos_wide = cosine[..., None, :]
    sin_wide = sine[..., None, :] * sign
    return jnp.concatenate(
        [
            front * cos_wide - behind * sin_wide,
            behind * cos_wide + front * sin_wide,
            heads[..., ROT:],
        ],
        -1,
    )


def gelu_slope(values):
    return (
        0.5 * (1.0 + lax.erf(values * 0.7071067811865476))
        + values * jnp.exp(-0.5 * values * values) * 0.3989422804014327
    )


def attention_inputs(rows, weights, cosine, sine):
    gain, shift, joined_weight, joined_bias = (weights[0], weights[1], weights[2], weights[3])
    normed, normalized, inverse = norm_rows(rows, gain, shift)
    normed_low = normed.astype(jnp.bfloat16)
    joined = jnp.dot(
        normed_low, joined_weight, preferred_element_type=jnp.float32
    ) + joined_bias.astype(jnp.float32)
    length = rows.shape[0]
    split = joined.reshape(length, 3, HEADS, HEAD_DIM)
    queries = turn(split[:, 0], cosine, sine, 1.0).astype(jnp.bfloat16)
    keys = turn(split[:, 1], cosine, sine, 1.0).astype(jnp.bfloat16)
    values = split[:, 2].astype(jnp.bfloat16)
    return (normed_low, normalized, inverse, queries, keys, values)


def score_block(queries, keys, allowed):
    scores = jnp.einsum(
        "thd,shd->hts", queries, keys, preferred_element_type=jnp.float32
    ) * HEAD_DIM ** (-0.5)
    return jnp.where(allowed[None], scores, masked_score)


def feedforward_inputs(rows, weights):
    gain, shift, expand_weight, expand_bias = (weights[0], weights[1], weights[2], weights[3])
    normed, normalized, inverse = norm_rows(rows, gain, shift)
    normed_low = normed.astype(jnp.bfloat16)
    expanded = jnp.dot(
        normed_low, expand_weight, preferred_element_type=jnp.float32
    ) + expand_bias.astype(jnp.float32)
    return (normed_low, normalized, inverse, expanded)


def body(
    layer_input,
    segment,
    live_mask,
    attention_gain,
    attention_shift,
    joined_weight,
    joined_bias,
    output_weight,
    output_bias,
    feedforward_gain,
    feedforward_shift,
    expand_weight,
    expand_bias,
    shrink_weight,
    shrink_bias,
    cotangent,
):
    rows = layer_input.astype(jnp.float32)
    seg_row = segment[0]
    live_rows = live_mask[0].astype(jnp.float32)[:, None]
    length = seg_row.shape[0]
    cosine, sine = rotary_tables(seg_row)
    places = jnp.arange(length, dtype=jnp.int32)
    allowed = (seg_row[:, None] == seg_row[None, :]) & (places[None, :] <= places[:, None])
    attention_parts = (
        attention_gain,
        attention_shift,
        joined_weight,
        joined_bias,
        output_weight,
        output_bias,
    )
    feedforward_parts = (
        feedforward_gain,
        feedforward_shift,
        expand_weight,
        expand_bias,
        shrink_weight,
        shrink_bias,
    )
    attention_full = (
        lax.all_gather(attention_gain, "fsdp", axis=0, tiled=True),
        lax.all_gather(attention_shift, "fsdp", axis=0, tiled=True),
        lax.all_gather(joined_weight, "fsdp", axis=0, tiled=True),
        lax.all_gather(joined_bias, "fsdp", axis=0, tiled=True),
        lax.all_gather(output_weight, "fsdp", axis=0, tiled=True),
        lax.all_gather(output_bias, "fsdp", axis=0, tiled=True),
    )
    feedforward_full = (
        lax.all_gather(feedforward_gain, "fsdp", axis=0, tiled=True),
        lax.all_gather(feedforward_shift, "fsdp", axis=0, tiled=True),
        lax.all_gather(expand_weight, "fsdp", axis=0, tiled=True),
        lax.all_gather(expand_bias, "fsdp", axis=0, tiled=True),
        lax.all_gather(shrink_weight, "fsdp", axis=0, tiled=True),
        lax.all_gather(shrink_bias, "fsdp", axis=0, tiled=True),
    )
    normed_one, normalized_one, inverse_one, queries, keys, values = attention_inputs(
        rows, attention_full, cosine, sine
    )
    scores = score_block(queries, keys, allowed)
    top = jnp.max(scores, -1, keepdims=True)
    expo = jnp.exp(scores - top)
    total = jnp.sum(expo, -1, keepdims=True)
    log_total = top + jnp.log(total)
    probs_low = (expo / total).astype(jnp.bfloat16)
    mixed = jnp.einsum("hts,shd->thd", probs_low, values, preferred_element_type=jnp.float32)
    mixed = mixed.reshape(length, D).astype(jnp.bfloat16)
    attended = jnp.dot(
        mixed, attention_full[4], preferred_element_type=jnp.float32
    ) + attention_full[5].astype(jnp.float32)
    normed_two, normalized_two, inverse_two, expanded = feedforward_inputs(rows, feedforward_full)
    activated = jax.nn.gelu(expanded, approximate=False).astype(jnp.bfloat16)
    shrunk = jnp.dot(
        activated, feedforward_full[4], preferred_element_type=jnp.float32
    ) + feedforward_full[5].astype(jnp.float32)
    layer_output = (rows + live_rows * (attended + shrunk)).astype(jnp.bfloat16)
    seed_rows = cotangent.astype(jnp.float32)
    branch_grad = (live_rows * seed_rows).astype(jnp.bfloat16)
    branch_total = jnp.sum(branch_grad.astype(jnp.float32), 0)
    feedforward_back = lax.all_gather(
        as_sent(lax.optimization_barrier((feedforward_parts, layer_output))[0]),
        "fsdp",
        axis=0,
        tiled=True,
    )
    normed_two, normalized_two, inverse_two, expanded = feedforward_inputs(rows, feedforward_back)
    activated = jax.nn.gelu(expanded, approximate=False).astype(jnp.bfloat16)
    shrink_weight_grad = jnp.einsum(
        "tf,td->fd", activated, branch_grad, preferred_element_type=jnp.float32
    )
    activated_grad = jnp.einsum(
        "td,fd->tf", branch_grad, feedforward_back[4], preferred_element_type=jnp.float32
    )
    expanded_grad = (activated_grad * gelu_slope(expanded)).astype(jnp.bfloat16)
    expand_bias_grad = jnp.sum(expanded_grad.astype(jnp.float32), 0)
    expand_weight_grad = jnp.einsum(
        "td,tf->df", normed_two, expanded_grad, preferred_element_type=jnp.float32
    )
    normed_two_grad = jnp.einsum(
        "tf,df->td", expanded_grad, feedforward_back[2], preferred_element_type=jnp.float32
    )
    rows_grad_two, ff_gain_grad, ff_shift_grad = norm_back(
        normed_two_grad, normalized_two, inverse_two, feedforward_back[0]
    )
    ff_terms = (
        ff_gain_grad,
        ff_shift_grad,
        expand_weight_grad,
        expand_bias_grad,
        shrink_weight_grad,
        branch_total,
    )
    ff_parts = (
        lax.psum_scatter(ff_terms[0], "fsdp", scatter_dimension=0, tiled=True),
        lax.psum_scatter(ff_terms[1], "fsdp", scatter_dimension=0, tiled=True),
        lax.psum_scatter(ff_terms[2], "fsdp", scatter_dimension=0, tiled=True),
        lax.psum_scatter(ff_terms[3], "fsdp", scatter_dimension=0, tiled=True),
        lax.psum_scatter(ff_terms[4], "fsdp", scatter_dimension=0, tiled=True),
        lax.psum_scatter(ff_terms[5], "fsdp", scatter_dimension=0, tiled=True),
    )
    attention_back = lax.all_gather(
        as_sent(lax.optimization_barrier((attention_parts, layer_output))[0]),
        "fsdp",
        axis=0,
        tiled=True,
    )
    normed_one, normalized_one, inverse_one, queries, keys, values = attention_inputs(
        rows, attention_back, cosine, sine
    )
    scores = score_block(queries, keys, allowed)
    probs = jnp.exp(scores - log_total)
    probs_low = probs.astype(jnp.bfloat16)
    mixed = jnp.einsum("hts,shd->thd", probs_low, values, preferred_element_type=jnp.float32)
    mixed = mixed.reshape(length, D).astype(jnp.bfloat16)
    output_weight_grad = jnp.einsum(
        "td,te->de", mixed, branch_grad, preferred_element_type=jnp.float32
    )
    mixed_grad = jnp.einsum(
        "te,de->td", branch_grad, attention_back[4], preferred_element_type=jnp.float32
    )
    mixed_grad = mixed_grad.astype(jnp.bfloat16).reshape(length, HEADS, HEAD_DIM)
    value_grad = jnp.einsum(
        "hts,thd->shd", probs_low, mixed_grad, preferred_element_type=jnp.float32
    )
    probs_grad = jnp.einsum("thd,shd->hts", mixed_grad, values, preferred_element_type=jnp.float32)
    scores_grad = (probs * (probs_grad - jnp.sum(probs_grad * probs, -1, keepdims=True))).astype(
        jnp.bfloat16
    )
    query_grad = jnp.einsum(
        "hts,shd->thd", scores_grad, keys, preferred_element_type=jnp.float32
    ) * HEAD_DIM ** (-0.5)
    key_grad = jnp.einsum(
        "hts,thd->shd", scores_grad, queries, preferred_element_type=jnp.float32
    ) * HEAD_DIM ** (-0.5)
    query_grad = turn(query_grad, cosine, sine, -1.0)
    key_grad = turn(key_grad, cosine, sine, -1.0)
    joined_grad = jnp.concatenate(
        [query_grad.reshape(length, D), key_grad.reshape(length, D), value_grad.reshape(length, D)],
        1,
    ).astype(jnp.bfloat16)
    joined_bias_grad = jnp.sum(joined_grad.astype(jnp.float32), 0)
    joined_weight_grad = jnp.einsum(
        "td,te->de", normed_one, joined_grad, preferred_element_type=jnp.float32
    )
    normed_one_grad = jnp.einsum(
        "te,de->td", joined_grad, attention_back[2], preferred_element_type=jnp.float32
    )
    rows_grad_one, at_gain_grad, at_shift_grad = norm_back(
        normed_one_grad, normalized_one, inverse_one, attention_back[0]
    )
    at_terms = (
        at_gain_grad,
        at_shift_grad,
        joined_weight_grad,
        joined_bias_grad,
        output_weight_grad,
        branch_total,
    )
    at_parts = (
        lax.psum_scatter(at_terms[0], "fsdp", scatter_dimension=0, tiled=True),
        lax.psum_scatter(at_terms[1], "fsdp", scatter_dimension=0, tiled=True),
        lax.psum_scatter(at_terms[2], "fsdp", scatter_dimension=0, tiled=True),
        lax.psum_scatter(at_terms[3], "fsdp", scatter_dimension=0, tiled=True),
        lax.psum_scatter(at_terms[4], "fsdp", scatter_dimension=0, tiled=True),
        lax.psum_scatter(at_terms[5], "fsdp", scatter_dimension=0, tiled=True),
    )
    input_grad = (seed_rows + rows_grad_one + rows_grad_two).astype(jnp.bfloat16)
    summed = (
        lax.psum(at_parts[0].astype(jnp.bfloat16), "rep").astype(jnp.float32),
        lax.psum(at_parts[1].astype(jnp.bfloat16), "rep").astype(jnp.float32),
        lax.psum(at_parts[2].astype(jnp.bfloat16), "rep").astype(jnp.float32),
        lax.psum(at_parts[3].astype(jnp.bfloat16), "rep").astype(jnp.float32),
        lax.psum(at_parts[4].astype(jnp.bfloat16), "rep").astype(jnp.float32),
        lax.psum(at_parts[5].astype(jnp.bfloat16), "rep").astype(jnp.float32),
        lax.psum(ff_parts[0].astype(jnp.bfloat16), "rep").astype(jnp.float32),
        lax.psum(ff_parts[1].astype(jnp.bfloat16), "rep").astype(jnp.float32),
        lax.psum(ff_parts[2].astype(jnp.bfloat16), "rep").astype(jnp.float32),
        lax.psum(ff_parts[3].astype(jnp.bfloat16), "rep").astype(jnp.float32),
        lax.psum(ff_parts[4].astype(jnp.bfloat16), "rep").astype(jnp.float32),
        lax.psum(ff_parts[5].astype(jnp.bfloat16), "rep").astype(jnp.float32),
    )
    return (
        layer_output,
        input_grad,
        summed[0],
        summed[1],
        summed[2],
        summed[3],
        summed[4],
        summed[5],
        summed[6],
        summed[7],
        summed[8],
        summed[9],
        summed[10],
        summed[11],
    )


MESH = pl.DeviceIdType.MESH
bf = jnp.bfloat16
f32 = jnp.float32
WIDE = 2048
TOK = 2048


def ds(start, size):
    return pl.ds(pl.multiple_of(start, size), size)


def mm(a, b, ca, cb):
    return lax.dot_general(a, b, (((ca,), (cb,)), ((), ())), preferred_element_type=f32)


def layer_kernel(
    x_ref, bg_ref, sm_ref, jw_ref, ew_ref, wo_ref, ws_ref, ct_ref, eb_ref,
    SO1, SO2, OSo, JWo, EWo, FIN, SMO,
    X, BG, WJ, WE, WOS, INNER, QKV, SLOPE, CT, PR, L1, RING, A1, B1, C1, A2,
    JB, RX, OSB, ROS, T1, SM, SMF, CV, GBR, VEC, VR, TOT, TX, BSUM,
    su, sd, sy, ss, rx_, bu, bd, by, bs, rb_, sw, rw, sxw, rxw, ssm, rsm,
    sa, ra, sbb, rbb, sc, rc_, sx, rxx, so, ro, so2, ro2, sg, rg, sf, rf, sv, rv, st_, rt_, lsem, ready,
):
    r = lax.axis_index("rep")
    f = lax.axis_index("fsdp")
    z = f // 4
    y = (f // 2) % 2
    c = f % 2
    sib = (r, z * 4 + y * 2 + (1 - c))
    yo = z * 4 + (1 - y) * 2 + c
    yp = (r, yo)
    xp = (1 - r, f)
    lower = z <= 1
    zz = jnp.where(lower, z, 3 - z)

    def phys(q):
        return jnp.where(lower, q, 3 - q)

    f_in = (r, jnp.where(lower, f + 4, f - 4))
    f_out = (r, jnp.where(lower, f - 4, f + 4))

    barrier = pltpu.get_barrier_semaphore()

    @pl.loop(1, 16)
    def _(k):
        pl.semaphore_signal(barrier, inc=1, device_id=(r, (f + k) % 16), device_id_type=MESH)

    pl.semaphore_signal(barrier, inc=1, device_id=xp, device_id_type=MESH)
    pl.semaphore_wait(barrier, 16)

    def rc(src, dst, s, q, dev):
        return pltpu.make_async_remote_copy(
            src_ref=src, dst_ref=dst, send_sem=s, recv_sem=q, device_id=dev, device_id_type=MESH
        )

    def lc(src, dst, s):
        return pltpu.make_async_copy(src, dst, s)

    def gather(own, OUT, su, sd, sy, ss, rr):
        def item(i):
            return OUT.at[ds(128 * i, 128)]

        def up(i, src=None):
            return rc(item(i) if src is None else src, item(i), su.at[i], rr.at[i], (r, f + 4))

        def dn(i, src=None):
            return rc(item(i) if src is None else src, item(i), sd.at[i], rr.at[i], (r, f - 4))

        def ac(i, src=None):
            return rc(item(i) if src is None else src, item(i), sy.at[i], rr.at[i], yp)

        def sb(i, src=None):
            return rc(item(i) if src is None else src, item(i), ss.at[i], rr.at[i], sib)

        def begin_z():
            pl.when(z < 3)(lambda: up(f, own).start())
            pl.when(z > 0)(lambda: dn(f, own).start())

        def begin_y():
            ac(f, own).start()
            sb(f, own).start()

        def step(s):
            @pl.when(z - s >= 0)
            def _():
                i = f - 4 * s
                up(i).wait_recv()
                pl.when(z < 3)(lambda: up(i).start())
                ac(i).start()
                sb(i).start()

            @pl.when(z + s <= 3)
            def _():
                i = f + 4 * s
                dn(i).wait_recv()
                pl.when(z > 0)(lambda: dn(i).start())
                ac(i).start()
                sb(i).start()

        def ystep(s):
            @pl.when(z - s >= 0)
            def _():
                ac(yo - 4 * s).wait_recv()
                sb(yo - 4 * s).start()

            @pl.when((s > 0) & (z + s <= 3))
            def _():
                ac(yo + 4 * s).wait_recv()
                sb(yo + 4 * s).start()

        def landed(q):
            for v in range(2):
                sb(4 * q + 2 * v + 1 - c).wait_recv()

        def finish():
            @pl.loop(0, 8)
            def _(k):
                sb(2 * k + c).wait_send()

            @pl.loop(0, 4)
            def _(k):
                i = k * 4 + y * 2 + c
                ac(i).wait_send()
                pl.when((k <= z) & (z < 3))(lambda: up(i).wait_send())
                pl.when((k >= z) & (z > 0))(lambda: dn(i).wait_send())

        return begin_z, begin_y, step, ystep, landed, finish

    xz, xo, xs, xy, xl, xf = gather(x_ref, X, su, sd, sy, ss, rx_)
    gz, go, gs, gy, gl, gf = gather(bg_ref, BG, bu, bd, by, bs, rb_)

    def wpieces(src, dst, from_arg):
        rows = ds(128 * src + 64 * r, 64)
        out = []
        for t in range(3):
            d = WJ.at[rows, pl.ds(128 * t, 128)]
            out.append((jw_ref.at[ds(64 * r, 64), ds(2048 * t + 128 * dst, 128)] if from_arg else d, d))
        d = WE.at[rows]
        out.append((ew_ref.at[ds(64 * r, 64), ds(512 * dst, 512)] if from_arg else d, d))
        return out

    def fwd(lo, hi):
        @pl.loop(lo, hi)
        def _(k):
            fs = (f + 16 - k) % 16
            for t, (s, d) in enumerate(wpieces(fs, f, False)):
                rc(s, d, sw.at[fs, t], rw.at[fs, t], (r, f)).wait_recv()
                rc(s, d, sxw.at[fs, t], rxw.at[fs, t], xp).start()

    own_x = lc(x_ref, X.at[ds(128 * f, 128)], lsem.at[0])
    own_b = lc(bg_ref, BG.at[ds(128 * f, 128)], lsem.at[1])
    load_o = lc(wo_ref, WOS.at[pl.ds(0, 128)], lsem.at[2])
    load_s = lc(ws_ref, WOS.at[pl.ds(128, 512)], lsem.at[3])
    own_s = lc(sm_ref, SM.at[f], lsem.at[4])
    def wsend(lo, hi):
        @pl.loop(lo, hi)
        def _(k):
            fd = (f + k) % 16
            for t, (s, d) in enumerate(wpieces(f, fd, True)):
                rc(s, d, sw.at[fd, t], rw.at[f, t], (r, fd)).start()

    def ssend():
        @pl.loop(1, 16)
        def _(k):
            fd = (f + k) % 16
            rc(sm_ref, SM.at[f], ssm.at[fd], rsm.at[f], (r, fd)).start()

    def wown():
        for t, (s, d) in enumerate(wpieces(f, f, True)):
            rc(s, d, sxw.at[f, t], rxw.at[f, t], xp).start()
            lc(s, d, rw.at[f, t]).start()

    for cp in (own_x, own_b, load_o, load_s, own_s):
        cp.start()
    ssend()
    wsend(1, 16)
    wown()
    xo()
    xz()
    go()
    fwd(1, 13)
    own_s.wait()

    @pl.loop(1, 16)
    def _(k):
        fs = (f + k) % 16
        other = rc(sm_ref, SM.at[fs], ssm.at[fs], rsm.at[fs], (r, fs))
        other.wait_recv()
        other.wait_send()

    @pl.loop(0, 16)
    def _(i):
        SMF[ds(16 * i, 16)] = SM[i].astype(f32)

    send_small = lc(SMF, SMO, lsem.at[4])
    send_small.start()

    @pl.loop(0, 16)
    def _(i):
        rows = ds(128 * i, 128)
        place = jnp.broadcast_to(SMF[pl.ds(16 * i + 10, 1)], (128, 128)).T
        pick = (place == lax.broadcasted_iota(jnp.int32, (128, 128), 1).astype(f32)).astype(f32)
        hi = lax.Precision.HIGHEST
        CT[rows] = jnp.dot(pick, ct_ref[...], precision=hi, preferred_element_type=f32)

    fwd(13, 16)
    xs(1)

    for t, (s, d) in enumerate(wpieces(f, f, True)):
        lc(s, d, rw.at[f, t]).wait()
    other_half = lambda src: ds(128 * src + 64 * (1 - r), 64)

    @pl.loop(0, 16)
    def _(fs):
        for t in range(4):
            d = WJ.at[other_half(fs), pl.ds(128 * t, 128)] if t < 3 else WE.at[other_half(fs)]
            cp = rc(d, d, sxw.at[fs, t], rxw.at[fs, t], xp)
            cp.wait_recv()
            cp.wait_send()

    load_o.wait()
    load_s.wait()

    def columns(j):
        for v in range(4):
            PR[pl.ds(128 * v, 128)] = jnp.broadcast_to(SMF[pl.ds(16 * j + v, 1)], (128, 128)).T

    def fold(v):
        return v[:8] + v[8:]

    CV[...] = jnp.zeros_like(CV)

    @pl.loop(0, 16)
    def _(j):
        columns(j)

        @pl.loop(0, 8)
        def _(k):
            w = ds(128 * j + 16 * k, 16)
            cw = ds(16 * k, 16)
            g1, s1, g2, s2 = (PR[ds(128 * v + 16 * k, 16)] for v in range(4))
            for t in range(3):
                l = pl.ds(128 * t, 128)
                v = WJ[w, l].astype(f32)
                CV[:, l] += fold(v * s1)
                WJ[w, l] = (v * g1).astype(bf)
            for t in range(4):
                l = pl.ds(128 * t, 128)
                lo = pl.ds(384 + 128 * t, 128)
                v = WE[w, l].astype(f32)
                CV[:, lo] += fold(v * s2)
                WE[w, l] = (v * g2).astype(bf)

    CV[...] = jnp.broadcast_to(jnp.sum(CV[...], 0, keepdims=True), CV.shape)
    for t in range(3):
        place = (16 * t + f) // 3 * 16 + 6 + (16 * t + f) % 3
        CV[:, pl.ds(128 * t, 128)] += SMF[pl.ds(place, 1)]
    CV[:, pl.ds(384, 512)] += eb_ref[...]

    lane = lax.broadcasted_iota(jnp.int32, (16, 128), 1)

    def angles(v, ln):
        return jnp.where(ln < 32, v, 1.0), jnp.where(ln < 32, pltpu.roll(v, 96, 1), 0.0)

    def swap(v, ln):
        return jnp.where(ln < 16, pltpu.roll(v, 112, 1), pltpu.roll(v, 16, 1))

    scale = HEAD_DIM ** (-0.5)
    down = lax.broadcasted_iota(jnp.int32, (128, 128), 0)
    across = lax.broadcasted_iota(jnp.int32, (128, 128), 1)

    own_x.wait()

    @pl.loop(0, 4)
    def _(p):
        i = phys(jnp.where((zz == 1) & (p < 2), 1 - p, p))
        rows = ds(512 * i, 512)
        pl.when((p > 0) & (p < 3))(lambda: xs(p + 1))
        @pl.when(p == 1)
        def _():
            gz()

        xy(p)
        xl(i)
        T1[:, pl.ds(0, 384)] = mm(X[rows], WJ[...], 1, 0)
        T1[:, pl.ds(384, 512)] = mm(X[rows], WE[...], 1, 0)

        @pl.loop(0, 32, unroll=2)
        def _(k):
            w = ds(16 * k, 16)
            gw = ds(512 * i + 16 * k, 16)
            cos, sin = angles(CT[gw], lane)
            for t in range(2):
                l = pl.ds(128 * t, 128)
                v = T1[w, l] + CV[0:1, l]
                QKV[gw, l] = (v * cos + swap(v, lane) * sin).astype(bf)
            l = pl.ds(256, 128)
            QKV[gw, l] = (T1[w, l] + CV[0:1, l]).astype(bf)
            for t in range(4):
                l = pl.ds(384 + 128 * t, 128)
                v = T1[w, l] + CV[0:1, l]
                part = 0.5 * (1.0 + lax.erf(v * 0.7071067811865476))
                INNER[gw, pl.ds(128 + 128 * t, 128)] = (v * part).astype(bf)
                SLOPE[gw, pl.ds(128 * t, 128)] = (
                    part + v * jnp.exp(-0.5 * v * v) * 0.3989422804014327
                ).astype(bf)

        @pl.loop(0, 4, unroll=2)
        def _(j):
            slot = 4 * i + j
            rows = ds(128 * slot, 128)
            q = QKV[rows, pl.ds(0, 128)]
            k = QKV[rows, pl.ds(128, 128)]
            v = QKV[rows, pl.ds(256, 128)]
            seg = jnp.broadcast_to(SMF[pl.ds(16 * slot + 9, 1)], (128, 128))
            s = mm(q, k, 1, 1) * scale
            s = jnp.where((seg == seg.T) & (across <= down), s, masked_score)
            e = jnp.exp(s - jnp.max(s, -1, keepdims=True))
            p = e / jnp.sum(e, -1, keepdims=True)
            PR[rows] = p
            INNER[rows, pl.ds(0, 128)] = mm(p.astype(bf), v, 1, 0).astype(bf)

        @pl.when(p == 2)
        def _():
            gs(1)
            gy(0)

        @pl.when(p == 3)
        def _():
            gs(2)
            gy(1)


    xf()

    def add_into(dst, src, rows):
        @pl.loop(0, rows // 16)
        def _(i):
            w = ds(i * 16, 16)
            dst[w] = (dst[w].astype(f32) + src[w].astype(f32)).astype(bf)

    def reducer(n, sent, own, AA, BB, CC, CX, SO):
        def a_send(k):
            return rc(sent(k), AA(k), sa.at[n, k], ra.at[n, k], sib)

        def b_send(zp):
            return rc(own(zp * 2 + 1 - y), BB(zp), sbb.at[n, zp], rbb.at[n, zp], yp)

        def prep(k):
            a_send(k).wait_recv()
            add_into(own(k), AA(k), 128)

        def far(*turns):
            for q in turns or (3, 0, 2, 1):
                prep(phys(q) * 2 + 1 - y)
                b_send(phys(q)).start()

        def near(q):
            zp = phys(q)
            k = zp * 2 + y
            prep(k)
            b_send(zp).wait_recv()
            add_into(own(k), BB(zp), 128)

        def got(q, extra=False):
            zp = phys(q)
            buf = CX if extra else CC(zp)
            slot = 4 if extra else zp
            rc(buf, buf, sc.at[n, zp], rc_.at[n, slot], f_in).wait_recv()
            return buf

        def send(q, dev, extra=False):
            zp = phys(q)
            return rc(
                own(zp * 2 + y), CX if extra else CC(zp), sc.at[n, zp], rc_.at[n, 4 if extra else zp], dev
            )

        def step(q):
            near(q)
            if q > 0:
                pl.when(zz == 0)(lambda: send(q, f_in).start())

        def relay(q):
            k = phys(q) * 2 + y

            @pl.when(zz == 1)
            def _():
                if q >= 2:
                    add_into(own(k), got(q), 128)
                    send(q, f_in, q == 2).start()
                if q == 0:
                    add_into(own(k), got(q), 128)
                    send(q, f_out).start()

        def total(q, bufs):
            k = phys(q) * 2 + y

            @pl.loop(0, 8)
            def _(i):
                w = ds(i * 16, 16)
                v = own(k)[w].astype(f32)
                for b in bufs:
                    v = v + b[w].astype(f32)
                for l, n in enumerate((896, 896, 256)):
                    T1[ds(128 * l + 16 * i, 16), pl.ds(0, n)] = v[:, 896 * l : 896 * l + n]

        def last():
            @pl.when(zz == 0)
            def _():
                total(0, [got(0)])

            @pl.when(zz == 1)
            def _():
                total(1, [got(1), got(1, True)])

            cps = [
                lc(T1.at[pl.ds(128 * l, 128), pl.ds(0, n)], SO.at[:, pl.ds(896 * l, n)], lsem.at[at])
                for l, n, at in ((0, 896, 5), (1, 896, 10), (2, 256, 11))
            ]
            for cp in cps:
                cp.start()
            for cp in cps:
                cp.wait()

        def drain(first=0):
            @pl.loop(first, 8)
            def _(k):
                a_send(k).wait_send()

            @pl.loop(0, 4)
            def _(zp):
                b_send(zp).wait_send()

            for q in range(4):
                if q > 0:
                    pl.when(zz == 0)(lambda: send(q, f_in).wait_send())
                if q >= 2:
                    pl.when(zz == 1)(lambda: send(q, f_in, q == 2).wait_send())
                if q == 0:
                    pl.when(zz == 1)(lambda: send(q, f_out).wait_send())

        return a_send, far, step, last, drain, relay

    R1 = reducer(
        0, lambda k: RING.at[k % 3], lambda k: L1.at[k], lambda k: A1.at[k], lambda k: B1.at[k],
        lambda k: C1.at[k], C1.at[4], SO1,
    )
    R2 = reducer(
        1,
        lambda k: BG.at[ds(128 * (2 * k + 1 - c), 128)],
        lambda k: BG.at[ds(128 * (2 * k + c), 128)],
        lambda k: A2.at[k],
        lambda k: RING.at[k],
        lambda k: WOS.at[ds(128 * k, 128)],
        WOS.at[pl.ds(512, 128)],
        SO2,
    )

    @pl.loop(0, 8)
    def _(b):
        res = mm(INNER[ds(256 * b, 256)], WOS[...], 1, 0)

        @pl.when(b >= 3)
        def _():
            R1[0](b - 3).wait_send()

        for side in range(2):
            @pl.when(c == side)
            def _():
                L1[b] = res[128 * side : 128 * side + 128].astype(bf)
                RING[b % 3] = res[128 - 128 * side : 256 - 128 * side].astype(bf)

        R1[0](b).start()

        @pl.when(b == 2)
        def _():
            gs(3)
            gy(2)

    gy(3)
    own_b.wait()
    for q in range(4):
        gl(q)
    gf()

    half = ds(320 * r, 320)
    away = ds(320 * (1 - r), 320)

    def o1(j):
        return rc(OSB.at[j, away], ROS.at[j], so.at[j], ro.at[j], xp)

    def o2(j):
        return rc(OSB.at[j, half], OSo.at[half, ds(512 * j, 512)], so2.at[j], ro2.at[j], xp)

    def o2r(j):
        return rc(OSB.at[j, half], OSo.at[away, ds(512 * j, 512)], so2.at[j], ro2.at[j], xp)

    def os_store(j):
        return lc(OSB.at[j, half], OSo.at[half, ds(512 * j, 512)], lsem.at[6 + j])

    def os_step(j):
        o1(j).wait_recv()
        add_into(OSB.at[j, half], ROS.at[j], 320)
        o2(j).start()
        os_store(j).start()

    def os_drain():
        for j in range(4):
            o1(j).wait_send()
            o2(j).wait_send()
            o2r(j).wait_recv()
            os_store(j).wait()

    @pl.loop(0, 4)
    def _(j):
        OSB[j] = mm(INNER[...], BG[:, ds(512 * j, 512)], 0, 0).astype(bf)
        o1(j).start()

    R1[1]()

    GBR[...] = jnp.zeros_like(GBR)
    VEC[...] = jnp.zeros_like(VEC)
    TOT[...] = jnp.zeros_like(TOT)
    mine = BG[:, ds(128 * f, 128)].astype(f32)
    BSUM[...] = jnp.sum(mine, 0, keepdims=True)

    def fold_rows(v, rows):
        return jnp.sum(v.reshape(rows // 8, 8, v.shape[-1]), 0)

    @pl.loop(0, 4)
    def _(i):
        rows = ds(512 * i, 512)
        T1[:, pl.ds(0, 640)] = mm(BG[rows], WOS[...], 1, 1)

        @pl.loop(0, 32, unroll=2)
        def _(k):
            w = ds(16 * k, 16)
            gw = ds(512 * i + 16 * k, 16)
            INNER[gw, pl.ds(0, 128)] = T1[w, pl.ds(0, 128)].astype(bf)
            e = (T1[w, pl.ds(128, 512)] * SLOPE[gw].astype(f32)).astype(bf)
            SLOPE[gw] = e
            GBR[:, pl.ds(384, 512)] += fold(e.astype(f32))

    @pl.loop(5, 8)
    def _(b):
        R1[0](b).wait_send()

    for dev in (sib, yp, f_in):
        pl.semaphore_signal(ready, inc=1, device_id=dev, device_id_type=MESH)

    @pl.when(zz == 1)
    def _():
        pl.semaphore_signal(ready, inc=1, device_id=f_out, device_id_type=MESH)

    os_step(0)
    os_step(1)

    lane_b = lax.broadcasted_iota(jnp.int32, (128, 128), 1)

    @pl.loop(0, 16, unroll=2)
    def _(i):
        rows = ds(128 * i, 128)
        q = QKV[rows, pl.ds(0, 128)]
        k = QKV[rows, pl.ds(128, 128)]
        v = QKV[rows, pl.ds(256, 128)]
        p = PR[rows]
        mg = INNER[rows, pl.ds(0, 128)]
        vg = mm(p.astype(bf), mg, 0, 0)
        pg = mm(mg, v, 1, 1)
        sgr = (p * (pg - jnp.sum(pg * p, -1, keepdims=True))).astype(bf)
        cos, sin = angles(CT[rows], lane_b)
        qg = mm(sgr, k, 1, 0) * scale
        kg = mm(sgr, q, 0, 0) * scale
        for t, g in enumerate((qg, kg, vg)):
            if t < 2:
                g = g * cos - swap(g, lane_b) * sin
            g = g.astype(bf)
            l = pl.ds(128 * t, 128)
            QKV[rows, l] = g
            GBR[:, l] += fold_rows(g.astype(f32), 128)

    os_step(2)
    os_step(3)
    GBR[...] = jnp.broadcast_to(jnp.sum(GBR[...], 0, keepdims=True), GBR.shape)

    keep = ds(64 * r, 64)
    give = ds(64 * (1 - r), 64)

    def x1(g):
        return rc(JB.at[ds(4 * g, 4), give], RX.at[ds(4 * g, 4)], sx.at[g], rxx.at[g], xp)

    def place_of(fs, t, rows):
        if t < 3:
            return JWo.at[rows, ds(2048 * t + 128 * fs, 128)]
        return EWo.at[rows, ds(512 * fs, 512)]

    def piece_of(fd, t):
        return JB.at[fd, keep, pl.ds(128 * t, 128)] if t < 3 else JB.at[fd, keep, pl.ds(384, 512)]

    def je_group(g):
        x1(g).wait_recv()

        @pl.loop(0, 4)
        def _(j):
            fd = 4 * g + j
            add_into(JB.at[fd, keep], RX.at[fd], 64)

            @pl.when(fd != f)
            def _():
                for t in range(4):
                    rc(piece_of(fd, t), place_of(f, t, keep), sg.at[fd, t], rg.at[f, t], (r, fd)).start()

            @pl.when(fd == f)
            def _():
                for t in range(4):
                    lc(piece_of(fd, t), place_of(f, t, keep), sg.at[fd, t]).start()
                    rc(piece_of(fd, t), place_of(f, t, keep), sf.at[fd, t], rf.at[f, t], xp).start()

    def fwd_group(g):
        @pl.loop(4 * g, 4 * g + 4)
        def _(fs):
            @pl.when(fs != f)
            def _():
                for t in range(4):
                    d = place_of(fs, t, keep)
                    rc(d, d, sg.at[fs, t], rg.at[fs, t], xp).wait_recv()
                    rc(d, d, sf.at[fs, t], rf.at[fs, t], xp).start()

    def je_drain():
        for g in range(4):
            x1(g).wait_send()

        @pl.loop(0, 16)
        def _(fs):
            for t in range(4):
                d = place_of(fs, t, give)
                cp = rc(d, d, sf.at[fs, t], rf.at[fs, t], xp)
                cp.wait_recv()
                cp.wait_send()

            @pl.when(fs != f)
            def _():
                for t in range(4):
                    rc(piece_of(fs, t), place_of(f, t, keep), sg.at[fs, t], rg.at[f, t], xp).wait_send()

            @pl.when(fs == f)
            def _():
                for t in range(4):
                    lc(piece_of(fs, t), place_of(f, t, keep), sg.at[fs, t]).wait()

    @pl.when(zz == 1)
    def _():
        pl.semaphore_wait(ready, 4)

    @pl.when(zz == 0)
    def _():
        pl.semaphore_wait(ready, 3)


    @pl.loop(0, 4)
    def _(i):
        left = X[:, ds(512 * i, 512)]
        T1[:, pl.ds(0, 384)] = mm(left, QKV[...], 0, 0)
        T1[:, pl.ds(384, 512)] = mm(left, SLOPE[...], 0, 0)

        @pl.loop(0, 4)
        def _(s):
            j = 4 * i + s
            columns(j)

            @pl.loop(0, 8)
            def _(k):
                w = ds(128 * s + 16 * k, 16)
                gw = ds(128 * j + 16 * k, 16)
                cw = ds(16 * k, 16)
                for b, (first, count, W) in enumerate(((0, 3, WJ), (384, 4, WE))):
                    g, sh = (PR[ds(256 * b + 128 * v + 16 * k, 16)] for v in range(2))
                    a1 = jnp.zeros((16, 128), f32)
                    a2 = jnp.zeros((16, 128), f32)
                    for t in range(count):
                        l = pl.ds(first + 128 * t, 128)
                        m = T1[w, l]
                        bias = GBR[0:1, l]
                        JB[j, cw, l] = (g * m + sh * bias).astype(bf)
                        wt = W[gw, pl.ds(128 * t, 128)].astype(f32)
                        a1 = a1 + wt * m
                        a2 = a2 + wt * bias
                    for v, a in ((2 * b, a1), (2 * b + 1, a2)):
                        CT[ds(128 * v + 16 * k, 16)] = jnp.broadcast_to(jnp.sum(a, -1, keepdims=True) / g, (16, 128))

            for v in range(4):
                VEC[j, pl.ds(v, 1)] = CT[pl.ds(128 * v, 128)].T[0:1]

        x1(i).start()

        turn_at = phys(jnp.where(i == 0, 3, jnp.where(i == 1, 0, 4 - i)))

        @pl.loop(2 * turn_at, 2 * turn_at + 2)
        def _(b):
            part = ds(256 * b, 256)
            BG[part] = (mm(QKV[part], WJ[...], 1, 1) + mm(SLOPE[part], WE[...], 1, 1)).astype(bf)
            R2[0](b).start()

        @pl.when(i == 0)
        def _():
            R1[2](3)

        @pl.when(i == 1)
        def _():
            R1[2](0)

        @pl.when(i == 2)
        def _():
            R1[2](2)
            R1[5](3)
            R2[1](3)

    def tile(fd, src):
        return rc(VEC.at[fd], VR.at[src], sv.at[fd], rv.at[src], (r, fd))

    for t in range(3):
        VEC[(16 * t + f) // 3, pl.ds(4 + (16 * t + f) % 3, 1)] = GBR[0:1, pl.ds(128 * t, 128)]
    TOT[pl.ds(7, 1)] = BSUM[...]
    for t in range(4):
        TOT[pl.ds(8 + t, 1)] = GBR[0:1, pl.ds(384 + 128 * t, 128)]

    @pl.loop(1, 16)
    def _(k):
        tile((f + k) % 16, f).start()

    VR[f] = VEC[f]
    je_group(0)
    R2[1](0)
    je_group(1)
    R1[2](1)
    R1[5](2)

    def total_rep():
        return rc(TOT, TX, st_, rt_, xp)

    @pl.loop(1, 16)
    def _(k):
        tile(f, (f + k) % 16).wait_recv()

    TOT[pl.ds(0, 7)] = jnp.sum(VR[...], 0)[0:7]
    total_rep().start()
    R2[1](2)
    R2[1](1)
    R1[5](0)
    je_group(2)
    je_group(3)
    R1[3]()
    R2[2](3)
    fwd_group(0)
    R2[2](0)
    fwd_group(1)
    R2[2](2)
    R2[5](3)
    fwd_group(2)
    R2[2](1)
    R2[5](2)
    R2[5](0)
    fwd_group(3)
    R2[3]()
    R1[4](8)
    R2[4]()
    send_small.wait()

    @pl.loop(1, 16)
    def _(k):
        fd = (f + k) % 16
        for t, (s, d) in enumerate(wpieces(f, fd, True)):
            rc(s, d, sw.at[fd, t], rw.at[f, t], (r, fd)).wait_send()

    @pl.loop(1, 16)
    def _(k):
        tile((f + k) % 16, f).wait_send()

    total_rep().wait_recv()
    total_rep().wait_send()
    FIN[...] = TOT[...] + TX[...]
    os_drain()
    je_drain()


def layer_call(x, bg, sm, jw, ew, wo, ws, ct, eb):
    S = jax.ShapeDtypeStruct
    D = pltpu.SemaphoreType.DMA
    V = pltpu.VMEM
    hbm = pl.BlockSpec(memory_space=pl.ANY)
    vm = pl.BlockSpec(memory_space=pltpu.VMEM)
    return pl.pallas_call(
        layer_kernel,
        out_shape=(
            S((128, WIDE), f32), S((128, WIDE), f32), S((640, WIDE), bf), S((128, 3 * WIDE), bf),
            S((128, 4 * WIDE), bf), S((16, 128), f32), S((256, 128), f32),
        ),
        in_specs=[hbm] * 7 + [vm] * 2,
        out_specs=(hbm, hbm, hbm, hbm, hbm, vm, hbm),
        scratch_shapes=[
            V((TOK, WIDE), bf), V((TOK, WIDE), bf), V((WIDE, 384), bf), V((WIDE, 512), bf), V((640, WIDE), bf),
            V((TOK, 640), bf), V((TOK, 384), bf), V((TOK, 512), bf), V((TOK, 128), f32),
            V((TOK, 128), f32), V((8, 128, WIDE), bf), V((4, 128, WIDE), bf), V((8, 128, WIDE), bf),
            V((4, 128, WIDE), bf), V((5, 128, WIDE), bf), V((8, 128, WIDE), bf),
            V((16, 128, 896), bf), V((16, 64, 896), bf), V((4, 640, 512), bf), V((4, 320, 512), bf),
            V((512, 896), f32), V((16, 16, 128), bf), V((256, 128), f32),
            V((8, 896), f32), V((8, 896), f32),
            V((16, 8, 128), f32), V((16, 8, 128), f32), V((16, 128), f32), V((16, 128), f32), V((1, 128), f32),
        ]
        + [D((16,))] * 10 + [D((16, 4))] * 4 + [D((16,))] * 2
        + [D((2, 8))] * 2 + [D((2, 4))] * 3 + [D((2, 5))] + [D((4,))] * 6 + [D((16, 4))] * 4
        + [D((16,))] * 2 + [D, D] + [D((12,)), pltpu.SemaphoreType.REGULAR],
        compiler_params=pltpu.CompilerParams(
            collective_id=0, has_side_effects=True, vmem_limit_bytes=67043328
        ),
    )(x, bg, sm, jw, ew, wo, ws, ct, eb)


def wide(a):
    return a.astype(f32)


def turn_tables(length):
    place = np.arange(length, dtype=np.float32)[:, None]
    power = np.arange(ROT // 2, dtype=np.float32) * np.float32(2.0) / np.float32(ROT)
    angle = place * np.power(np.float32(rotary_base), -power)
    cosine, sine = (np.cos(angle), np.sin(angle))
    rest = np.zeros((length, HEAD_DIM - 2 * ROT))
    return jnp.asarray(np.concatenate([cosine, cosine, -sine, sine, rest], 1), f32)


def head_body(
    n,
    layer_input,
    segment,
    live_mask,
    attention_gain,
    attention_shift,
    joined_weight,
    joined_bias,
    output_weight,
    output_bias,
    feedforward_gain,
    feedforward_shift,
    expand_weight,
    expand_bias,
    shrink_weight,
    shrink_bias,
    cotangent,
):
    own, width = layer_input.shape
    part = width // n
    live_rows = wide(live_mask[0])[:, None]
    seeds = wide(cotangent)
    branch_own = (live_rows * seeds).astype(bf)
    seg = segment[0]
    places = jnp.arange(own, dtype=jnp.int32)
    earlier = jnp.sum((seg[None, :] < seg[:, None]).astype(jnp.int32), -1)
    lines = (
        attention_gain.reshape(1, part),
        attention_shift.reshape(1, part),
        feedforward_gain.reshape(1, part),
        feedforward_shift.reshape(1, part),
        output_bias.reshape(1, part),
        shrink_bias.reshape(1, part),
        joined_bias.reshape(3, part),
        segment.astype(bf),
        (places - earlier).astype(bf).reshape(1, own),
    )
    row = lax.broadcasted_iota(jnp.int32, (16, 128), 0)
    small = jnp.zeros((16, 128), bf)
    at = 0
    for item in lines:
        for k in range(item.shape[0]):
            small = jnp.where(row == at, item[k : k + 1], small)
            at += 1
    ct = turn_tables(own)
    rows_own = wide(layer_input)
    centred = rows_own - jnp.mean(rows_own, -1, keepdims=True)
    inverse = lax.rsqrt(jnp.mean(centred * centred, -1, keepdims=True) + epsilon)
    normalized = centred * inverse
    summed, hat_own, os_grad, joined_grad, expand_grad, sums, small_all = layer_call(
        normalized.astype(bf), branch_own, small, joined_weight, expand_weight, output_weight, shrink_weight,
        ct, wide(expand_bias).reshape(1, -1),
    )
    small_all = small_all.reshape(n, 16, part)
    bias = (small_all[:, 4] + small_all[:, 5]).reshape(width)
    layer_output = (rows_own + live_rows * (summed + bias)).astype(bf)
    row_grad = inverse * (
        hat_own
        - jnp.mean(hat_own, -1, keepdims=True)
        - normalized * jnp.mean(hat_own * normalized, -1, keepdims=True)
    )
    input_grad = (seeds + row_grad).astype(bf)

    return (
        layer_output,
        input_grad,
        sums[0],
        sums[1],
        wide(joined_grad),
        sums[4:7].reshape(-1),
        wide(os_grad[:part]),
        sums[7],
        sums[2],
        sums[3],
        wide(expand_grad),
        sums[8:12].reshape(-1),
        wide(os_grad[part:]),
        sums[7],
    )


def solution(mesh):
    n = mesh.shape["fsdp"]
    fits = n == HEADS and mesh.shape["rep"] == 2
    chosen = functools.partial(head_body, n) if fits else body
    placed = (
        P(("rep", "fsdp"), None),
        P(("rep", "fsdp"), None),
        P(("rep", "fsdp"), None),
        P("fsdp"),
        P("fsdp"),
        P("fsdp", None),
        P("fsdp"),
        P("fsdp", None),
        P("fsdp"),
        P("fsdp"),
        P("fsdp"),
        P("fsdp", None),
        P("fsdp"),
        P("fsdp", None),
        P("fsdp"),
        P(("rep", "fsdp"), None),
    )
    return jax.shard_map(
        chosen,
        mesh=mesh,
        in_specs=placed,
        out_specs=(
            P(("rep", "fsdp"), None),
            P(("rep", "fsdp"), None),
            P("fsdp"),
            P("fsdp"),
            P("fsdp", None),
            P("fsdp"),
            P("fsdp", None),
            P("fsdp"),
            P("fsdp"),
            P("fsdp"),
            P("fsdp", None),
            P("fsdp"),
            P("fsdp", None),
            P("fsdp"),
        ),
        check_vma=False,
    )
```
